8 devices in a mesh: tp: 2 (over z, y), dp: 4 (over x, core).
Axes of the slice: x: 2, y: 2, z: 1, core: 2. Of those that a mesh axis runs over, the one named last changes fastest.
Arguments:
- x_in: bfloat16 [128, 4096], P('dp')
- w_gate: bfloat16 [4096, 11008], P('dp', 'tp')
- w_up: bfloat16 [4096, 11008], P('dp', 'tp')
- w_down: bfloat16 [11008, 4096], P('tp', 'dp')
- dy_in: bfloat16 [128, 4096], P('dp')
Outputs:
- output 1: bfloat16 [128, 4096], P('dp')
- output 2: bfloat16 [128, 4096], P('dp')
- output 3: float32 [4096, 11008], P('dp', 'tp')
- output 4: float32 [4096, 11008], P('dp', 'tp')
- output 5: float32 [11008, 4096], P('tp', 'dp')
All inputs are finite; a program needn't handle non-finite values.
Results may differ from the reference program's by a relative error of at most 0.001.
Values are sent between devices in bfloat16 or wider.
A program may use at most 1 GiB of HBM per device.

```python
import jax
import jax.numpy as jnp
from jax import lax

MODEL_DIM = 4096
HIDDEN_DIM = 11008
SHARD_TOKENS = 32
DATA_SHARDS = 4


def setup_inputs(seed: int = 0) -> dict:
    key_list = jax.random.split(jax.random.key(seed), 5)
    row_count = DATA_SHARDS * SHARD_TOKENS
    x_vals = jax.random.normal(key_list[0], (row_count, MODEL_DIM), jnp.float32)
    gate_vals = jax.random.normal(key_list[1], (MODEL_DIM, HIDDEN_DIM), jnp.float32) * MODEL_DIM ** -0.5
    up_vals = jax.random.normal(key_list[2], (MODEL_DIM, HIDDEN_DIM), jnp.float32) * MODEL_DIM ** -0.5
    down_vals = jax.random.normal(key_list[3], (HIDDEN_DIM, MODEL_DIM), jnp.float32) * HIDDEN_DIM ** -0.5
    dy_vals = jax.random.normal(key_list[4], (row_count, MODEL_DIM), jnp.float32)
    return {
        'x_in': x_vals.astype(jnp.bfloat16),
        'w_gate': gate_vals.astype(jnp.bfloat16),
        'w_up': up_vals.astype(jnp.bfloat16),
        'w_down': down_vals.astype(jnp.bfloat16),
        'dy_in': dy_vals.astype(jnp.bfloat16),
    }


def reference(x_in, w_gate, w_up, w_down, dy_in):
    row_count = DATA_SHARDS * SHARD_TOKENS
    x_blocks = x_in.reshape(DATA_SHARDS, SHARD_TOKENS, MODEL_DIM)
    dy_blocks = dy_in.reshape(DATA_SHARDS, SHARD_TOKENS, MODEL_DIM)

    def shard_pass(carry, block):
        acc_gate, acc_up, acc_down = carry
        x_blk, dy_blk = block
        gate_pre = jnp.dot(x_blk, w_gate, preferred_element_type=jnp.float32)
        up_pre = jnp.dot(x_blk, w_up, preferred_element_type=jnp.float32)
        sig_gate = jax.nn.sigmoid(gate_pre)
        silu_gate = gate_pre * sig_gate
        hidden = (silu_gate * up_pre).astype(jnp.bfloat16)
        y_blk = (x_blk.astype(jnp.float32) + jnp.dot(hidden, w_down, preferred_element_type=jnp.float32)).astype(jnp.bfloat16)
        grad_h = jnp.dot(dy_blk, w_down.T, preferred_element_type=jnp.float32)
        d_gate = (grad_h * up_pre * sig_gate * (1.0 + gate_pre * (1.0 - sig_gate))).astype(jnp.bfloat16)
        d_up = (grad_h * silu_gate).astype(jnp.bfloat16)
        dx_blk = (dy_blk.astype(jnp.float32)
                  + jnp.dot(d_gate, w_gate.T, preferred_element_type=jnp.float32)
                  + jnp.dot(d_up, w_up.T, preferred_element_type=jnp.float32)).astype(jnp.bfloat16)
        acc_gate = acc_gate + jnp.dot(x_blk.T, d_gate, preferred_element_type=jnp.float32)
        acc_up = acc_up + jnp.dot(x_blk.T, d_up, preferred_element_type=jnp.float32)
        acc_down = acc_down + jnp.dot(hidden.T, dy_blk, preferred_element_type=jnp.float32)
        return (acc_gate, acc_up, acc_down), (y_blk, dx_blk)

    zero_acc = (jnp.zeros((MODEL_DIM, HIDDEN_DIM), jnp.float32),
                jnp.zeros((MODEL_DIM, HIDDEN_DIM), jnp.float32),
                jnp.zeros((HIDDEN_DIM, MODEL_DIM), jnp.float32))
    sums, outs = lax.scan(shard_pass, zero_acc, (x_blocks, dy_blocks))
    y_blocks, dx_blocks = outs
    return (y_blocks.reshape(row_count, MODEL_DIM), dx_blocks.reshape(row_count, MODEL_DIM), sums[0], sums[1], sums[2])
```

```python
import functools

import jax
import jax.numpy as jnp
from jax import lax
from jax.experimental import pallas as pl
from jax.experimental.pallas import tpu as pltpu
from jax.sharding import PartitionSpec as P

MESH = pl.DeviceIdType.MESH
F32, BF16 = jnp.float32, jnp.bfloat16
VMEM_CAP = 67043328
WIDTHS = (256, 768, 1024, 1024, 1024, 1024, 384)
STARTS = tuple(sum(WIDTHS[:k]) for k in range(len(WIDTHS)))
NCH = len(WIDTHS)
HID = sum(WIDTHS)


def column_tiles(start, width, body):
    full = width // 256

    def step(i, carry):
        body(pl.multiple_of(start + i * 256, 128), 256)
        return carry

    lax.fori_loop(0, full, step, 0)
    if width % 256:
        body(start + full * 256, width % 256)


def exchange_kernel(x_ref, dy_ref, wg_hbm, wu_hbm, wd_hbm,
                    act_out, cols_out, keep_out, give_out, kept_cols_out,
                    wg, wu, wd, part, from_sib, from_opp, act, cols, acc,
                    w_sem, x_send, x_recv, s1_send, s1_recv, s2_send, s2_recv,
                    sib_send, sib_recv, opp_send, opp_recv, fwd_send, fwd_recv, out_sem, col_sem, acc_sem):
    t = lax.axis_index('tp')
    d = lax.axis_index('dp')
    cx, c = d // 2, lax.rem(d, 2)
    sib = 2 * cx + (1 - c)
    opp = 2 * (1 - cx) + c
    far = 2 * (1 - cx) + (1 - c)
    own_row = pl.multiple_of(32 * (2 * c + cx), 32)
    opp_row = pl.multiple_of(32 * (2 * c + 1 - cx), 32)
    sib_row = pl.multiple_of(32 * (2 * (1 - c) + cx), 32)
    far_row = pl.multiple_of(32 * (2 * (1 - c) + 1 - cx), 32)
    sib_half = pl.multiple_of(64 * (1 - c), 64)

    def weight_copies(k):
        cs = pl.ds(STARTS[k], WIDTHS[k])
        return (pltpu.make_async_copy(wg_hbm.at[:, cs], wg.at[:, cs], w_sem.at[0, k]),
                pltpu.make_async_copy(wu_hbm.at[:, cs], wu.at[:, cs], w_sem.at[1, k]),
                pltpu.make_async_copy(wd_hbm.at[cs, :], wd.at[cs, :], w_sem.at[2, k]))

    for k in range(NCH):
        for copy in weight_copies(k):
            copy.start()

    barrier = pltpu.get_barrier_semaphore()
    peers = (sib, opp, far)
    for p in peers:
        pl.semaphore_signal(barrier, inc=1, device_id={'dp': p}, device_id_type=MESH)
    pl.semaphore_wait(barrier, 3)

    def token_copy(i, ref, q, row):
        block = pl.ds(pl.multiple_of(1024 * peers[q], 128), 1024)
        return pltpu.make_async_remote_copy(
            src_ref=ref.at[:, block], dst_ref=cols.at[i, pl.ds(row, 32), :],
            send_sem=x_send.at[i, q], recv_sem=x_recv.at[i, q],
            device_id={'dp': peers[q]}, device_id_type=MESH)

    own_block = pl.ds(pl.multiple_of(1024 * d, 128), 1024)
    for i, ref in enumerate((x_ref, dy_ref)):
        for q in (2, 1, 0):
            token_copy(i, ref, q, own_row).start()
    for i, ref in enumerate((x_ref, dy_ref)):
        cols[i, pl.ds(own_row, 32), :] = ref[:, own_block]
    arrival_rows = (sib_row, opp_row, far_row)

    def token_wait(i, ref):
        for q in range(3):
            token_copy(i, ref, q, arrival_rows[q]).wait_recv()

    def s1(k):
        cs = pl.ds(STARTS[k], WIDTHS[k])
        return pltpu.make_async_remote_copy(
            src_ref=part.at[:, pl.ds(sib_half, 64), cs], dst_ref=from_sib.at[:, :, cs],
            send_sem=s1_send.at[k], recv_sem=s1_recv.at[k], device_id={'dp': sib}, device_id_type=MESH)

    def s2(k):
        cs = pl.ds(STARTS[k], WIDTHS[k])
        return pltpu.make_async_remote_copy(
            src_ref=part.at[:, pl.ds(opp_row, 32), cs], dst_ref=from_opp.at[:, :, cs],
            send_sem=s2_send.at[k], recv_sem=s2_recv.at[k], device_id={'dp': opp}, device_id_type=MESH)

    def act_copy(k, src_row, dst_row, send, recv, to):
        cs = pl.ds(STARTS[k], WIDTHS[k])
        return pltpu.make_async_remote_copy(
            src_ref=act.at[:, pl.ds(src_row, 32), cs], dst_ref=act.at[:, pl.ds(dst_row, 32), cs],
            send_sem=send.at[k], recv_sem=recv.at[k], device_id={'dp': to}, device_id_type=MESH)

    def partials(k):
        copies = weight_copies(k)
        copies[0].wait()
        copies[1].wait()
        if k == 0:
            token_wait(0, x_ref)

        def first(col, width):
            cs = pl.ds(col, width)
            part[0, :, cs] = jnp.dot(cols[0], wg[:, cs], preferred_element_type=F32)
            part[1, :, cs] = jnp.dot(cols[0], wu[:, cs], preferred_element_type=F32)

        def second(col, width):
            cs = pl.ds(col, width)
            part[2, :, cs] = lax.dot_general(cols[1], wd[cs, :], (((1,), (1,)), ((), ())),
                                             preferred_element_type=F32)

        def both(col, width):
            first(col, width)
            second(col, width)

        if k == 0:
            column_tiles(STARTS[k], WIDTHS[k], first)
            copies[2].wait()
            token_wait(1, dy_ref)
            column_tiles(STARTS[k], WIDTHS[k], second)
        else:
            copies[2].wait()
            column_tiles(STARTS[k], WIDTHS[k], both)
        s1(k).start()

    def chip_sum(k):
        s1(k).wait_recv()
        half = pl.multiple_of(32 * (1 - cx), 32)

        def add(col, width):
            cs = pl.ds(col, width)
            for i in range(3):
                part[i, pl.ds(opp_row, 32), cs] += from_sib[i, pl.ds(half, 32), cs]

        column_tiles(STARTS[k], WIDTHS[k], add)
        s2(k).start()

    def activations(k):
        s2(k).wait_recv()
        half = pl.multiple_of(32 * cx, 32)

        def body(col, width):
            cs = pl.ds(col, width)
            own = pl.ds(own_row, 32)
            mine = [part[i, own, cs] + from_sib[i, pl.ds(half, 32), cs] for i in range(3)]
            a, b, g = [mine[i] + from_opp[i, :, cs] for i in range(3)]
            s = jax.nn.sigmoid(a)
            silu = a * s
            act[0, own, cs] = (silu * b).astype(BF16)
            act[1, own, cs] = (g * b * s * (1.0 + a * (1.0 - s))).astype(BF16)
            act[2, own, cs] = (g * silu).astype(BF16)

        column_tiles(STARTS[k], WIDTHS[k], body)
        act_copy(k, own_row, own_row, opp_send, opp_recv, opp).start()
        act_copy(k, own_row, own_row, sib_send, sib_recv, sib).start()

    def forward(k):
        act_copy(k, own_row, opp_row, opp_send, opp_recv, opp).wait_recv()
        act_copy(k, opp_row, opp_row, fwd_send, fwd_recv, sib).start()

    def act_store(k):
        cs = pl.ds(STARTS[k], WIDTHS[k])
        return pltpu.make_async_copy(act.at[:, :, cs], act_out.at[:, :, cs], out_sem.at[k])

    def outputs(k):
        act_copy(k, own_row, sib_row, sib_send, sib_recv, sib).wait_recv()
        act_copy(k, opp_row, far_row, fwd_send, fwd_recv, sib).wait_recv()
        act_store(k).start()
        cs = pl.ds(STARTS[k], WIDTHS[k])

        def step(n, carry):
            ns = pl.ds(pl.multiple_of(n * 256, 256), 256)
            y = jnp.dot(act[0, :, cs], wd[cs, ns], preferred_element_type=F32)
            dx = (lax.dot_general(act[1, :, cs], wg[ns, cs], (((1,), (1,)), ((), ())), preferred_element_type=F32)
                  + lax.dot_general(act[2, :, cs], wu[ns, cs], (((1,), (1,)), ((), ())), preferred_element_type=F32))
            if k == 0:
                acc[0, :, ns] = y
                acc[1, :, ns] = dx
            else:
                acc[0, :, ns] += y
                acc[1, :, ns] += dx
            return carry

        lax.fori_loop(0, 4, step, 0)

    for k in range(NCH):
        partials(k)
        if k == 0:
            store_cols = pltpu.make_async_copy(cols, cols_out, col_sem.at[0])
            store_cols.start()
            store_kept = pltpu.make_async_copy(cols.at[:, pl.ds(pl.multiple_of(64 * t, 64), 64), :],
                                               kept_cols_out, col_sem.at[1])
            store_kept.start()
        if k >= 1:
            chip_sum(k - 1)
    chip_sum(NCH - 1)
    for k in range(NCH):
        activations(k)
    for k in range(NCH):
        forward(k)
        if k >= 1:
            outputs(k - 1)
    outputs(NCH - 1)
    store_keep = pltpu.make_async_copy(acc.at[:, pl.ds(pl.multiple_of(64 * t, 64), 64), :], keep_out, acc_sem.at[0])
    store_give = pltpu.make_async_copy(acc.at[:, pl.ds(pl.multiple_of(64 * (1 - t), 64), 64), :], give_out,
                                       acc_sem.at[1])
    store_give.start()
    store_keep.start()
    for i, ref in enumerate((x_ref, dy_ref)):
        for q in range(3):
            token_copy(i, ref, q, own_row).wait_send()
    for k in range(NCH):
        s1(k).wait_send()
        s2(k).wait_send()
        act_copy(k, own_row, own_row, opp_send, opp_recv, opp).wait_send()
        act_copy(k, own_row, own_row, sib_send, sib_recv, sib).wait_send()
        act_copy(k, opp_row, opp_row, fwd_send, fwd_recv, sib).wait_send()
        act_store(k).wait()
    store_cols.wait()
    store_kept.wait()
    store_give.wait()
    store_keep.wait()


def exchange(x_rows, dy_rows, gate, up, down):
    hbm = pl.BlockSpec(memory_space=pl.ANY)
    vmem = pl.BlockSpec(memory_space=pltpu.VMEM)
    dma = pltpu.SemaphoreType.DMA
    return pl.pallas_call(
        exchange_kernel,
        name='exchange',
        out_shape=(jax.ShapeDtypeStruct((3, 128, HID), BF16),
                   jax.ShapeDtypeStruct((2, 128, 1024), BF16),
                   jax.ShapeDtypeStruct((2, 64, 1024), F32),
                   jax.ShapeDtypeStruct((2, 64, 1024), F32),
                   jax.ShapeDtypeStruct((2, 64, 1024), BF16)),
        in_specs=[vmem, vmem, hbm, hbm, hbm],
        out_specs=(hbm,) * 5,
        scratch_shapes=[
            pltpu.VMEM((1024, HID), BF16), pltpu.VMEM((1024, HID), BF16), pltpu.VMEM((HID, 1024), BF16),
            pltpu.VMEM((3, 128, HID), F32), pltpu.VMEM((3, 64, HID), F32), pltpu.VMEM((3, 32, HID), F32),
            pltpu.VMEM((3, 128, HID), BF16), pltpu.VMEM((2, 128, 1024), BF16), pltpu.VMEM((2, 128, 1024), F32),
            dma((3, NCH)), dma((2, 3)), dma((2, 3)),
            dma((NCH,)), dma((NCH,)), dma((NCH,)), dma((NCH,)),
            dma((NCH,)), dma((NCH,)), dma((NCH,)), dma((NCH,)), dma((NCH,)), dma((NCH,)),
            dma((NCH,)), dma((2,)), dma((2,)),
        ],
        compiler_params=pltpu.CompilerParams(collective_id=0, has_side_effects=True, vmem_limit_bytes=VMEM_CAP),
        cost_estimate=pl.CostEstimate(flops=9 * 10**9, bytes_accessed=4 * 10**7, transcendentals=0),
    )(x_rows, dy_rows, gate, up, down)


def finish_kernel(keep_ref, got_ref, kept_cols_ref, y_out, dx_out, ready, landed, send_sem, recv_sem, loc_sem):
    t = lax.axis_index('tp')
    d = lax.axis_index('dp')
    cx, c = d // 2, lax.rem(d, 2)
    barrier = pltpu.get_barrier_semaphore()
    for dt in range(2):
        for dd in range(4):
            if dt or dd:
                pl.semaphore_signal(barrier, inc=1, device_id={'tp': lax.rem(t + dt, 2), 'dp': lax.rem(d + dd, 4)},
                                    device_id_type=MESH)
    total = keep_ref[...] + got_ref[...]
    ready[...] = (kept_cols_ref[...].astype(F32) + total).astype(BF16)
    pl.semaphore_wait(barrier, 7)
    block = pl.ds(pl.multiple_of(1024 * d, 128), 1024)

    def send(ocx, ot):
        chip = cx if ocx == 0 else 1 - cx
        return pltpu.make_async_remote_copy(
            src_ref=ready.at[:, pl.ds(pl.multiple_of(32 * chip, 32), 32), :],
            dst_ref=landed.at[:, :, block],
            send_sem=send_sem.at[2 * ocx + ot], recv_sem=recv_sem.at[d],
            device_id={'tp': t if ot == 0 else 1 - t, 'dp': 2 * chip + t}, device_id_type=MESH)

    def arrive(s):
        return pltpu.make_async_remote_copy(
            src_ref=ready.at[:, pl.ds(0, 32), :], dst_ref=landed.at[:, :, pl.ds(1024 * s, 1024)],
            send_sem=send_sem.at[0], recv_sem=recv_sem.at[s],
            device_id={'tp': 1 - t}, device_id_type=MESH)

    local = c == t
    for ocx, ot in ((1, 1), (1, 0), (0, 1)):
        send(ocx, ot).start()

    @pl.when(jnp.logical_not(local))
    def _():
        send(0, 0).start()

    @pl.when(local)
    def _():
        landed[:, :, block] = ready[:, pl.ds(pl.multiple_of(32 * cx, 32), 32), :]

    for s in range(4):
        @pl.when(jnp.logical_not(jnp.logical_and(local, d == s)))
        def _():
            arrive(s).wait_recv()

    stores = (pltpu.make_async_copy(landed.at[0], y_out, loc_sem.at[0]),
              pltpu.make_async_copy(landed.at[1], dx_out, loc_sem.at[1]))
    for s in stores:
        s.start()
    for ocx, ot in ((1, 1), (1, 0), (0, 1)):
        send(ocx, ot).wait_send()

    @pl.when(jnp.logical_not(local))
    def _():
        send(0, 0).wait_send()

    for s in stores:
        s.wait()


def finish(keep, got, kept_cols):
    vmem = pl.BlockSpec(memory_space=pltpu.VMEM)
    hbm = pl.BlockSpec(memory_space=pl.ANY)
    rows = jax.ShapeDtypeStruct((32, 4096), BF16)
    dma = pltpu.SemaphoreType.DMA
    return pl.pallas_call(
        finish_kernel,
        name='finish',
        out_shape=(rows, rows),
        in_specs=[vmem] * 3,
        out_specs=(hbm, hbm),
        scratch_shapes=[pltpu.VMEM((2, 64, 1024), BF16), pltpu.VMEM((2, 32, 4096), BF16),
                        dma((4,)), dma((4,)), dma((2,))],
        compiler_params=pltpu.CompilerParams(collective_id=1, has_side_effects=True),
        cost_estimate=pl.CostEstimate(flops=10**6, bytes_accessed=2 * 10**6, transcendentals=0),
    )(keep, got, kept_cols)


def grad_cols_kernel(cols_ref, act_ref, o_ref):
    o_ref[...] = lax.dot_general(cols_ref[...], act_ref[...], (((0,), (0,)), ((), ())), preferred_element_type=F32)


def grad_up(cols, act, which):
    return pl.pallas_call(
        grad_cols_kernel,
        name='grad_in',
        grid=(pl.cdiv(HID, 512),),
        out_shape=jax.ShapeDtypeStruct((1024, HID), F32),
        in_specs=[pl.BlockSpec((None, 128, 1024), lambda i: (0, 0, 0)),
                  pl.BlockSpec((None, 128, 512), lambda i: (which, 0, i))],
        out_specs=pl.BlockSpec((1024, 512), lambda i: (0, i)),
        cost_estimate=pl.CostEstimate(flops=2 * 128 * 1024 * HID, bytes_accessed=4 * 1024 * HID, transcendentals=0),
    )(cols, act)


def grad_down(cols, act):
    return pl.pallas_call(
        grad_cols_kernel,
        name='grad_out',
        grid=(pl.cdiv(HID, 512),),
        out_shape=jax.ShapeDtypeStruct((HID, 1024), F32),
        in_specs=[pl.BlockSpec((None, 128, 512), lambda i: (0, 0, i)),
                  pl.BlockSpec((None, 128, 1024), lambda i: (1, 0, 0))],
        out_specs=pl.BlockSpec((512, 1024), lambda i: (i, 0)),
        cost_estimate=pl.CostEstimate(flops=2 * 128 * 1024 * HID, bytes_accessed=4 * 1024 * HID, transcendentals=0),
    )(act, cols)


def solution(mesh):
    def device_pass(x_rows, gate_blk, up_blk, down_blk, dy_rows):
        act, cols, keep, give, kept_cols = exchange(x_rows, dy_rows, gate_blk, up_blk, down_blk)
        got = lax.ppermute(give, 'tp', [(0, 1), (1, 0)])
        dw_down = grad_down(cols, act)
        dw_gate = grad_up(cols, act, 1)
        dw_up = grad_up(cols, act, 2)
        y_rows, dx_rows = finish(keep, got, kept_cols)
        return y_rows, dx_rows, dw_gate, dw_up, dw_down

    row_spec = P('dp', None)
    weight_spec = P('dp', 'tp')
    down_spec = P('tp', 'dp')
    return jax.shard_map(device_pass, mesh=mesh,
                         in_specs=(row_spec, weight_spec, weight_spec, down_spec, row_spec),
                         out_specs=(row_spec, row_spec, weight_spec, weight_spec, down_spec),
                         check_vma=False)
```

```python
import functools

import jax
import jax.numpy as jnp
from jax import lax
from jax.experimental import pallas as pl
from jax.experimental.pallas import tpu as pltpu
from jax.sharding import PartitionSpec as P

MESH = pl.DeviceIdType.MESH
F32, BF16 = jnp.float32, jnp.bfloat16
VMEM_CAP = 67043328
WIDTHS = (256, 768, 1024, 1024, 1024, 1024, 384)
STARTS = tuple(sum(WIDTHS[:k]) for k in range(len(WIDTHS)))
NCH = len(WIDTHS)
HID = sum(WIDTHS)


def column_tiles(start, width, body):
    full = width // 256

    def step(i, carry):
        body(pl.multiple_of(start + i * 256, 128), 256)
        return carry

    lax.fori_loop(0, full, step, 0)
    if width % 256:
        body(start + full * 256, width % 256)


def exchange_kernel(x_ref, dy_ref, wg_hbm, wu_hbm, wd_hbm,
                    act_out, act_t_out, cols_t_out, dy_cols_out, keep_out, give_out, kept_cols_out,
                    wg, wu, wd, part, from_sib, from_opp, act, act_t, cols, cols_t, acc,
                    w_sem, x_send, x_recv, s1_send, s1_recv, s2_send, s2_recv,
                    sib_send, sib_recv, opp_send, opp_recv, fwd_send, fwd_recv, out_sem, out_t_sem, col_sem, acc_sem):
    t = lax.axis_index('tp')
    d = lax.axis_index('dp')
    cx, c = d // 2, lax.rem(d, 2)
    sib = 2 * cx + (1 - c)
    opp = 2 * (1 - cx) + c
    far = 2 * (1 - cx) + (1 - c)
    own_row = pl.multiple_of(32 * (2 * c + cx), 32)
    opp_row = pl.multiple_of(32 * (2 * c + 1 - cx), 32)
    sib_row = pl.multiple_of(32 * (2 * (1 - c) + cx), 32)
    far_row = pl.multiple_of(32 * (2 * (1 - c) + 1 - cx), 32)
    sib_half = pl.multiple_of(64 * (1 - c), 64)

    def weight_copies(k):
        cs = pl.ds(STARTS[k], WIDTHS[k])
        return (pltpu.make_async_copy(wg_hbm.at[:, cs], wg.at[:, cs], w_sem.at[0, k]),
                pltpu.make_async_copy(wu_hbm.at[:, cs], wu.at[:, cs], w_sem.at[1, k]),
                pltpu.make_async_copy(wd_hbm.at[cs, :], wd.at[cs, :], w_sem.at[2, k]))

    for k in range(NCH):
        for copy in weight_copies(k):
            copy.start()

    barrier = pltpu.get_barrier_semaphore()
    peers = (sib, opp, far)
    for p in peers:
        pl.semaphore_signal(barrier, inc=1, device_id={'dp': p}, device_id_type=MESH)
    pl.semaphore_wait(barrier, 3)

    def token_copy(i, ref, q, row):
        block = pl.ds(pl.multiple_of(1024 * peers[q], 128), 1024)
        return pltpu.make_async_remote_copy(
            src_ref=ref.at[:, block], dst_ref=cols.at[i, pl.ds(row, 32), :],
            send_sem=x_send.at[i, q], recv_sem=x_recv.at[i, q],
            device_id={'dp': peers[q]}, device_id_type=MESH)

    own_block = pl.ds(pl.multiple_of(1024 * d, 128), 1024)
    for i, ref in enumerate((x_ref, dy_ref)):
        for q in (2, 1, 0):
            token_copy(i, ref, q, own_row).start()
    for i, ref in enumerate((x_ref, dy_ref)):
        cols[i, pl.ds(own_row, 32), :] = ref[:, own_block]
    arrival_rows = (sib_row, opp_row, far_row)

    def token_wait(i, ref):
        for q in range(3):
            token_copy(i, ref, q, arrival_rows[q]).wait_recv()

    def s1(k):
        cs = pl.ds(STARTS[k], WIDTHS[k])
        return pltpu.make_async_remote_copy(
            src_ref=part.at[:, pl.ds(sib_half, 64), cs], dst_ref=from_sib.at[:, :, cs],
            send_sem=s1_send.at[k], recv_sem=s1_recv.at[k], device_id={'dp': sib}, device_id_type=MESH)

    def s2(k):
        cs = pl.ds(STARTS[k], WIDTHS[k])
        return pltpu.make_async_remote_copy(
            src_ref=part.at[:, pl.ds(opp_row, 32), cs], dst_ref=from_opp.at[:, :, cs],
            send_sem=s2_send.at[k], recv_sem=s2_recv.at[k], device_id={'dp': opp}, device_id_type=MESH)

    def act_copy(k, src_row, dst_row, send, recv, to):
        cs = pl.ds(STARTS[k], WIDTHS[k])
        return pltpu.make_async_remote_copy(
            src_ref=act.at[:, pl.ds(src_row, 32), cs], dst_ref=act.at[:, pl.ds(dst_row, 32), cs],
            send_sem=send.at[k], recv_sem=recv.at[k], device_id={'dp': to}, device_id_type=MESH)

    def partials(k):
        copies = weight_copies(k)
        copies[0].wait()
        copies[1].wait()
        if k == 0:
            token_wait(0, x_ref)

        def first(col, width):
            cs = pl.ds(col, width)
            part[0, :, cs] = jnp.dot(cols[0], wg[:, cs], preferred_element_type=F32)
            part[1, :, cs] = jnp.dot(cols[0], wu[:, cs], preferred_element_type=F32)

        def second(col, width):
            cs = pl.ds(col, width)
            part[2, :, cs] = lax.dot_general(cols[1], wd[cs, :], (((1,), (1,)), ((), ())),
                                             preferred_element_type=F32)

        def both(col, width):
            first(col, width)
            second(col, width)

        if k == 0:
            column_tiles(STARTS[k], WIDTHS[k], first)
            copies[2].wait()
            token_wait(1, dy_ref)
            column_tiles(STARTS[k], WIDTHS[k], second)
        else:
            copies[2].wait()
            column_tiles(STARTS[k], WIDTHS[k], both)
        s1(k).start()

    def chip_sum(k):
        s1(k).wait_recv()
        half = pl.multiple_of(32 * (1 - cx), 32)

        def add(col, width):
            cs = pl.ds(col, width)
            for i in range(3):
                part[i, pl.ds(opp_row, 32), cs] += from_sib[i, pl.ds(half, 32), cs]

        column_tiles(STARTS[k], WIDTHS[k], add)
        s2(k).start()

    def activations(k):
        s2(k).wait_recv()
        half = pl.multiple_of(32 * cx, 32)

        def body(col, width):
            cs = pl.ds(col, width)
            own = pl.ds(own_row, 32)
            mine = [part[i, own, cs] + from_sib[i, pl.ds(half, 32), cs] for i in range(3)]
            a, b, g = [mine[i] + from_opp[i, :, cs] for i in range(3)]
            s = jax.nn.sigmoid(a)
            silu = a * s
            act[0, own, cs] = (silu * b).astype(BF16)
            act[1, own, cs] = (g * b * s * (1.0 + a * (1.0 - s))).astype(BF16)
            act[2, own, cs] = (g * silu).astype(BF16)

        column_tiles(STARTS[k], WIDTHS[k], body)
        act_copy(k, own_row, own_row, opp_send, opp_recv, opp).start()
        act_copy(k, own_row, own_row, sib_send, sib_recv, sib).start()

    def forward(k):
        act_copy(k, own_row, opp_row, opp_send, opp_recv, opp).wait_recv()
        act_copy(k, opp_row, opp_row, fwd_send, fwd_recv, sib).start()

    def act_store(k):
        cs = pl.ds(STARTS[k], WIDTHS[k])
        return (pltpu.make_async_copy(act.at[pl.ds(1, 2), :, cs], act_out.at[:, :, cs], out_sem.at[k]),
                pltpu.make_async_copy(act_t.at[cs, :], act_t_out.at[cs, :], out_t_sem.at[k]))

    def outputs(k):
        act_copy(k, own_row, sib_row, sib_send, sib_recv, sib).wait_recv()
        act_copy(k, opp_row, far_row, fwd_send, fwd_recv, sib).wait_recv()
        cs = pl.ds(STARTS[k], WIDTHS[k])

        def flip(col, width):
            ts = pl.ds(col, width)
            act_t[ts, :] = act[0, :, ts].T

        column_tiles(STARTS[k], WIDTHS[k], flip)
        for copy in act_store(k):
            copy.start()

        def step(n, carry):
            ns = pl.ds(pl.multiple_of(n * 256, 256), 256)
            y = jnp.dot(act[0, :, cs], wd[cs, ns], preferred_element_type=F32)
            dx = (lax.dot_general(act[1, :, cs], wg[ns, cs], (((1,), (1,)), ((), ())), preferred_element_type=F32)
                  + lax.dot_general(act[2, :, cs], wu[ns, cs], (((1,), (1,)), ((), ())), preferred_element_type=F32))
            if k == 0:
                acc[0, :, ns] = y
                acc[1, :, ns] = dx
            else:
                acc[0, :, ns] += y
                acc[1, :, ns] += dx
            return carry

        lax.fori_loop(0, 4, step, 0)

    for k in range(NCH):
        partials(k)
        if k == 0:
            store_dy = pltpu.make_async_copy(cols.at[1], dy_cols_out, col_sem.at[0])
            store_dy.start()
            store_kept = pltpu.make_async_copy(cols.at[:, pl.ds(pl.multiple_of(64 * t, 64), 64), :],
                                               kept_cols_out, col_sem.at[1])
            store_kept.start()
        if k == 1:
            for n in range(4):
                cols_t[n * 256:(n + 1) * 256, :] = cols[0, :, n * 256:(n + 1) * 256].T
            store_cols_t = pltpu.make_async_copy(cols_t, cols_t_out, col_sem.at[2])
            store_cols_t.start()
        if k >= 1:
            chip_sum(k - 1)
    chip_sum(NCH - 1)
    for k in range(NCH):
        activations(k)
    for k in range(NCH):
        forward(k)
        if k >= 1:
            outputs(k - 1)
    outputs(NCH - 1)
    store_keep = pltpu.make_async_copy(acc.at[:, pl.ds(pl.multiple_of(64 * t, 64), 64), :], keep_out, acc_sem.at[0])
    store_give = pltpu.make_async_copy(acc.at[:, pl.ds(pl.multiple_of(64 * (1 - t), 64), 64), :], give_out,
                                       acc_sem.at[1])
    store_give.start()
    store_keep.start()
    for i, ref in enumerate((x_ref, dy_ref)):
        for q in range(3):
            token_copy(i, ref, q, own_row).wait_send()
    for k in range(NCH):
        s1(k).wait_send()
        s2(k).wait_send()
        act_copy(k, own_row, own_row, opp_send, opp_recv, opp).wait_send()
        act_copy(k, own_row, own_row, sib_send, sib_recv, sib).wait_send()
        act_copy(k, opp_row, opp_row, fwd_send, fwd_recv, sib).wait_send()
        for copy in act_store(k):
            copy.wait()
    store_dy.wait()
    store_cols_t.wait()
    store_kept.wait()
    store_give.wait()
    store_keep.wait()


def exchange(x_rows, dy_rows, gate, up, down):
    hbm = pl.BlockSpec(memory_space=pl.ANY)
    vmem = pl.BlockSpec(memory_space=pltpu.VMEM)
    dma = pltpu.SemaphoreType.DMA
    return pl.pallas_call(
        exchange_kernel,
        name='exchange',
        out_shape=(jax.ShapeDtypeStruct((2, 128, HID), BF16),
                   jax.ShapeDtypeStruct((HID, 128), BF16),
                   jax.ShapeDtypeStruct((1024, 128), BF16),
                   jax.ShapeDtypeStruct((128, 1024), BF16),
                   jax.ShapeDtypeStruct((2, 64, 1024), F32),
                   jax.ShapeDtypeStruct((2, 64, 1024), F32),
                   jax.ShapeDtypeStruct((2, 64, 1024), BF16)),
        in_specs=[vmem, vmem, hbm, hbm, hbm],
        out_specs=(hbm,) * 7,
        scratch_shapes=[
            pltpu.VMEM((1024, HID), BF16), pltpu.VMEM((1024, HID), BF16), pltpu.VMEM((HID, 1024), BF16),
            pltpu.VMEM((3, 128, HID), F32), pltpu.VMEM((3, 64, HID), F32), pltpu.VMEM((3, 32, HID), F32),
            pltpu.VMEM((3, 128, HID), BF16), pltpu.VMEM((HID, 128), BF16), pltpu.VMEM((2, 128, 1024), BF16),
            pltpu.VMEM((1024, 128), BF16), pltpu.VMEM((2, 128, 1024), F32),
            dma((3, NCH)), dma((2, 3)), dma((2, 3)),
            dma((NCH,)), dma((NCH,)), dma((NCH,)), dma((NCH,)),
            dma((NCH,)), dma((NCH,)), dma((NCH,)), dma((NCH,)), dma((NCH,)), dma((NCH,)),
            dma((NCH,)), dma((NCH,)), dma((3,)), dma((2,)),
        ],
        compiler_params=pltpu.CompilerParams(collective_id=0, has_side_effects=True, vmem_limit_bytes=VMEM_CAP),
        cost_estimate=pl.CostEstimate(flops=9 * 10**9, bytes_accessed=4 * 10**7, transcendentals=0),
    )(x_rows, dy_rows, gate, up, down)


def finish_kernel(keep_ref, got_ref, kept_cols_ref, y_out, dx_out, ready, landed, send_sem, recv_sem, loc_sem):
    t = lax.axis_index('tp')
    d = lax.axis_index('dp')
    cx, c = d // 2, lax.rem(d, 2)
    barrier = pltpu.get_barrier_semaphore()
    for dt in range(2):
        for dd in range(4):
            if dt or dd:
                pl.semaphore_signal(barrier, inc=1, device_id={'tp': lax.rem(t + dt, 2), 'dp': lax.rem(d + dd, 4)},
                                    device_id_type=MESH)
    total = keep_ref[...] + got_ref[...]
    ready[...] = (kept_cols_ref[...].astype(F32) + total).astype(BF16)
    pl.semaphore_wait(barrier, 7)
    block = pl.ds(pl.multiple_of(1024 * d, 128), 1024)

    def send(ocx, ot):
        chip = cx if ocx == 0 else 1 - cx
        return pltpu.make_async_remote_copy(
            src_ref=ready.at[:, pl.ds(pl.multiple_of(32 * chip, 32), 32), :],
            dst_ref=landed.at[:, :, block],
            send_sem=send_sem.at[2 * ocx + ot], recv_sem=recv_sem.at[d],
            device_id={'tp': t if ot == 0 else 1 - t, 'dp': 2 * chip + t}, device_id_type=MESH)

    def arrive(s):
        return pltpu.make_async_remote_copy(
            src_ref=ready.at[:, pl.ds(0, 32), :], dst_ref=landed.at[:, :, pl.ds(1024 * s, 1024)],
            send_sem=send_sem.at[0], recv_sem=recv_sem.at[s],
            device_id={'tp': 1 - t}, device_id_type=MESH)

    local = c == t
    for ocx, ot in ((1, 1), (1, 0), (0, 1)):
        send(ocx, ot).start()

    @pl.when(jnp.logical_not(local))
    def _():
        send(0, 0).start()

    @pl.when(local)
    def _():
        landed[:, :, block] = ready[:, pl.ds(pl.multiple_of(32 * cx, 32), 32), :]

    for s in range(4):
        @pl.when(jnp.logical_not(jnp.logical_and(local, d == s)))
        def _():
            arrive(s).wait_recv()

    stores = (pltpu.make_async_copy(landed.at[0], y_out, loc_sem.at[0]),
              pltpu.make_async_copy(landed.at[1], dx_out, loc_sem.at[1]))
    for s in stores:
        s.start()
    for ocx, ot in ((1, 1), (1, 0), (0, 1)):
        send(ocx, ot).wait_send()

    @pl.when(jnp.logical_not(local))
    def _():
        send(0, 0).wait_send()

    for s in stores:
        s.wait()


def finish(keep, got, kept_cols):
    vmem = pl.BlockSpec(memory_space=pltpu.VMEM)
    hbm = pl.BlockSpec(memory_space=pl.ANY)
    rows = jax.ShapeDtypeStruct((32, 4096), BF16)
    dma = pltpu.SemaphoreType.DMA
    return pl.pallas_call(
        finish_kernel,
        name='finish',
        out_shape=(rows, rows),
        in_specs=[vmem] * 3,
        out_specs=(hbm, hbm),
        scratch_shapes=[pltpu.VMEM((2, 64, 1024), BF16), pltpu.VMEM((2, 32, 4096), BF16),
                        dma((4,)), dma((4,)), dma((2,))],
        compiler_params=pltpu.CompilerParams(collective_id=1, has_side_effects=True),
        cost_estimate=pl.CostEstimate(flops=10**6, bytes_accessed=2 * 10**6, transcendentals=0),
    )(keep, got, kept_cols)


TILE = 512
TILES = HID // TILE
LAST = HID - TILES * TILE
SLOTS = 6


def stream_tiles(compute, store):
    def step(i, carry):
        slot = lax.rem(i, SLOTS)

        @pl.when(i >= SLOTS)
        def _():
            store(i - SLOTS, slot, TILE).wait()

        compute(i, slot, TILE)
        store(i, slot, TILE).start()
        return carry

    lax.fori_loop(0, TILES, step, 0)
    store(TILES - SLOTS, TILES % SLOTS, TILE).wait()
    compute(TILES, TILES % SLOTS, LAST)
    store(TILES, TILES % SLOTS, LAST).start()


def drain_tiles(store):
    for i in range(TILES - SLOTS + 1, TILES):
        store(i, i % SLOTS, TILE).wait()
    store(TILES, TILES % SLOTS, LAST).wait()


def tile_slice(i, width):
    return pl.ds(pl.multiple_of(i * TILE, 128), width)


def column_job(left, right, ring, out, sem):
    def compute(i, slot, width):
        ring[slot, :, pl.ds(0, width)] = jnp.dot(left[...], right[:, tile_slice(i, width)],
                                                 preferred_element_type=F32)

    def store(i, slot, width):
        return pltpu.make_async_copy(ring.at[slot, :, pl.ds(0, width)], out.at[:, tile_slice(i, width)], sem.at[slot])

    return compute, store


def row_job(left, right, ring, out, sem):
    def compute(i, slot, width):
        ring[slot, pl.ds(0, width), :] = jnp.dot(left[tile_slice(i, width), :], right[...],
                                                 preferred_element_type=F32)

    def store(i, slot, width):
        return pltpu.make_async_copy(ring.at[slot, pl.ds(0, width), :], out.at[tile_slice(i, width), :], sem.at[slot])

    return compute, store


def grads_first_kernel(act_t_hbm, dy_cols_hbm, cols_t_hbm, act_hbm, down_out, gate_out,
                       act_t, dy_cols, cols_t, act, ring_a, ring_b, in_sem, sem_a, sem_b):
    loads = [pltpu.make_async_copy(src, dst, in_sem.at[n]) for n, (src, dst) in enumerate((
        (dy_cols_hbm, dy_cols), (act_t_hbm, act_t), (cols_t_hbm, cols_t), (act_hbm.at[0], act)))]
    for load in loads:
        load.start()
    loads[0].wait()
    loads[1].wait()
    compute, store = row_job(act_t, dy_cols, ring_a, down_out, sem_a)
    stream_tiles(compute, store)
    loads[2].wait()
    loads[3].wait()
    compute_b, store_b = column_job(cols_t, act, ring_b, gate_out, sem_b)
    stream_tiles(compute_b, store_b)
    drain_tiles(store)
    drain_tiles(store_b)


def grads_first(act_t, dy_cols, cols_t, act):
    hbm = pl.BlockSpec(memory_space=pl.ANY)
    dma = pltpu.SemaphoreType.DMA
    return pl.pallas_call(
        grads_first_kernel,
        name='grads_first',
        out_shape=(jax.ShapeDtypeStruct((HID, 1024), F32), jax.ShapeDtypeStruct((1024, HID), F32)),
        in_specs=[hbm] * 4,
        out_specs=(hbm, hbm),
        scratch_shapes=[pltpu.VMEM((HID, 128), BF16), pltpu.VMEM((128, 1024), BF16), pltpu.VMEM((1024, 128), BF16),
                        pltpu.VMEM((128, HID), BF16), pltpu.VMEM((SLOTS, TILE, 1024), F32),
                        pltpu.VMEM((SLOTS, 1024, TILE), F32), dma((4,)), dma((SLOTS,)), dma((SLOTS,))],
        compiler_params=pltpu.CompilerParams(vmem_limit_bytes=VMEM_CAP),
        cost_estimate=pl.CostEstimate(flops=4 * 128 * 1024 * HID, bytes_accessed=8 * 1024 * HID, transcendentals=0),
    )(act_t, dy_cols, cols_t, act)


def grads_last_kernel(cols_t_hbm, act_hbm, y_hbm, dx_hbm, up_out, y_out, dx_out,
                      cols_t, act, rows, ring, in_sem, sem, row_sem):
    loads = [pltpu.make_async_copy(src, dst, in_sem.at[n]) for n, (src, dst) in enumerate((
        (cols_t_hbm, cols_t), (act_hbm.at[1], act), (y_hbm, rows.at[0]), (dx_hbm, rows.at[1])))]
    for load in loads:
        load.start()
    loads[0].wait()
    loads[1].wait()
    compute, store = column_job(cols_t, act, ring, up_out, sem)
    stream_tiles(compute, store)
    loads[2].wait()
    loads[3].wait()
    copies = (pltpu.make_async_copy(rows.at[0], y_out, row_sem.at[0]),
              pltpu.make_async_copy(rows.at[1], dx_out, row_sem.at[1]))
    for copy in copies:
        copy.start()
    drain_tiles(store)
    for copy in copies:
        copy.wait()


def grads_last(cols_t, act, y, dx):
    hbm = pl.BlockSpec(memory_space=pl.ANY)
    dma = pltpu.SemaphoreType.DMA
    rows = jax.ShapeDtypeStruct((32, 4096), BF16)
    return pl.pallas_call(
        grads_last_kernel,
        name='grads_last',
        out_shape=(jax.ShapeDtypeStruct((1024, HID), F32), rows, rows),
        in_specs=[hbm] * 4,
        out_specs=(hbm, hbm, hbm),
        scratch_shapes=[pltpu.VMEM((1024, 128), BF16), pltpu.VMEM((128, HID), BF16), pltpu.VMEM((2, 32, 4096), BF16),
                        pltpu.VMEM((SLOTS, 1024, TILE), F32), dma((4,)), dma((SLOTS,)), dma((2,))],
        compiler_params=pltpu.CompilerParams(vmem_limit_bytes=VMEM_CAP),
        cost_estimate=pl.CostEstimate(flops=2 * 128 * 1024 * HID, bytes_accessed=4 * 1024 * HID, transcendentals=0),
    )(cols_t, act, y, dx)


def solution(mesh):
    def device_pass(x_rows, gate_blk, up_blk, down_blk, dy_rows):
        act, act_t, cols_t, dy_cols, keep, give, kept_cols = exchange(x_rows, dy_rows, gate_blk, up_blk, down_blk)
        got = lax.ppermute(give, 'tp', [(0, 1), (1, 0)])
        dw_down, dw_gate = grads_first(act_t, dy_cols, cols_t, act)
        y_part, dx_part = finish(keep, got, kept_cols)
        dw_up, y_rows, dx_rows = grads_last(cols_t, act, y_part, dx_part)
        return y_rows, dx_rows, dw_gate, dw_up, dw_down

    row_spec = P('dp', None)
    weight_spec = P('dp', 'tp')
    down_spec = P('tp', 'dp')
    return jax.shard_map(device_pass, mesh=mesh,
                         in_specs=(row_spec, weight_spec, weight_spec, down_spec, row_spec),
                         out_specs=(row_spec, row_spec, weight_spec, weight_spec, down_spec),
                         check_vma=False)
```

```python
import jax
import jax.numpy as jnp
from jax import lax
from jax.experimental import pallas as pl
from jax.experimental.pallas import tpu as pltpu
from jax.sharding import PartitionSpec as P

MESH = pl.DeviceIdType.MESH
F32, BF16 = jnp.float32, jnp.bfloat16
VMEM_CAP = 67043328
HID = 5504


def chunks(start, widths):
    out = []
    for w in widths:
        out.append((start, w))
        start += w
    return tuple(out)


AB = chunks(0, (512, 512, 1024, 1024, 1024, 1024, 384))
GG = chunks(0, (1024, 1024, 1024, 1024, 768, 384, 256))
NA, NG = len(AB), len(GG)
NT = 4
TW = 1024 // NT
MW = 512


def aligned(v, m):
    return pl.multiple_of(v, m)


def cols_of(chunk):
    return pl.ds(chunk[0], chunk[1])


def column_tiles(chunk, body, tile=256):
    start, width = chunk
    full = width // tile

    def step(i, carry):
        body(aligned(start + i * tile, 128), tile)
        return carry

    lax.fori_loop(0, full, step, 0)
    if width % tile:
        body(start + full * tile, width % tile)


def dot_nt(a, b):
    return lax.dot_general(a, b, (((1,), (1,)), ((), ())), preferred_element_type=F32)


def dot_nn(a, b):
    return jnp.dot(a, b, preferred_element_type=F32)


class Place:
    def __init__(self):
        self.t = lax.axis_index('tp')
        self.d = lax.axis_index('dp')
        self.cx, self.c = self.d // 2, lax.rem(self.d, 2)
        cx, c = self.cx, self.c
        self.sib = 2 * cx + (1 - c)
        self.opp = 2 * (1 - cx) + c
        self.far = 2 * (1 - cx) + (1 - c)
        self.own_row = aligned(32 * (2 * c + cx), 32)
        self.opp_row = aligned(32 * (2 * c + 1 - cx), 32)
        self.sib_row = aligned(32 * (2 * (1 - c) + cx), 32)
        self.far_row = aligned(32 * (2 * (1 - c) + 1 - cx), 32)
        self.keep = pl.ds(aligned(64 * self.t, 64), 64)
        self.give = pl.ds(aligned(64 * (1 - self.t), 64), 64)

    def enter(self):
        barrier = pltpu.get_barrier_semaphore()
        for dt in range(2):
            for dd in range(4):
                if dt or dd:
                    pl.semaphore_signal(barrier, inc=1, device_id_type=MESH, device_id={
                        'tp': lax.rem(self.t + dt, 2), 'dp': lax.rem(self.d + dd, 4)})
        return barrier


class Gather:
    def __init__(self, at, buf, parts, chunk_list, sems):
        self.at, self.buf, self.parts, self.chunks = at, buf, parts, chunk_list
        self.opp_s, self.opp_r, self.sib_s, self.sib_r, self.fwd_s, self.fwd_r = sems

    def copy(self, k, src_row, dst_row, send, recv, to):
        cs = cols_of(self.chunks[k])
        return pltpu.make_async_remote_copy(
            src_ref=self.buf.at[self.parts, pl.ds(src_row, 32), cs],
            dst_ref=self.buf.at[self.parts, pl.ds(dst_row, 32), cs],
            send_sem=send.at[k], recv_sem=recv.at[k], device_id={'dp': to}, device_id_type=MESH)

    def out_opp(self, k, dst=None):
        at = self.at
        return self.copy(k, at.own_row, at.own_row if dst is None else dst, self.opp_s, self.opp_r, at.opp)

    def out_sib(self, k, dst=None):
        at = self.at
        return self.copy(k, at.own_row, at.own_row if dst is None else dst, self.sib_s, self.sib_r, at.sib)

    def out_fwd(self, k, dst=None):
        at = self.at
        return self.copy(k, at.opp_row, at.opp_row if dst is None else dst, self.fwd_s, self.fwd_r, at.sib)

    def send(self, k):
        self.out_opp(k).start()
        self.out_sib(k).start()

    def forward(self, k):
        self.out_opp(k, self.at.opp_row).wait_recv()
        self.out_fwd(k).start()

    def arrived(self, k):
        self.out_sib(k, self.at.sib_row).wait_recv()
        self.out_fwd(k, self.at.far_row).wait_recv()

    def drain(self):
        for k in range(len(self.chunks)):
            self.out_opp(k).wait_send()
            self.out_sib(k).wait_send()
            self.out_fwd(k).wait_send()


class RowSum:
    def __init__(self, at, acc, kept, got, ready, landed, sems):
        self.at, self.acc, self.kept, self.got, self.ready, self.landed = at, acc, kept, got, ready, landed
        self.sum_s, self.sum_r, self.row_s, self.row_r = sems
        self.local = at.c == at.t

    def tile(self, n):
        return pl.ds(n * TW, TW)

    def swap(self, n):
        at = self.at
        return pltpu.make_async_remote_copy(
            src_ref=self.acc.at[at.give, self.tile(n)], dst_ref=self.got.at[:, self.tile(n)],
            send_sem=self.sum_s.at[n], recv_sem=self.sum_r.at[n], device_id={'tp': 1 - at.t}, device_id_type=MESH)

    def row_copy(self, n, ox, ot):
        at = self.at
        chip = 1 - at.cx if ox else at.cx
        return pltpu.make_async_remote_copy(
            src_ref=self.ready.at[pl.ds(aligned(32 * chip, 32), 32), self.tile(n)],
            dst_ref=self.landed.at[:, pl.ds(aligned(1024 * at.d + n * TW, 128), TW)],
            send_sem=self.row_s.at[n, 2 * ox + ot], recv_sem=self.row_r.at[n, at.d],
            device_id={'tp': 1 - at.t if ot else at.t, 'dp': 2 * chip + at.t}, device_id_type=MESH)

    def row_arrive(self, n, s):
        return pltpu.make_async_remote_copy(
            src_ref=self.ready.at[pl.ds(0, 32), self.tile(n)],
            dst_ref=self.landed.at[:, pl.ds(1024 * s + n * TW, TW)],
            send_sem=self.row_s.at[n, 0], recv_sem=self.row_r.at[n, s],
            device_id={'tp': 1 - self.at.t}, device_id_type=MESH)

    def finish(self, n):
        at, ns = self.at, self.tile(n)
        self.swap(n).wait_recv()
        total = self.acc[at.keep, ns] + self.got[:, ns]
        self.ready[:, ns] = (self.kept[at.keep, ns].astype(F32) + total).astype(BF16)
        for ox, ot in ((1, 1), (1, 0), (0, 1)):
            self.row_copy(n, ox, ot).start()

        @pl.when(jnp.logical_not(self.local))
        def _():
            self.row_copy(n, 0, 0).start()

        @pl.when(self.local)
        def _():
            self.landed[:, pl.ds(aligned(1024 * at.d + n * TW, 128), TW)] = (
                self.ready[pl.ds(aligned(32 * at.cx, 32), 32), ns])

    def collect(self):
        for n in range(NT):
            for s in range(4):
                @pl.when(jnp.logical_not(jnp.logical_and(self.local, self.at.d == s)))
                def _():
                    self.row_arrive(n, s).wait_recv()

    def drain(self):
        for n in range(NT):
            self.swap(n).wait_send()
            for ox, ot in ((1, 1), (1, 0), (0, 1)):
                self.row_copy(n, ox, ot).wait_send()

        @pl.when(jnp.logical_not(self.local))
        def _():
            for n in range(NT):
                self.row_copy(n, 0, 0).wait_send()


def gate_grads(act, slot, own, cs, a, b, g):
    s = jax.nn.sigmoid(a)
    act[slot, own, cs] = (g * b * s * (1.0 + a * (1.0 - s))).astype(BF16)
    act[slot + 1, own, cs] = (g * (a * s)).astype(BF16)


def add_dx(acc, act, slot, wg, wu, cs, fresh):
    @pl.loop(0, 1024 // MW)
    def _(n):
        ns = pl.ds(aligned(n * MW, 128), MW)
        dx = dot_nt(act[slot, :, cs], wg[ns, cs]) + dot_nt(act[slot + 1, :, cs], wu[ns, cs])
        acc[:, ns] = dx if fresh else acc[:, ns] + dx


def front_kernel(x_hbm, dy_hbm, wg_hbm, wu_hbm, wd_hbm,
                 act_out, act_t_out, cols_t_out, dy_cols_out, y_out, dx_out,
                 x_ref, dy_ref, wg, wu, wd, part, from_sib, from_opp, act, act_t, cols, cols_t, y_acc, dx_acc, y_got, y_ready, y_rows,
                 in_sem, gu_sem, d_sem, x_send, x_recv, a1_s, a1_r, a2_s, a2_r, g1_s, g1_r, g2_s, g2_r,
                 h_sems, q_sems, sum_s, sum_r, row_s, row_r, t_sem, q_sem, o_sem, dx_sem):
    at = Place()
    own, opp = pl.ds(at.own_row, 32), pl.ds(at.opp_row, 32)
    sib_half = pl.ds(aligned(64 * (1 - at.c), 64), 64)
    mine, theirs = pl.ds(aligned(32 * at.cx, 32), 32), pl.ds(aligned(32 * (1 - at.cx), 32), 32)

    def gate_up_loads(k):
        cs = cols_of(AB[k])
        return (pltpu.make_async_copy(wg_hbm.at[:, cs], wg.at[:, cs], gu_sem.at[0, k]),
                pltpu.make_async_copy(wu_hbm.at[:, cs], wu.at[:, cs], gu_sem.at[1, k]))

    def down_load(k):
        cs = cols_of(GG[k])
        return pltpu.make_async_copy(wd_hbm.at[cs, :], wd.at[cs, :], d_sem.at[k])

    barrier = at.enter()
    token_loads = (pltpu.make_async_copy(x_hbm, x_ref, in_sem.at[0]),
                   pltpu.make_async_copy(dy_hbm, dy_ref, in_sem.at[1]))
    for load in token_loads:
        load.start()
    for k in range(2):
        for load in gate_up_loads(k):
            load.start()
    pl.semaphore_wait(barrier, 7)

    peers = (at.sib, at.opp, at.far)
    tokens = (x_ref, dy_ref)

    def token_copy(i, q, row):
        return pltpu.make_async_remote_copy(
            src_ref=tokens[i].at[:, pl.ds(aligned(1024 * peers[q], 128), 1024)],
            dst_ref=cols.at[i, pl.ds(row, 32), :],
            send_sem=x_send.at[i, q], recv_sem=x_recv.at[i, q],
            device_id={'dp': peers[q]}, device_id_type=MESH)

    for i in range(2):
        token_loads[i].wait()
        for q in (2, 1, 0):
            token_copy(i, q, at.own_row).start()
    for k in range(2, NA):
        for load in gate_up_loads(k):
            load.start()
    for k in range(NG):
        down_load(k).start()
    for i in range(2):
        cols[i, own, :] = tokens[i][:, pl.ds(aligned(1024 * at.d, 128), 1024)]

    def token_wait(i):
        for q, row in enumerate((at.sib_row, at.opp_row, at.far_row)):
            token_copy(i, q, row).wait_recv()

    def core_copy(parts, chunk, k, send, recv):
        cs = cols_of(chunk)
        return pltpu.make_async_remote_copy(
            src_ref=part.at[parts, sib_half, cs], dst_ref=from_sib.at[parts, :, cs],
            send_sem=send.at[k], recv_sem=recv.at[k], device_id={'dp': at.sib}, device_id_type=MESH)

    def chip_copy(parts, chunk, k, send, recv):
        cs = cols_of(chunk)
        return pltpu.make_async_remote_copy(
            src_ref=part.at[parts, opp, cs], dst_ref=from_opp.at[parts, :, cs],
            send_sem=send.at[k], recv_sem=recv.at[k], device_id={'dp': at.opp}, device_id_type=MESH)

    ab, gg = pl.ds(0, 2), pl.ds(2, 1)

    def a1(k):
        return core_copy(ab, AB[k], k, a1_s, a1_r)

    def a2(k):
        return chip_copy(ab, AB[k], k, a2_s, a2_r)

    def g1(k):
        return core_copy(gg, GG[k], k, g1_s, g1_r)

    def g2(k):
        return chip_copy(gg, GG[k], k, g2_s, g2_r)

    def ab_partials(k):
        for load in gate_up_loads(k):
            load.wait()
        if k == 0:
            token_wait(0)

        def body(col, width):
            cs = pl.ds(col, width)
            part[0, :, cs] = dot_nn(cols[0], wg[:, cs])
            part[1, :, cs] = dot_nn(cols[0], wu[:, cs])

        column_tiles(AB[k], body, 512)
        a1(k).start()

    def ab_sum(k):
        a1(k).wait_recv()

        def add(col, width):
            cs = pl.ds(col, width)
            for i in range(2):
                part[i, opp, cs] += from_sib[i, theirs, cs]

        column_tiles(AB[k], add)
        a2(k).start()

    def g_partials(k):
        down_load(k).wait()
        if k == 0:
            token_wait(1)

        def body(col, width):
            cs = pl.ds(col, width)
            part[2, :, cs] = dot_nt(cols[1], wd[cs, :])

        column_tiles(GG[k], body, 512)
        g1(k).start()

    def g_sum(k):
        g1(k).wait_recv()

        def add(col, width):
            cs = pl.ds(col, width)
            part[2, opp, cs] += from_sib[2, theirs, cs]
            part[2, own, cs] += from_sib[2, mine, cs]

        column_tiles(GG[k], add)

    hg = Gather(at, act, pl.ds(0, 1), AB, [h_sems.at[i] for i in range(6)])
    qg = Gather(at, act, pl.ds(1, 2), GG, [q_sems.at[i] for i in range(6)])

    def hidden(k):
        a2(k).wait_recv()

        def body(col, width):
            cs = pl.ds(col, width)
            a, b = [part[i, own, cs] + from_sib[i, mine, cs] + from_opp[i, :, cs] for i in range(2)]
            part[0, own, cs] = a
            part[1, own, cs] = b
            act[0, own, cs] = (a * jax.nn.sigmoid(a) * b).astype(BF16)

        column_tiles(AB[k], body)
        hg.send(k)

    def act_t_store(k):
        cs = cols_of(AB[k])
        return pltpu.make_async_copy(act_t.at[cs, :], act_t_out.at[cs, :], t_sem.at[k])

    ysum = RowSum(at, y_acc, cols.at[0], y_got, y_ready, y_rows, (sum_s, sum_r, row_s, row_r))

    def outputs(k):
        hg.arrived(k)
        cs = cols_of(AB[k])

        def flip(col, width):
            ts = pl.ds(col, width)
            act_t[ts, :] = act[0, :, ts].T

        column_tiles(AB[k], flip)
        act_t_store(k).start()

        def tile(ns):
            y = dot_nn(act[0, :, cs], wd[cs, ns])
            y_acc[:, ns] = y if k == 0 else y_acc[:, ns] + y

        if k < NA - 1:
            @pl.loop(0, 1024 // MW)
            def _(n):
                tile(pl.ds(aligned(n * MW, 128), MW))
        else:
            for n in range(NT):
                tile(pl.ds(n * TW, TW))
                ysum.swap(n).start()

    def hidden_grads(k):
        g2(k).wait_recv()

        def body(col, width):
            cs = pl.ds(col, width)
            gate_grads(act, 1, own, cs, part[0, own, cs], part[1, own, cs], part[2, own, cs] + from_opp[2, :, cs])

        column_tiles(GG[k], body)
        qg.send(k)

    def act_store(k):
        cs = cols_of(GG[k])
        return pltpu.make_async_copy(act.at[pl.ds(1, 2), :, cs], act_out.at[:, :, cs], q_sem.at[k])

    def dx_part(k):
        qg.arrived(k)
        act_store(k).start()
        add_dx(dx_acc, act, 1, wg, wu, cols_of(GG[k]), k == 0)

    def dx_stores():
        for dt in range(2):
            for dd in range(4):
                row = 32 * (2 * (dd % 2) + dd // 2)
                yield pltpu.make_async_copy(dx_acc.at[pl.ds(row, 32), :], dx_out.at[4 * dt + dd],
                                            dx_sem.at[4 * dt + dd])

    stores = [
        pltpu.make_async_copy(cols.at[1], dy_cols_out, o_sem.at[0]),
        pltpu.make_async_copy(cols_t, cols_t_out, o_sem.at[1]),
        pltpu.make_async_copy(y_rows, y_out, o_sem.at[2]),
    ]

    for k in range(NA):
        ab_partials(k)
        if k >= 1:
            ab_sum(k - 1)
    ab_sum(NA - 1)
    for k in range(NG):
        g_partials(k)
        if k >= 1:
            g_sum(k - 1)
    g_sum(NG - 1)
    stores[0].start()
    for n in range(4):
        cols_t[n * 256:(n + 1) * 256, :] = cols[0, :, n * 256:(n + 1) * 256].T
    stores[1].start()
    for k in range(NA):
        hidden(k)
    for k in range(NG):
        g2(k).start()
    for k in range(NA):
        hg.forward(k)
        if k >= 1:
            outputs(k - 1)
    outputs(NA - 1)
    for k in range(NG):
        hidden_grads(k)
        if k == 2:
            for n in range(NT):
                ysum.finish(n)
    for k in range(NG):
        qg.forward(k)
        if k >= 1:
            dx_part(k - 1)
        if k == 1:
            ysum.collect()
            stores[2].start()
    dx_part(NG - 1)
    for store in dx_stores():
        store.start()
    for i in range(2):
        for q in range(3):
            token_copy(i, q, at.own_row).wait_send()
    for k in range(NA):
        a1(k).wait_send()
        a2(k).wait_send()
        act_t_store(k).wait()
    for k in range(NG):
        g1(k).wait_send()
        g2(k).wait_send()
        act_store(k).wait()
    hg.drain()
    qg.drain()
    ysum.drain()
    for store in stores:
        store.wait()
    for store in dx_stores():
        store.wait()


DMA = pltpu.SemaphoreType.DMA
ANY = pl.BlockSpec(memory_space=pl.ANY)
VMEM = pl.BlockSpec(memory_space=pltpu.VMEM)


def shape(dims, dtype):
    return jax.ShapeDtypeStruct(dims, dtype)


def front(x_rows, dy_rows, gate, up, down):
    return pl.pallas_call(
        front_kernel,
        name='front',
        out_shape=(shape((2, 128, HID), BF16), shape((HID, 128), BF16), shape((1024, 128), BF16),
                   shape((128, 1024), BF16), shape((32, 4096), BF16), shape((8, 32, 1024), F32)),
        in_specs=[ANY] * 5,
        out_specs=(ANY,) * 6,
        scratch_shapes=[
            pltpu.VMEM((32, 4096), BF16), pltpu.VMEM((32, 4096), BF16),
            pltpu.VMEM((1024, HID), BF16), pltpu.VMEM((1024, HID), BF16), pltpu.VMEM((HID, 1024), BF16),
            pltpu.VMEM((3, 128, HID), F32), pltpu.VMEM((3, 64, HID), F32), pltpu.VMEM((3, 32, HID), F32),
            pltpu.VMEM((3, 128, HID), BF16), pltpu.VMEM((HID, 128), BF16), pltpu.VMEM((2, 128, 1024), BF16),
            pltpu.VMEM((1024, 128), BF16), pltpu.VMEM((128, 1024), F32), pltpu.VMEM((128, 1024), F32),
            pltpu.VMEM((64, 1024), F32), pltpu.VMEM((64, 1024), BF16), pltpu.VMEM((32, 4096), BF16),
            DMA((2,)), DMA((2, NA)), DMA((NG,)), DMA((2, 3)), DMA((2, 3)),
            DMA((NA,)), DMA((NA,)), DMA((NA,)), DMA((NA,)),
            DMA((NG,)), DMA((NG,)), DMA((NG,)), DMA((NG,)),
            DMA((6, NA)), DMA((6, NG)), DMA((NT,)), DMA((NT,)), DMA((NT, 4)), DMA((NT, 4)),
            DMA((NA,)), DMA((NG,)), DMA((3,)), DMA((8,)),
        ],
        compiler_params=pltpu.CompilerParams(collective_id=0, has_side_effects=True, vmem_limit_bytes=VMEM_CAP),
        cost_estimate=pl.CostEstimate(flops=9 * 10**9, bytes_accessed=4 * 10**7, transcendentals=0),
    )(x_rows, dy_rows, gate, up, down)


TILE = 512
SLOTS = 6


def stream_tiles(compute, store, width):
    full, last = width // TILE, width % TILE

    def step(i, carry):
        slot = lax.rem(i, SLOTS)

        @pl.when(i >= SLOTS)
        def _():
            store(i - SLOTS, slot, TILE).wait()

        compute(i, slot, TILE)
        store(i, slot, TILE).start()
        return carry

    lax.fori_loop(0, full, step, 0)
    total = full
    if last:
        if full >= SLOTS:
            store(full - SLOTS, full % SLOTS, TILE).wait()
        compute(full, full % SLOTS, last)
        store(full, full % SLOTS, last).start()
        total += 1

    def drain():
        for i in range(max(0, total - SLOTS), total):
            store(i, i % SLOTS, TILE if i < full else last).wait()

    return drain


def column_job(left, right, ring, out, base, sem):
    def compute(i, slot, width):
        cs = pl.ds(aligned(i * TILE, 128), width)
        ring[slot, :, pl.ds(0, width)] = dot_nn(left[...], right[:, cs])

    def store(i, slot, width):
        return pltpu.make_async_copy(ring.at[slot, :, pl.ds(0, width)],
                                     out.at[:, pl.ds(aligned(base + i * TILE, 128), width)], sem.at[slot])

    return compute, store


def row_job(left, right, ring, out, sem):
    def compute(i, slot, width):
        ring[slot, pl.ds(0, width), :] = dot_nn(left[pl.ds(aligned(i * TILE, 128), width), :], right[...])

    def store(i, slot, width):
        return pltpu.make_async_copy(ring.at[slot, pl.ds(0, width), :],
                                     out.at[pl.ds(aligned(i * TILE, 128), width), :], sem.at[slot])

    return compute, store


def grads_first_kernel(act_t_hbm, dy_cols_hbm, cols_t_hbm, act_hbm, down_out, gate_out,
                       act_t, dy_cols, cols_t, act, ring_d, ring_c, in_sem, sem_d, sem_c):
    loads = [pltpu.make_async_copy(src, dst, in_sem.at[n]) for n, (src, dst) in enumerate((
        (dy_cols_hbm, dy_cols), (act_t_hbm, act_t), (cols_t_hbm, cols_t), (act_hbm.at[0], act)))]
    for load in loads:
        load.start()
    loads[0].wait()
    loads[1].wait()
    drain_d = stream_tiles(*row_job(act_t, dy_cols, ring_d, down_out, sem_d), HID)
    loads[2].wait()
    loads[3].wait()
    drain_c = stream_tiles(*column_job(cols_t, act, ring_c, gate_out, 0, sem_c), HID)
    drain_d()
    drain_c()


def grads_first(act_t, dy_cols, cols_t, act):
    return pl.pallas_call(
        grads_first_kernel,
        name='grads_first',
        out_shape=(shape((HID, 1024), F32), shape((1024, HID), F32)),
        in_specs=[ANY] * 4,
        out_specs=(ANY,) * 2,
        scratch_shapes=[pltpu.VMEM((HID, 128), BF16), pltpu.VMEM((128, 1024), BF16), pltpu.VMEM((1024, 128), BF16),
                        pltpu.VMEM((128, HID), BF16),
                        pltpu.VMEM((SLOTS, TILE, 1024), F32), pltpu.VMEM((SLOTS, 1024, TILE), F32),
                        DMA((4,)), DMA((SLOTS,)), DMA((SLOTS,))],
        compiler_params=pltpu.CompilerParams(vmem_limit_bytes=VMEM_CAP),
        cost_estimate=pl.CostEstimate(flops=2 * 10**10, bytes_accessed=5 * 10**7, transcendentals=0),
    )(act_t, dy_cols, cols_t, act)


def grads_last_kernel(cols_t_hbm, act_hbm, y_hbm, dy_hbm, got_hbm, up_out, y_out, dx_out,
                      cols_t, act, y_rows, dy_rows, got, dx_rows, ring, in_sem, sem, row_sem):
    loads = [pltpu.make_async_copy(src, dst, in_sem.at[n]) for n, (src, dst) in enumerate((
        (cols_t_hbm, cols_t), (act_hbm.at[1], act), (y_hbm, y_rows), (dy_hbm, dy_rows), (got_hbm, got)))]
    for load in loads:
        load.start()
    loads[0].wait()
    loads[1].wait()
    drain = stream_tiles(*column_job(cols_t, act, ring, up_out, 0, sem), HID)
    for load in loads[2:]:
        load.wait()
    copies = (pltpu.make_async_copy(y_rows, y_out, row_sem.at[0]), pltpu.make_async_copy(dx_rows, dx_out, row_sem.at[1]))
    copies[0].start()
    for d in range(4):
        cs = pl.ds(1024 * d, 1024)
        dx_rows[:, cs] = (dy_rows[:, cs].astype(F32) + (got[d] + got[4 + d])).astype(BF16)
    copies[1].start()
    drain()
    for copy in copies:
        copy.wait()


def grads_last(cols_t, act, y, dy, got):
    return pl.pallas_call(
        grads_last_kernel,
        name='grads_last',
        out_shape=(shape((1024, HID), F32), shape((32, 4096), BF16), shape((32, 4096), BF16)),
        in_specs=[ANY] * 5,
        out_specs=(ANY,) * 3,
        scratch_shapes=[pltpu.VMEM((1024, 128), BF16), pltpu.VMEM((128, HID), BF16), pltpu.VMEM((32, 4096), BF16),
                        pltpu.VMEM((32, 4096), BF16), pltpu.VMEM((8, 32, 1024), F32), pltpu.VMEM((32, 4096), BF16),
                        pltpu.VMEM((SLOTS, 1024, TILE), F32), DMA((5,)), DMA((SLOTS,)), DMA((2,))],
        compiler_params=pltpu.CompilerParams(vmem_limit_bytes=VMEM_CAP),
        cost_estimate=pl.CostEstimate(flops=10**10, bytes_accessed=3 * 10**7, transcendentals=0),
    )(cols_t, act, y, dy, got)


def solution(mesh):
    def device_pass(x_rows, gate_blk, up_blk, down_blk, dy_rows):
        act, act_t, cols_t, dy_cols, y_part, dx_part = front(x_rows, dy_rows, gate_blk, up_blk, down_blk)
        got = lax.all_to_all(dx_part, ('tp', 'dp'), 0, 0, tiled=True)
        dw_down, dw_gate = grads_first(act_t, dy_cols, cols_t, act)
        dw_up, y_rows, dx_rows = grads_last(cols_t, act, y_part, dy_rows, got)
        return y_rows, dx_rows, dw_gate, dw_up, dw_down

    row_spec = P('dp', None)
    weight_spec = P('dp', 'tp')
    down_spec = P('tp', 'dp')
    return jax.shard_map(device_pass, mesh=mesh,
                         in_specs=(row_spec, weight_spec, weight_spec, down_spec, row_spec),
                         out_specs=(row_spec, row_spec, weight_spec, weight_spec, down_spec),
                         check_vma=False)
```

```python
import jax
import jax.numpy as jnp
from jax import lax
from jax.experimental import pallas as pl
from jax.experimental.pallas import tpu as pltpu
from jax.sharding import PartitionSpec as P

MESH = pl.DeviceIdType.MESH
F32, BF16 = jnp.float32, jnp.bfloat16
VMEM_CAP = 67043328
HID = 5504


def chunks(start, widths):
    out = []
    for w in widths:
        out.append((start, w))
        start += w
    return tuple(out)


AB = chunks(0, (256, 256, 512, 1024, 1024, 1024, 1024, 384))
GG = chunks(0, (1024, 1024, 1024, 1024, 768, 512, 128))
NA, NG = len(AB), len(GG)
NT = 4
TW = 1024 // NT
MW = 512


def aligned(v, m):
    return pl.multiple_of(v, m)


def cols_of(chunk):
    return pl.ds(chunk[0], chunk[1])


def column_tiles(chunk, body, tile=256):
    start, width = chunk
    full = width // tile

    def step(i, carry):
        body(aligned(start + i * tile, 128), tile)
        return carry

    lax.fori_loop(0, full, step, 0)
    if width % tile:
        body(start + full * tile, width % tile)


def dot_nt(a, b):
    return lax.dot_general(a, b, (((1,), (1,)), ((), ())), preferred_element_type=F32)


def dot_nn(a, b):
    return jnp.dot(a, b, preferred_element_type=F32)


class Place:
    def __init__(self):
        self.t = lax.axis_index('tp')
        self.d = lax.axis_index('dp')
        self.cx, self.c = self.d // 2, lax.rem(self.d, 2)
        cx, c = self.cx, self.c
        self.sib = 2 * cx + (1 - c)
        self.opp = 2 * (1 - cx) + c
        self.far = 2 * (1 - cx) + (1 - c)
        self.own_row = aligned(32 * (2 * c + cx), 32)
        self.opp_row = aligned(32 * (2 * c + 1 - cx), 32)
        self.sib_row = aligned(32 * (2 * (1 - c) + cx), 32)
        self.far_row = aligned(32 * (2 * (1 - c) + 1 - cx), 32)
        self.keep = pl.ds(aligned(64 * self.t, 64), 64)
        self.give = pl.ds(aligned(64 * (1 - self.t), 64), 64)

    def enter(self):
        barrier = pltpu.get_barrier_semaphore()
        for dt in range(2):
            for dd in range(4):
                if dt or dd:
                    pl.semaphore_signal(barrier, inc=1, device_id_type=MESH, device_id={
                        'tp': lax.rem(self.t + dt, 2), 'dp': lax.rem(self.d + dd, 4)})
        return barrier


class Gather:
    def __init__(self, at, buf, parts, chunk_list, sems):
        self.at, self.buf, self.parts, self.chunks = at, buf, parts, chunk_list
        self.opp_s, self.opp_r, self.sib_s, self.sib_r, self.fwd_s, self.fwd_r = sems

    def copy(self, k, src_row, dst_row, send, recv, to):
        cs = cols_of(self.chunks[k])
        return pltpu.make_async_remote_copy(
            src_ref=self.buf.at[self.parts, pl.ds(src_row, 32), cs],
            dst_ref=self.buf.at[self.parts, pl.ds(dst_row, 32), cs],
            send_sem=send.at[k], recv_sem=recv.at[k], device_id={'dp': to}, device_id_type=MESH)

    def out_opp(self, k, dst=None):
        at = self.at
        return self.copy(k, at.own_row, at.own_row if dst is None else dst, self.opp_s, self.opp_r, at.opp)

    def out_sib(self, k, dst=None):
        at = self.at
        return self.copy(k, at.own_row, at.own_row if dst is None else dst, self.sib_s, self.sib_r, at.sib)

    def out_fwd(self, k, dst=None):
        at = self.at
        return self.copy(k, at.opp_row, at.opp_row if dst is None else dst, self.fwd_s, self.fwd_r, at.sib)

    def send(self, k):
        self.out_opp(k).start()
        self.out_sib(k).start()

    def forward(self, k):
        self.out_opp(k, self.at.opp_row).wait_recv()
        self.out_fwd(k).start()

    def arrived(self, k):
        self.out_sib(k, self.at.sib_row).wait_recv()
        self.out_fwd(k, self.at.far_row).wait_recv()

    def drain(self):
        for k in range(len(self.chunks)):
            self.out_opp(k).wait_send()
            self.out_sib(k).wait_send()
            self.out_fwd(k).wait_send()


class RowSum:
    def __init__(self, at, acc, kept, got, ready, landed, sems):
        self.at, self.acc, self.kept, self.got, self.ready, self.landed = at, acc, kept, got, ready, landed
        self.sum_s, self.sum_r, self.row_s, self.row_r = sems
        self.local = at.c == at.t

    def tile(self, n):
        return pl.ds(n * TW, TW)

    def swap(self, n):
        at = self.at
        return pltpu.make_async_remote_copy(
            src_ref=self.acc.at[at.give, self.tile(n)], dst_ref=self.got.at[:, self.tile(n)],
            send_sem=self.sum_s.at[n], recv_sem=self.sum_r.at[n], device_id={'tp': 1 - at.t}, device_id_type=MESH)

    def row_copy(self, n, ox, ot):
        at = self.at
        chip = 1 - at.cx if ox else at.cx
        return pltpu.make_async_remote_copy(
            src_ref=self.ready.at[pl.ds(aligned(32 * chip, 32), 32), self.tile(n)],
            dst_ref=self.landed.at[:, pl.ds(aligned(1024 * at.d + n * TW, 128), TW)],
            send_sem=self.row_s.at[n, 2 * ox + ot], recv_sem=self.row_r.at[n, at.d],
            device_id={'tp': 1 - at.t if ot else at.t, 'dp': 2 * chip + at.t}, device_id_type=MESH)

    def own_copy(self, n):
        at = self.at
        return pltpu.make_async_copy(
            self.ready.at[pl.ds(aligned(32 * at.cx, 32), 32), self.tile(n)],
            self.landed.at[:, pl.ds(aligned(1024 * at.d + n * TW, 128), TW)], self.row_r.at[n, at.d])

    def row_arrive(self, n, s):
        return pltpu.make_async_remote_copy(
            src_ref=self.ready.at[pl.ds(0, 32), self.tile(n)],
            dst_ref=self.landed.at[:, pl.ds(1024 * s + n * TW, TW)],
            send_sem=self.row_s.at[n, 0], recv_sem=self.row_r.at[n, s],
            device_id={'tp': 1 - self.at.t}, device_id_type=MESH)

    def finish(self, n):
        at, ns = self.at, self.tile(n)
        self.swap(n).wait_recv()
        total = self.acc[at.keep, ns] + self.got[:, ns]
        self.ready[:, ns] = (self.kept[at.keep, ns].astype(F32) + total).astype(BF16)
        for ox, ot in ((1, 1), (1, 0), (0, 1)):
            self.row_copy(n, ox, ot).start()

        @pl.when(jnp.logical_not(self.local))
        def _():
            self.row_copy(n, 0, 0).start()

        @pl.when(self.local)
        def _():
            self.own_copy(n).start()

    def collect(self):
        for n in range(NT):
            for s in range(4):
                @pl.when(jnp.logical_not(jnp.logical_and(self.local, self.at.d == s)))
                def _():
                    self.row_arrive(n, s).wait_recv()

            @pl.when(self.local)
            def _():
                self.own_copy(n).wait()

    def drain(self):
        for n in range(NT):
            self.swap(n).wait_send()
            for ox, ot in ((1, 1), (1, 0), (0, 1)):
                self.row_copy(n, ox, ot).wait_send()

        @pl.when(jnp.logical_not(self.local))
        def _():
            for n in range(NT):
                self.row_copy(n, 0, 0).wait_send()


def gate_grads(act, slot, own, cs, a, b, g):
    s = jax.nn.sigmoid(a)
    act[slot, own, cs] = (g * b * s * (1.0 + a * (1.0 - s))).astype(BF16)
    act[slot + 1, own, cs] = (g * (a * s)).astype(BF16)


def add_dx(acc, act, slot, wg, wu, cs, fresh):
    @pl.loop(0, 1024 // MW)
    def _(n):
        ns = pl.ds(aligned(n * MW, 128), MW)
        dx = dot_nt(act[slot, :, cs], wg[ns, cs]) + dot_nt(act[slot + 1, :, cs], wu[ns, cs])
        acc[:, ns] = dx if fresh else acc[:, ns] + dx


def front_kernel(x_hbm, dy_hbm, wg_hbm, wu_hbm, wd_hbm,
                 act_out, act_t_out, cols_t_out, dy_cols_out, y_out, dx_out,
                 x_ref, dy_ref, wg, wu, wd, part, from_sib, from_opp, act, act_t, cols, cols_t, y_acc, dx_acc, y_got, y_ready,
                 in_sem, gu_sem, d_sem, x_send, x_recv, a1_s, a1_r, a2_s, a2_r, g1_s, g1_r, g2_s, g2_r,
                 h_sems, q_sems, sum_s, sum_r, row_s, row_r, t_sem, q_sem, o_sem, dx_sem):
    at = Place()
    own, opp = pl.ds(at.own_row, 32), pl.ds(at.opp_row, 32)
    sib_half = pl.ds(aligned(64 * (1 - at.c), 64), 64)
    mine, theirs = pl.ds(aligned(32 * at.cx, 32), 32), pl.ds(aligned(32 * (1 - at.cx), 32), 32)

    def gate_up_loads(k):
        cs = cols_of(AB[k])
        return (pltpu.make_async_copy(wg_hbm.at[:, cs], wg.at[:, cs], gu_sem.at[0, k]),
                pltpu.make_async_copy(wu_hbm.at[:, cs], wu.at[:, cs], gu_sem.at[1, k]))

    def down_load(k):
        cs = cols_of(GG[k])
        return pltpu.make_async_copy(wd_hbm.at[cs, :], wd.at[cs, :], d_sem.at[k])

    barrier = at.enter()
    token_loads = (pltpu.make_async_copy(x_hbm, x_ref, in_sem.at[0]),
                   pltpu.make_async_copy(dy_hbm, dy_ref, in_sem.at[1]))
    for load in token_loads:
        load.start()
    for k in range(2):
        for load in gate_up_loads(k):
            load.start()
    pl.semaphore_wait(barrier, 7)

    peers = (at.sib, at.opp, at.far)
    tokens = (x_ref, dy_ref)

    def token_copy(i, q, row):
        return pltpu.make_async_remote_copy(
            src_ref=tokens[i].at[:, pl.ds(aligned(1024 * peers[q], 128), 1024)],
            dst_ref=cols.at[i, pl.ds(row, 32), :],
            send_sem=x_send.at[i, q], recv_sem=x_recv.at[i, q],
            device_id={'dp': peers[q]}, device_id_type=MESH)

    for i in range(2):
        token_loads[i].wait()
        for q in (2, 1, 0):
            token_copy(i, q, at.own_row).start()
    for k in range(2, NA):
        for load in gate_up_loads(k):
            load.start()
    for k in range(NG):
        down_load(k).start()
    for i in range(2):
        cols[i, own, :] = tokens[i][:, pl.ds(aligned(1024 * at.d, 128), 1024)]

    def token_wait(i):
        for q, row in enumerate((at.sib_row, at.opp_row, at.far_row)):
            token_copy(i, q, row).wait_recv()

    def core_copy(parts, chunk, k, send, recv):
        cs = cols_of(chunk)
        return pltpu.make_async_remote_copy(
            src_ref=part.at[parts, sib_half, cs], dst_ref=from_sib.at[parts, :, cs],
            send_sem=send.at[k], recv_sem=recv.at[k], device_id={'dp': at.sib}, device_id_type=MESH)

    def chip_copy(parts, chunk, k, send, recv):
        cs = cols_of(chunk)
        return pltpu.make_async_remote_copy(
            src_ref=part.at[parts, opp, cs], dst_ref=from_opp.at[parts, :, cs],
            send_sem=send.at[k], recv_sem=recv.at[k], device_id={'dp': at.opp}, device_id_type=MESH)

    ab, gg = pl.ds(0, 2), pl.ds(2, 1)

    def a1(k):
        return core_copy(ab, AB[k], k, a1_s, a1_r)

    def a2(k):
        return chip_copy(ab, AB[k], k, a2_s, a2_r)

    def g1(k):
        return core_copy(gg, GG[k], k, g1_s, g1_r)

    def g2(k):
        return chip_copy(gg, GG[k], k, g2_s, g2_r)

    def ab_partials(k):
        for load in gate_up_loads(k):
            load.wait()
        if k == 0:
            token_wait(0)

        def body(col, width):
            cs = pl.ds(col, width)
            part[0, :, cs] = dot_nn(cols[0], wg[:, cs])
            part[1, :, cs] = dot_nn(cols[0], wu[:, cs])

        column_tiles(AB[k], body, 512)
        a1(k).start()

    def ab_sum(k):
        a1(k).wait_recv()

        def add(col, width):
            cs = pl.ds(col, width)
            for i in range(2):
                part[i, opp, cs] += from_sib[i, theirs, cs]

        column_tiles(AB[k], add)
        a2(k).start()

    def g_partials(k):
        down_load(k).wait()
        if k == 0:
            token_wait(1)

        def body(col, width):
            cs = pl.ds(col, width)
            part[2, :, cs] = dot_nt(cols[1], wd[cs, :])

        column_tiles(GG[k], body, 512)
        g1(k).start()

    def g_sum(k):
        g1(k).wait_recv()

        def add(col, width):
            cs = pl.ds(col, width)
            part[2, opp, cs] += from_sib[2, theirs, cs]
            part[2, own, cs] += from_sib[2, mine, cs]

        column_tiles(GG[k], add)

    hg = Gather(at, act, pl.ds(0, 1), AB, [h_sems.at[i] for i in range(6)])
    qg = Gather(at, act, pl.ds(1, 2), GG, [q_sems.at[i] for i in range(6)])

    def hidden(k):
        a2(k).wait_recv()

        def body(col, width):
            cs = pl.ds(col, width)
            a, b = [part[i, own, cs] + from_sib[i, mine, cs] + from_opp[i, :, cs] for i in range(2)]
            part[0, own, cs] = a
            part[1, own, cs] = b
            act[0, own, cs] = (a * jax.nn.sigmoid(a) * b).astype(BF16)

        column_tiles(AB[k], body)
        hg.send(k)

    def act_t_store(k):
        cs = cols_of(AB[k])
        return pltpu.make_async_copy(act_t.at[cs, :], act_t_out.at[cs, :], t_sem.at[k])

    ysum = RowSum(at, y_acc, cols.at[0], y_got, y_ready, y_out, (sum_s, sum_r, row_s, row_r))

    def outputs(k):
        hg.arrived(k)
        cs = cols_of(AB[k])

        def flip(col, width):
            ts = pl.ds(col, width)
            act_t[ts, :] = act[0, :, ts].T

        column_tiles(AB[k], flip)
        act_t_store(k).start()

        def tile(ns):
            y = dot_nn(act[0, :, cs], wd[cs, ns])
            y_acc[:, ns] = y if k == 0 else y_acc[:, ns] + y

        if k < NA - 1:
            @pl.loop(0, 1024 // MW)
            def _(n):
                tile(pl.ds(aligned(n * MW, 128), MW))
        else:
            for n in range(NT):
                tile(pl.ds(n * TW, TW))
                ysum.swap(n).start()

    def hidden_grads(k):
        g2(k).wait_recv()

        def body(col, width):
            cs = pl.ds(col, width)
            gate_grads(act, 1, own, cs, part[0, own, cs], part[1, own, cs], part[2, own, cs] + from_opp[2, :, cs])

        column_tiles(GG[k], body)
        qg.send(k)

    def act_store(k):
        cs = cols_of(GG[k])
        return pltpu.make_async_copy(act.at[pl.ds(1, 2), :, cs], act_out.at[:, :, cs], q_sem.at[k])

    def dx_part(k):
        qg.arrived(k)
        act_store(k).start()
        add_dx(dx_acc, act, 1, wg, wu, cols_of(GG[k]), k == 0)

    def dx_stores():
        for dt in range(2):
            for dd in range(4):
                row = 32 * (2 * (dd % 2) + dd // 2)
                yield pltpu.make_async_copy(dx_acc.at[pl.ds(row, 32), :], dx_out.at[4 * dt + dd],
                                            dx_sem.at[4 * dt + dd])

    stores = [
        pltpu.make_async_copy(cols.at[1], dy_cols_out, o_sem.at[0]),
        pltpu.make_async_copy(cols_t, cols_t_out, o_sem.at[1]),
    ]

    for k in range(NA):
        ab_partials(k)
        if k >= 1:
            ab_sum(k - 1)
    ab_sum(NA - 1)
    for k in range(NG):
        g_partials(k)
        if k >= 1:
            g_sum(k - 1)
    g_sum(NG - 1)
    stores[0].start()
    for n in range(4):
        cols_t[n * 256:(n + 1) * 256, :] = cols[0, :, n * 256:(n + 1) * 256].T
    stores[1].start()
    for k in range(NA):
        hidden(k)
    for k in range(NG):
        g2(k).start()
    for k in range(NA):
        hg.forward(k)
        if k >= 1:
            outputs(k - 1)
    outputs(NA - 1)
    for k in range(NG):
        hidden_grads(k)
    for n in range(NT):
        ysum.finish(n)
    for k in range(NG):
        qg.forward(k)
        if k >= 1:
            dx_part(k - 1)
    dx_part(NG - 1)
    for store in dx_stores():
        store.start()
    ysum.collect()
    for i in range(2):
        for q in range(3):
            token_copy(i, q, at.own_row).wait_send()
    for k in range(NA):
        a1(k).wait_send()
        a2(k).wait_send()
        act_t_store(k).wait()
    for k in range(NG):
        g1(k).wait_send()
        g2(k).wait_send()
        act_store(k).wait()
    hg.drain()
    qg.drain()
    ysum.drain()
    for store in stores:
        store.wait()
    for store in dx_stores():
        store.wait()


DMA = pltpu.SemaphoreType.DMA
ANY = pl.BlockSpec(memory_space=pl.ANY)
VMEM = pl.BlockSpec(memory_space=pltpu.VMEM)


def shape(dims, dtype):
    return jax.ShapeDtypeStruct(dims, dtype)


def front(x_rows, dy_rows, gate, up, down):
    return pl.pallas_call(
        front_kernel,
        name='front',
        out_shape=(shape((2, 128, HID), BF16), shape((HID, 128), BF16), shape((1024, 128), BF16),
                   shape((128, 1024), BF16), shape((32, 4096), BF16), shape((8, 32, 1024), F32)),
        in_specs=[ANY] * 5,
        out_specs=(ANY,) * 6,
        scratch_shapes=[
            pltpu.VMEM((32, 4096), BF16), pltpu.VMEM((32, 4096), BF16),
            pltpu.VMEM((1024, HID), BF16), pltpu.VMEM((1024, HID), BF16), pltpu.VMEM((HID, 1024), BF16),
            pltpu.VMEM((3, 128, HID), F32), pltpu.VMEM((3, 64, HID), F32), pltpu.VMEM((3, 32, HID), F32),
            pltpu.VMEM((3, 128, HID), BF16), pltpu.VMEM((HID, 128), BF16), pltpu.VMEM((2, 128, 1024), BF16),
            pltpu.VMEM((1024, 128), BF16), pltpu.VMEM((128, 1024), F32), pltpu.VMEM((128, 1024), F32),
            pltpu.VMEM((64, 1024), F32), pltpu.VMEM((64, 1024), BF16),
            DMA((2,)), DMA((2, NA)), DMA((NG,)), DMA((2, 3)), DMA((2, 3)),
            DMA((NA,)), DMA((NA,)), DMA((NA,)), DMA((NA,)),
            DMA((NG,)), DMA((NG,)), DMA((NG,)), DMA((NG,)),
            DMA((6, NA)), DMA((6, NG)), DMA((NT,)), DMA((NT,)), DMA((NT, 4)), DMA((NT, 4)),
            DMA((NA,)), DMA((NG,)), DMA((2,)), DMA((8,)),
        ],
        compiler_params=pltpu.CompilerParams(collective_id=0, has_side_effects=True, vmem_limit_bytes=VMEM_CAP),
        cost_estimate=pl.CostEstimate(flops=9 * 10**9, bytes_accessed=4 * 10**7, transcendentals=0),
    )(x_rows, dy_rows, gate, up, down)


TILE = 512
SLOTS = 6


def stream_tiles(compute, store, width, rest):
    full, last = width // TILE, width % TILE
    compute(0, 0, TILE)
    store(0, 0, TILE).start()
    rest()

    def step(i, carry):
        slot = lax.rem(i, SLOTS)

        @pl.when(i >= SLOTS)
        def _():
            store(i - SLOTS, slot, TILE).wait()

        compute(i, slot, TILE)
        store(i, slot, TILE).start()
        return carry

    lax.fori_loop(1, full, step, 0)
    total = full
    if last:
        if full >= SLOTS:
            store(full - SLOTS, full % SLOTS, TILE).wait()
        compute(full, full % SLOTS, last)
        store(full, full % SLOTS, last).start()
        total += 1

    def drain():
        for i in range(max(0, total - SLOTS), total):
            store(i, i % SLOTS, TILE if i < full else last).wait()

    return drain


def load_all(pairs, sem):
    loads = [pltpu.make_async_copy(src, dst, sem.at[n]) for n, (src, dst) in enumerate(pairs)]
    for load in loads:
        load.start()

    def wait(*which):
        for n in which:
            loads[n].wait()

    return wait


def column_job(left, right, ring, out, base, sem):
    def compute(i, slot, width):
        cs = pl.ds(aligned(i * TILE, 128), width)
        ring[slot, :, pl.ds(0, width)] = dot_nn(left[...], right[:, cs])

    def store(i, slot, width):
        return pltpu.make_async_copy(ring.at[slot, :, pl.ds(0, width)],
                                     out.at[:, pl.ds(aligned(base + i * TILE, 128), width)], sem.at[slot])

    return compute, store


def row_job(left, right, ring, out, sem):
    def compute(i, slot, width):
        ring[slot, pl.ds(0, width), :] = dot_nn(left[pl.ds(aligned(i * TILE, 128), width), :], right[...])

    def store(i, slot, width):
        return pltpu.make_async_copy(ring.at[slot, pl.ds(0, width), :],
                                     out.at[pl.ds(aligned(i * TILE, 128), width), :], sem.at[slot])

    return compute, store


def grads_first_kernel(act_t_hbm, dy_cols_hbm, cols_t_hbm, act_hbm, down_out, gate_out,
                       act_t, dy_cols, cols_t, act, ring_d, ring_c, in_sem, sem_d, sem_c):
    head, tail = pl.ds(0, TILE), pl.ds(TILE, HID - TILE)
    wait = load_all(((dy_cols_hbm, dy_cols), (act_t_hbm.at[head, :], act_t.at[head, :]),
                     (act_t_hbm.at[tail, :], act_t.at[tail, :]), (cols_t_hbm, cols_t), (act_hbm.at[0], act)), in_sem)
    wait(0, 1)
    drain_d = stream_tiles(*row_job(act_t, dy_cols, ring_d, down_out, sem_d), HID, lambda: wait(2, 3, 4))
    drain_c = stream_tiles(*column_job(cols_t, act, ring_c, gate_out, 0, sem_c), HID, lambda: None)
    drain_d()
    drain_c()


def grads_first(act_t, dy_cols, cols_t, act):
    return pl.pallas_call(
        grads_first_kernel,
        name='grads_first',
        out_shape=(shape((HID, 1024), F32), shape((1024, HID), F32)),
        in_specs=[ANY] * 4,
        out_specs=(ANY,) * 2,
        scratch_shapes=[pltpu.VMEM((HID, 128), BF16), pltpu.VMEM((128, 1024), BF16), pltpu.VMEM((1024, 128), BF16),
                        pltpu.VMEM((128, HID), BF16),
                        pltpu.VMEM((SLOTS, TILE, 1024), F32), pltpu.VMEM((SLOTS, 1024, TILE), F32),
                        DMA((5,)), DMA((SLOTS,)), DMA((SLOTS,))],
        compiler_params=pltpu.CompilerParams(vmem_limit_bytes=VMEM_CAP),
        cost_estimate=pl.CostEstimate(flops=2 * 10**10, bytes_accessed=5 * 10**7, transcendentals=0),
    )(act_t, dy_cols, cols_t, act)


def grads_last_kernel(cols_t_hbm, act_hbm, y_hbm, dy_hbm, got_hbm, up_out, y_out, dx_out,
                      cols_t, act, y_rows, dy_rows, got, dx_rows, ring, in_sem, sem, row_sem):
    head, tail = pl.ds(0, TILE), pl.ds(TILE, HID - TILE)
    wait = load_all(((cols_t_hbm, cols_t), (act_hbm.at[1, :, head], act.at[:, head]),
                     (act_hbm.at[1, :, tail], act.at[:, tail]), (y_hbm, y_rows), (dy_hbm, dy_rows),
                     (got_hbm, got)), in_sem)
    wait(0, 1)
    drain = stream_tiles(*column_job(cols_t, act, ring, up_out, 0, sem), HID, lambda: wait(2))
    wait(3, 4, 5)
    copies = (pltpu.make_async_copy(y_rows, y_out, row_sem.at[0]), pltpu.make_async_copy(dx_rows, dx_out, row_sem.at[1]))
    copies[0].start()
    for d in range(4):
        cs = pl.ds(1024 * d, 1024)
        dx_rows[:, cs] = (dy_rows[:, cs].astype(F32) + (got[d] + got[4 + d])).astype(BF16)
    copies[1].start()
    drain()
    for copy in copies:
        copy.wait()


def grads_last(cols_t, act, y, dy, got):
    return pl.pallas_call(
        grads_last_kernel,
        name='grads_last',
        out_shape=(shape((1024, HID), F32), shape((32, 4096), BF16), shape((32, 4096), BF16)),
        in_specs=[ANY] * 5,
        out_specs=(ANY,) * 3,
        scratch_shapes=[pltpu.VMEM((1024, 128), BF16), pltpu.VMEM((128, HID), BF16), pltpu.VMEM((32, 4096), BF16),
                        pltpu.VMEM((32, 4096), BF16), pltpu.VMEM((8, 32, 1024), F32), pltpu.VMEM((32, 4096), BF16),
                        pltpu.VMEM((SLOTS, 1024, TILE), F32), DMA((6,)), DMA((SLOTS,)), DMA((2,))],
        compiler_params=pltpu.CompilerParams(vmem_limit_bytes=VMEM_CAP),
        cost_estimate=pl.CostEstimate(flops=10**10, bytes_accessed=3 * 10**7, transcendentals=0),
    )(cols_t, act, y, dy, got)


def solution(mesh):
    def device_pass(x_rows, gate_blk, up_blk, down_blk, dy_rows):
        act, act_t, cols_t, dy_cols, y_part, dx_part = front(x_rows, dy_rows, gate_blk, up_blk, down_blk)
        got = lax.all_to_all(dx_part, ('tp', 'dp'), 0, 0, tiled=True)
        dw_down, dw_gate = grads_first(act_t, dy_cols, cols_t, act)
        dw_up, y_rows, dx_rows = grads_last(cols_t, act, y_part, dy_rows, got)
        return y_rows, dx_rows, dw_gate, dw_up, dw_down

    row_spec = P('dp', None)
    weight_spec = P('dp', 'tp')
    down_spec = P('tp', 'dp')
    return jax.shard_map(device_pass, mesh=mesh,
                         in_specs=(row_spec, weight_spec, weight_spec, down_spec, row_spec),
                         out_specs=(row_spec, row_spec, weight_spec, weight_spec, down_spec),
                         check_vma=False)
```

```python
import jax
import jax.numpy as jnp
from jax import lax
from jax.experimental import pallas as pl
from jax.experimental.pallas import tpu as pltpu
from jax.sharding import PartitionSpec as P

MESH = pl.DeviceIdType.MESH
F32, BF16 = jnp.float32, jnp.bfloat16
VMEM_CAP = 67043328
HID = 5504


def chunks(start, widths):
    out = []
    for w in widths:
        out.append((start, w))
        start += w
    return tuple(out)


AB = chunks(0, (512, 512, 1024, 1024, 1024, 1024, 384))
GG = chunks(0, (512, 1024, 1024, 1024, 1024, 512, 256, 128))
NA, NG = len(AB), len(GG)
NT = 4
TW = 1024 // NT
MW = 512


def aligned(v, m):
    return pl.multiple_of(v, m)


def cols_of(chunk):
    return pl.ds(chunk[0], chunk[1])


def column_tiles(chunk, body, tile=256):
    start, width = chunk
    full = width // tile

    def step(i, carry):
        body(aligned(start + i * tile, 128), tile)
        return carry

    lax.fori_loop(0, full, step, 0)
    if width % tile:
        body(start + full * tile, width % tile)


def dot_nt(a, b):
    return lax.dot_general(a, b, (((1,), (1,)), ((), ())), preferred_element_type=F32)


def dot_nn(a, b):
    return jnp.dot(a, b, preferred_element_type=F32)


class Place:
    def __init__(self):
        self.t = lax.axis_index('tp')
        self.d = lax.axis_index('dp')
        self.cx, self.c = self.d // 2, lax.rem(self.d, 2)
        cx, c = self.cx, self.c
        self.sib = 2 * cx + (1 - c)
        self.opp = 2 * (1 - cx) + c
        self.far = 2 * (1 - cx) + (1 - c)
        self.own_row = aligned(32 * (2 * c + cx), 32)
        self.opp_row = aligned(32 * (2 * c + 1 - cx), 32)
        self.sib_row = aligned(32 * (2 * (1 - c) + cx), 32)
        self.far_row = aligned(32 * (2 * (1 - c) + 1 - cx), 32)
        self.keep = pl.ds(aligned(64 * self.t, 64), 64)
        self.give = pl.ds(aligned(64 * (1 - self.t), 64), 64)

    def rows(self, k):
        if k == 0:
            return self.opp_row, self.own_row, self.far_row, self.sib_row
        return self.own_row, self.opp_row, self.sib_row, self.far_row

    def enter(self):
        barrier = pltpu.get_barrier_semaphore()
        for dt in range(2):
            for dd in range(4):
                if dt or dd:
                    pl.semaphore_signal(barrier, inc=1, device_id_type=MESH, device_id={
                        'tp': lax.rem(self.t + dt, 2), 'dp': lax.rem(self.d + dd, 4)})
        return barrier


class Gather:
    def __init__(self, at, buf, parts, chunk_list, sems):
        self.at, self.buf, self.parts, self.chunks = at, buf, parts, chunk_list
        self.opp_s, self.opp_r, self.sib_s, self.sib_r, self.fwd_s, self.fwd_r = sems

    def copy(self, k, src_row, dst_row, send, recv, to):
        cs = cols_of(self.chunks[k])
        return pltpu.make_async_remote_copy(
            src_ref=self.buf.at[self.parts, pl.ds(src_row, 32), cs],
            dst_ref=self.buf.at[self.parts, pl.ds(dst_row, 32), cs],
            send_sem=send.at[k], recv_sem=recv.at[k], device_id={'dp': to}, device_id_type=MESH)

    def out_opp(self, k, dst=None):
        own = self.at.rows(k)[0]
        return self.copy(k, own, own if dst is None else dst, self.opp_s, self.opp_r, self.at.opp)

    def out_sib(self, k, dst=None):
        own = self.at.rows(k)[0]
        return self.copy(k, own, own if dst is None else dst, self.sib_s, self.sib_r, self.at.sib)

    def out_fwd(self, k, dst=None):
        opp = self.at.rows(k)[1]
        return self.copy(k, opp, opp if dst is None else dst, self.fwd_s, self.fwd_r, self.at.sib)

    def send(self, k):
        self.out_opp(k).start()
        self.out_sib(k).start()

    def forward(self, k):
        self.out_opp(k, self.at.rows(k)[1]).wait_recv()
        self.out_fwd(k).start()

    def arrived(self, k):
        self.out_sib(k, self.at.rows(k)[2]).wait_recv()
        self.out_fwd(k, self.at.rows(k)[3]).wait_recv()

    def drain(self):
        for k in range(len(self.chunks)):
            self.out_opp(k).wait_send()
            self.out_sib(k).wait_send()
            self.out_fwd(k).wait_send()


class RowSum:
    def __init__(self, at, acc, kept, got, ready, landed, sems):
        self.at, self.acc, self.kept, self.got, self.ready, self.landed = at, acc, kept, got, ready, landed
        self.sum_s, self.sum_r, self.row_s, self.row_r = sems
        self.local = at.c == at.t

    def tile(self, n):
        return pl.ds(n * TW, TW)

    def swap(self, n):
        at = self.at
        return pltpu.make_async_remote_copy(
            src_ref=self.acc.at[at.give, self.tile(n)], dst_ref=self.got.at[:, self.tile(n)],
            send_sem=self.sum_s.at[n], recv_sem=self.sum_r.at[n], device_id={'tp': 1 - at.t}, device_id_type=MESH)

    def row_copy(self, n, ox, ot):
        at = self.at
        chip = 1 - at.cx if ox else at.cx
        return pltpu.make_async_remote_copy(
            src_ref=self.ready.at[pl.ds(aligned(32 * chip, 32), 32), self.tile(n)],
            dst_ref=self.landed.at[:, pl.ds(aligned(1024 * at.d + n * TW, 128), TW)],
            send_sem=self.row_s.at[n, 2 * ox + ot], recv_sem=self.row_r.at[n, at.d],
            device_id={'tp': 1 - at.t if ot else at.t, 'dp': 2 * chip + at.t}, device_id_type=MESH)

    def own_copy(self, n):
        at = self.at
        return pltpu.make_async_copy(
            self.ready.at[pl.ds(aligned(32 * at.cx, 32), 32), self.tile(n)],
            self.landed.at[:, pl.ds(aligned(1024 * at.d + n * TW, 128), TW)], self.row_r.at[n, at.d])

    def row_arrive(self, n, s):
        return pltpu.make_async_remote_copy(
            src_ref=self.ready.at[pl.ds(0, 32), self.tile(n)],
            dst_ref=self.landed.at[:, pl.ds(1024 * s + n * TW, TW)],
            send_sem=self.row_s.at[n, 0], recv_sem=self.row_r.at[n, s],
            device_id={'tp': 1 - self.at.t}, device_id_type=MESH)

    def finish(self, n):
        at, ns = self.at, self.tile(n)
        self.swap(n).wait_recv()
        total = self.acc[at.keep, ns] + self.got[:, ns]
        self.ready[:, ns] = (self.kept[at.keep, ns].astype(F32) + total).astype(BF16)
        for ox, ot in ((1, 1), (0, 1)):
            self.row_copy(n, ox, ot).start()

        @pl.when(jnp.logical_not(self.local))
        def _():
            self.row_copy(n, 0, 0).start()

        @pl.when(self.local)
        def _():
            self.own_copy(n).start()

    def collect(self):
        for n in range(NT):
            for s in range(4):
                @pl.when(jnp.logical_not(jnp.logical_and(self.local, self.at.d == s)))
                def _():
                    self.row_arrive(n, s).wait_recv()

            @pl.when(self.local)
            def _():
                self.own_copy(n).wait()

    def drain(self):
        for n in range(NT):
            self.swap(n).wait_send()
            for ox, ot in ((1, 1), (1, 0), (0, 1)):
                self.row_copy(n, ox, ot).wait_send()

        @pl.when(jnp.logical_not(self.local))
        def _():
            for n in range(NT):
                self.row_copy(n, 0, 0).wait_send()


def gate_grads(act, slot, own, cs, a, b, g):
    s = jax.nn.sigmoid(a)
    act[slot, own, cs] = (g * b * s * (1.0 + a * (1.0 - s))).astype(BF16)
    act[slot + 1, own, cs] = (g * (a * s)).astype(BF16)


def front_kernel(x_hbm, dy_hbm, wg_hbm, wu_hbm, wd_hbm,
                 act_out, act_t_out, cols_t_out, dy_cols_out, y_out, dx_out,
                 x_ref, dy_ref, wg, wu, wd, part, from_sib, from_opp, act, act_t, cols, cols_t, y_acc, dx_acc, y_got, y_ready,
                 in_sem, gu_sem, d_sem, x_send, x_recv, a0_s, a0_r, a1_s, a1_r, a2_s, a2_r, g1_s, g1_r, g2_s, g2_r,
                 h_sems, q_sems, sum_s, sum_r, row_s, row_r, t_sem, q_sem, o_sem, dx_sem):
    at = Place()
    own, opp = pl.ds(at.own_row, 32), pl.ds(at.opp_row, 32)
    sib_half = pl.ds(aligned(64 * (1 - at.c), 64), 64)
    mine, theirs = pl.ds(aligned(32 * at.cx, 32), 32), pl.ds(aligned(32 * (1 - at.cx), 32), 32)

    def gate_up_loads(k):
        cs = cols_of(AB[k])
        return (pltpu.make_async_copy(wg_hbm.at[:, cs], wg.at[:, cs], gu_sem.at[0, k]),
                pltpu.make_async_copy(wu_hbm.at[:, cs], wu.at[:, cs], gu_sem.at[1, k]))

    def down_load(k):
        cs = cols_of(GG[k])
        return pltpu.make_async_copy(wd_hbm.at[cs, :], wd.at[cs, :], d_sem.at[k])

    barrier = at.enter()
    token_loads = (pltpu.make_async_copy(x_hbm, x_ref, in_sem.at[0]),
                   pltpu.make_async_copy(dy_hbm, dy_ref, in_sem.at[1]))
    for load in token_loads:
        load.start()
    for k in range(2):
        for load in gate_up_loads(k):
            load.start()
    pl.semaphore_wait(barrier, 7)

    peers = (at.sib, at.opp, at.far)
    tokens = (x_ref, dy_ref)

    def token_copy(i, q, row):
        return pltpu.make_async_remote_copy(
            src_ref=tokens[i].at[:, pl.ds(aligned(1024 * peers[q], 128), 1024)],
            dst_ref=cols.at[i, pl.ds(row, 32), :],
            send_sem=x_send.at[i, q], recv_sem=x_recv.at[i, q],
            device_id={'dp': peers[q]}, device_id_type=MESH)

    for i in range(2):
        token_loads[i].wait()
        for q in (2, 1, 0):
            token_copy(i, q, at.own_row).start()
    for k in range(2, NA):
        for load in gate_up_loads(k):
            load.start()
    for k in range(NG):
        down_load(k).start()
    for i in range(2):
        cols[i, own, :] = tokens[i][:, pl.ds(aligned(1024 * at.d, 128), 1024)]

    def token_wait(i, which=(0, 1, 2)):
        for q in which:
            token_copy(i, q, (at.sib_row, at.opp_row, at.far_row)[q]).wait_recv()

    def core_copy(parts, chunk, k, send, recv):
        cs = cols_of(chunk)
        return pltpu.make_async_remote_copy(
            src_ref=part.at[parts, sib_half, cs], dst_ref=from_sib.at[parts, :, cs],
            send_sem=send.at[k], recv_sem=recv.at[k], device_id={'dp': at.sib}, device_id_type=MESH)

    def chip_copy(parts, chunk, k, send, recv):
        cs = cols_of(chunk)
        return pltpu.make_async_remote_copy(
            src_ref=part.at[parts, pl.ds(at.rows(k)[1], 32), cs], dst_ref=from_opp.at[parts, :, cs],
            send_sem=send.at[k], recv_sem=recv.at[k], device_id={'dp': at.opp}, device_id_type=MESH)

    ab, gg = pl.ds(0, 2), pl.ds(2, 1)

    def a1(k):
        return core_copy(ab, AB[k], k, a1_s, a1_r)

    def a2(k):
        return chip_copy(ab, AB[k], k, a2_s, a2_r)

    def g1(k):
        return core_copy(gg, GG[k], k, g1_s, g1_r)

    def g2(k):
        return chip_copy(gg, GG[k], k, g2_s, g2_r)

    def first_core_copy(which):
        cs = cols_of(AB[0])
        return pltpu.make_async_remote_copy(
            src_ref=part.at[ab, pl.ds((at.sib_row, at.far_row)[which], 32), cs],
            dst_ref=from_sib.at[ab, (mine, theirs)[which], cs],
            send_sem=a0_s.at[which], recv_sem=a0_r.at[which], device_id={'dp': at.sib}, device_id_type=MESH)

    def first_partials(which):
        upper, lower = [pl.ds(row, 32) for row in ((at.own_row, at.sib_row), (at.opp_row, at.far_row))[which]]
        cs = cols_of(AB[0])
        rows = jnp.concatenate([cols[0, upper, :], cols[0, lower, :]], axis=0)
        for i, w in enumerate((wg, wu)):
            out = dot_nn(rows, w[:, cs])
            part[i, upper, cs] = out[:32]
            part[i, lower, cs] = out[32:]
        first_core_copy(which).start()

    def first_chunk():
        for load in gate_up_loads(0):
            load.wait()
        token_wait(0, (0,))
        first_partials(0)
        first_core_copy(0).wait_recv()
        cs = cols_of(AB[0])
        for i in range(2):
            part[i, own, cs] += from_sib[i, mine, cs]
        a2(0).start()
        token_wait(0, (1, 2))
        first_partials(1)

    def ab_partials(k):
        for load in gate_up_loads(k):
            load.wait()

        def body(col, width):
            cs = pl.ds(col, width)
            part[0, :, cs] = dot_nn(cols[0], wg[:, cs])
            part[1, :, cs] = dot_nn(cols[0], wu[:, cs])

        column_tiles(AB[k], body, 512)
        a1(k).start()

    def ab_sum(k):
        a1(k).wait_recv()

        def add(col, width):
            cs = pl.ds(col, width)
            for i in range(2):
                part[i, opp, cs] += from_sib[i, theirs, cs]

        column_tiles(AB[k], add)
        a2(k).start()

    def g_partials(k):
        down_load(k).wait()
        if k == 0:
            token_wait(1)

        def body(col, width):
            cs = pl.ds(col, width)
            part[2, :, cs] = dot_nt(cols[1], wd[cs, :])

        column_tiles(GG[k], body, 512)
        g1(k).start()

    def g_sum(k):
        g1(k).wait_recv()

        def add(col, width):
            cs = pl.ds(col, width)
            part[2, opp, cs] += from_sib[2, theirs, cs]
            part[2, own, cs] += from_sib[2, mine, cs]

        column_tiles(GG[k], add)

    hg = Gather(at, act, pl.ds(0, 1), AB, [h_sems.at[i] for i in range(6)])
    qg = Gather(at, act, pl.ds(1, 2), GG, [q_sems.at[i] for i in range(6)])

    def hidden(k):
        if k == 0:
            first_core_copy(1).wait_recv()
        a2(k).wait_recv()
        here = pl.ds(at.rows(k)[0], 32)
        core = theirs if k == 0 else mine

        def body(col, width):
            cs = pl.ds(col, width)
            a, b = [part[i, here, cs] + from_sib[i, core, cs] + from_opp[i, :, cs] for i in range(2)]
            part[0, here, cs] = a
            part[1, here, cs] = b
            act[0, here, cs] = (a * jax.nn.sigmoid(a) * b).astype(BF16)

        column_tiles(AB[k], body)
        hg.send(k)

    def act_t_store(k):
        cs = cols_of(AB[k])
        return pltpu.make_async_copy(act_t.at[cs, :], act_t_out.at[cs, :], t_sem.at[k])

    ysum = RowSum(at, y_acc, cols.at[0], y_got, y_ready, y_out, (sum_s, sum_r, row_s, row_r))

    def outputs(k):
        hg.arrived(k)
        cs = cols_of(AB[k])

        def flip(col, width):
            ts = pl.ds(col, width)
            act_t[ts, :] = act[0, :, ts].T

        column_tiles(AB[k], flip)
        act_t_store(k).start()

        def tile(ns):
            y = dot_nn(act[0, :, cs], wd[cs, ns])
            y_acc[:, ns] = y if k == 0 else y_acc[:, ns] + y

        if k < NA - 1:
            @pl.loop(0, 1024 // MW)
            def _(n):
                tile(pl.ds(aligned(n * MW, 128), MW))
        else:
            for n in range(NT):
                tile(pl.ds(n * TW, TW))
                ysum.swap(n).start()

    def hidden_grads(k):
        g2(k).wait_recv()
        here = pl.ds(at.rows(k)[0], 32)

        def body(col, width):
            cs = pl.ds(col, width)
            gate_grads(act, 1, here, cs, part[0, here, cs], part[1, here, cs], part[2, here, cs] + from_opp[2, :, cs])

        column_tiles(GG[k], body)
        qg.send(k)

    def act_store(k):
        cs = cols_of(GG[k])
        return pltpu.make_async_copy(act.at[pl.ds(1, 2), :, cs], act_out.at[:, :, cs], q_sem.at[k])

    def dx_part(k, n):
        cs, ns = cols_of(GG[k]), pl.ds(n * MW, MW)
        if n == 0:
            qg.arrived(k)
            act_store(k).start()
        dx = dot_nt(act[1, :, cs], wg[ns, cs]) + dot_nt(act[2, :, cs], wu[ns, cs])
        dx_acc[:, ns] = dx if k == 0 else dx_acc[:, ns] + dx

    def dx_stores(n):
        ns = pl.ds(n * MW, MW)
        for dt in range(2):
            for dd in range(4):
                row = 32 * (2 * (dd % 2) + dd // 2)
                yield pltpu.make_async_copy(dx_acc.at[pl.ds(row, 32), ns], dx_out.at[4 * dt + dd, :, ns],
                                            dx_sem.at[n, 4 * dt + dd])

    stores = [
        pltpu.make_async_copy(cols.at[1], dy_cols_out, o_sem.at[0]),
        pltpu.make_async_copy(cols_t, cols_t_out, o_sem.at[1]),
    ]

    first_chunk()
    for k in range(1, NA):
        ab_partials(k)
        if k >= 2:
            ab_sum(k - 1)
    ab_sum(NA - 1)
    for k in range(NG):
        g_partials(k)
        if k >= 1:
            g_sum(k - 1)
    g_sum(NG - 1)
    stores[0].start()
    for n in range(4):
        cols_t[n * 256:(n + 1) * 256, :] = cols[0, :, n * 256:(n + 1) * 256].T
    stores[1].start()
    for k in range(NA):
        hidden(k)
    for k in range(NG):
        g2(k).start()
    for k in range(NA):
        hg.forward(k)
        if k >= 1:
            outputs(k - 1)
    outputs(NA - 1)
    for k in range(NG):
        hidden_grads(k)
    for n in range(NT):
        ysum.finish(n)
    for n in range(NT):
        ysum.row_copy(n, 1, 0).start()
    for step in ('f0', 'f1', 'd0', 'D0', 'f2', 'd1', 'D1', 'd2', 'f3', 'D2', 'f4', 'd3', 'f5', 'D3', 'f6', 'f7',
                 'd4', 'D4', 'd5', 'D5', 'd6', 'D6', 'd7'):
        k = int(step[1])
        if step[0] == 'f':
            qg.forward(k)
        else:
            dx_part(k, 0 if step[0] == 'd' else 1)
    for n in range(2):
        if n:
            dx_part(NG - 1, n)
        for store in dx_stores(n):
            store.start()
    ysum.collect()
    for i in range(2):
        for q in range(3):
            token_copy(i, q, at.own_row).wait_send()
    for k in range(NA):
        if k == 0:
            first_core_copy(0).wait_send()
            first_core_copy(1).wait_send()
        else:
            a1(k).wait_send()
        a2(k).wait_send()
        act_t_store(k).wait()
    for k in range(NG):
        g1(k).wait_send()
        g2(k).wait_send()
        act_store(k).wait()
    hg.drain()
    qg.drain()
    ysum.drain()
    for store in stores:
        store.wait()
    for n in range(2):
        for store in dx_stores(n):
            store.wait()


DMA = pltpu.SemaphoreType.DMA
ANY = pl.BlockSpec(memory_space=pl.ANY)
VMEM = pl.BlockSpec(memory_space=pltpu.VMEM)


def shape(dims, dtype):
    return jax.ShapeDtypeStruct(dims, dtype)


def front(x_rows, dy_rows, gate, up, down):
    return pl.pallas_call(
        front_kernel,
        name='front',
        out_shape=(shape((2, 128, HID), BF16), shape((HID, 128), BF16), shape((1024, 128), BF16),
                   shape((128, 1024), BF16), shape((32, 4096), BF16), shape((8, 32, 1024), F32)),
        in_specs=[ANY] * 5,
        out_specs=(ANY,) * 6,
        scratch_shapes=[
            pltpu.VMEM((32, 4096), BF16), pltpu.VMEM((32, 4096), BF16),
            pltpu.VMEM((1024, HID), BF16), pltpu.VMEM((1024, HID), BF16), pltpu.VMEM((HID, 1024), BF16),
            pltpu.VMEM((3, 128, HID), F32), pltpu.VMEM((3, 64, HID), F32), pltpu.VMEM((3, 32, HID), F32),
            pltpu.VMEM((3, 128, HID), BF16), pltpu.VMEM((HID, 128), BF16), pltpu.VMEM((2, 128, 1024), BF16),
            pltpu.VMEM((1024, 128), BF16), pltpu.VMEM((128, 1024), F32), pltpu.VMEM((128, 1024), F32),
            pltpu.VMEM((64, 1024), F32), pltpu.VMEM((64, 1024), BF16),
            DMA((2,)), DMA((2, NA)), DMA((NG,)), DMA((2, 3)), DMA((2, 3)),
            DMA((2,)), DMA((2,)), DMA((NA,)), DMA((NA,)), DMA((NA,)), DMA((NA,)),
            DMA((NG,)), DMA((NG,)), DMA((NG,)), DMA((NG,)),
            DMA((6, NA)), DMA((6, NG)), DMA((NT,)), DMA((NT,)), DMA((NT, 4)), DMA((NT, 4)),
            DMA((NA,)), DMA((NG,)), DMA((2,)), DMA((2, 8)),
        ],
        compiler_params=pltpu.CompilerParams(collective_id=0, has_side_effects=True, vmem_limit_bytes=VMEM_CAP),
        cost_estimate=pl.CostEstimate(flops=9 * 10**9, bytes_accessed=4 * 10**7, transcendentals=0),
    )(x_rows, dy_rows, gate, up, down)


TILE = 512
SLOTS = 6


def stream_tiles(compute, store, width, rest):
    full, last = width // TILE, width % TILE
    compute(0, 0, TILE)
    store(0, 0, TILE).start()
    rest()

    def step(i, carry):
        slot = lax.rem(i, SLOTS)

        @pl.when(i >= SLOTS)
        def _():
            store(i - SLOTS, slot, TILE).wait()

        compute(i, slot, TILE)
        store(i, slot, TILE).start()
        return carry

    lax.fori_loop(1, full, step, 0)
    total = full
    if last:
        if full >= SLOTS:
            store(full - SLOTS, full % SLOTS, TILE).wait()
        compute(full, full % SLOTS, last)
        store(full, full % SLOTS, last).start()
        total += 1

    def drain():
        for i in range(max(0, total - SLOTS), total):
            store(i, i % SLOTS, TILE if i < full else last).wait()

    return drain


def load_all(pairs, sem):
    loads = [pltpu.make_async_copy(src, dst, sem.at[n]) for n, (src, dst) in enumerate(pairs)]
    for load in loads:
        load.start()

    def wait(*which):
        for n in which:
            loads[n].wait()

    return wait


def column_job(left, right, ring, out, base, sem):
    def compute(i, slot, width):
        cs = pl.ds(aligned(i * TILE, 128), width)
        ring[slot, :, pl.ds(0, width)] = dot_nn(left[...], right[:, cs])

    def store(i, slot, width):
        return pltpu.make_async_copy(ring.at[slot, :, pl.ds(0, width)],
                                     out.at[:, pl.ds(aligned(base + i * TILE, 128), width)], sem.at[slot])

    return compute, store


def row_job(left, right, ring, out, sem):
    def compute(i, slot, width):
        ring[slot, pl.ds(0, width), :] = dot_nn(left[pl.ds(aligned(i * TILE, 128), width), :], right[...])

    def store(i, slot, width):
        return pltpu.make_async_copy(ring.at[slot, pl.ds(0, width), :],
                                     out.at[pl.ds(aligned(i * TILE, 128), width), :], sem.at[slot])

    return compute, store


def grads_first_kernel(act_t_hbm, dy_cols_hbm, cols_t_hbm, act_hbm, down_out, gate_out,
                       act_t, dy_cols, cols_t, act, ring_d, ring_c, in_sem, sem_d, sem_c):
    head, tail = pl.ds(0, TILE), pl.ds(TILE, HID - TILE)
    wait = load_all(((dy_cols_hbm, dy_cols), (act_t_hbm.at[head, :], act_t.at[head, :]),
                     (act_t_hbm.at[tail, :], act_t.at[tail, :]), (cols_t_hbm, cols_t), (act_hbm.at[0], act)), in_sem)
    wait(0, 1)
    drain_d = stream_tiles(*row_job(act_t, dy_cols, ring_d, down_out, sem_d), HID, lambda: wait(2, 3, 4))
    drain_c = stream_tiles(*column_job(cols_t, act, ring_c, gate_out, 0, sem_c), HID, lambda: None)
    drain_d()
    drain_c()


def grads_first(act_t, dy_cols, cols_t, act):
    return pl.pallas_call(
        grads_first_kernel,
        name='grads_first',
        out_shape=(shape((HID, 1024), F32), shape((1024, HID), F32)),
        in_specs=[ANY] * 4,
        out_specs=(ANY,) * 2,
        scratch_shapes=[pltpu.VMEM((HID, 128), BF16), pltpu.VMEM((128, 1024), BF16), pltpu.VMEM((1024, 128), BF16),
                        pltpu.VMEM((128, HID), BF16),
                        pltpu.VMEM((SLOTS, TILE, 1024), F32), pltpu.VMEM((SLOTS, 1024, TILE), F32),
                        DMA((5,)), DMA((SLOTS,)), DMA((SLOTS,))],
        compiler_params=pltpu.CompilerParams(vmem_limit_bytes=VMEM_CAP),
        cost_estimate=pl.CostEstimate(flops=2 * 10**10, bytes_accessed=5 * 10**7, transcendentals=0),
    )(act_t, dy_cols, cols_t, act)


def grads_last_kernel(cols_t_hbm, act_hbm, y_hbm, dy_hbm, got_hbm, up_out, y_out, dx_out,
                      cols_t, act, y_rows, dy_rows, got, dx_rows, ring, in_sem, sem, row_sem):
    head, tail = pl.ds(0, TILE), pl.ds(TILE, HID - TILE)
    wait = load_all(((cols_t_hbm, cols_t), (act_hbm.at[1, :, head], act.at[:, head]),
                     (act_hbm.at[1, :, tail], act.at[:, tail]), (y_hbm, y_rows), (dy_hbm, dy_rows),
                     (got_hbm, got)), in_sem)
    wait(0, 1)
    drain = stream_tiles(*column_job(cols_t, act, ring, up_out, 0, sem), HID, lambda: wait(2))
    wait(3, 4, 5)
    copies = (pltpu.make_async_copy(y_rows, y_out, row_sem.at[0]), pltpu.make_async_copy(dx_rows, dx_out, row_sem.at[1]))
    copies[0].start()
    for d in range(4):
        cs = pl.ds(1024 * d, 1024)
        dx_rows[:, cs] = (dy_rows[:, cs].astype(F32) + (got[d] + got[4 + d])).astype(BF16)
    copies[1].start()
    drain()
    for copy in copies:
        copy.wait()


def grads_last(cols_t, act, y, dy, got):
    return pl.pallas_call(
        grads_last_kernel,
        name='grads_last',
        out_shape=(shape((1024, HID), F32), shape((32, 4096), BF16), shape((32, 4096), BF16)),
        in_specs=[ANY] * 5,
        out_specs=(ANY,) * 3,
        scratch_shapes=[pltpu.VMEM((1024, 128), BF16), pltpu.VMEM((128, HID), BF16), pltpu.VMEM((32, 4096), BF16),
                        pltpu.VMEM((32, 4096), BF16), pltpu.VMEM((8, 32, 1024), F32), pltpu.VMEM((32, 4096), BF16),
                        pltpu.VMEM((SLOTS, 1024, TILE), F32), DMA((6,)), DMA((SLOTS,)), DMA((2,))],
        compiler_params=pltpu.CompilerParams(vmem_limit_bytes=VMEM_CAP),
        cost_estimate=pl.CostEstimate(flops=10**10, bytes_accessed=3 * 10**7, transcendentals=0),
    )(cols_t, act, y, dy, got)


def solution(mesh):
    def device_pass(x_rows, gate_blk, up_blk, down_blk, dy_rows):
        act, act_t, cols_t, dy_cols, y_part, dx_part = front(x_rows, dy_rows, gate_blk, up_blk, down_blk)
        got = lax.all_to_all(dx_part, ('tp', 'dp'), 0, 0, tiled=True)
        dw_down, dw_gate = grads_first(act_t, dy_cols, cols_t, act)
        dw_up, y_rows, dx_rows = grads_last(cols_t, act, y_part, dy_rows, got)
        return y_rows, dx_rows, dw_gate, dw_up, dw_down

    row_spec = P('dp', None)
    weight_spec = P('dp', 'tp')
    down_spec = P('tp', 'dp')
    return jax.shard_map(device_pass, mesh=mesh,
                         in_specs=(row_spec, weight_spec, weight_spec, down_spec, row_spec),
                         out_specs=(row_spec, row_spec, weight_spec, weight_spec, down_spec),
                         check_vma=False)
```

```python
import jax
import jax.numpy as jnp
from jax import lax
from jax.experimental import pallas as pl
from jax.experimental.pallas import tpu as pltpu
from jax.sharding import PartitionSpec as P

MESH = pl.DeviceIdType.MESH
F32, BF16 = jnp.float32, jnp.bfloat16
VMEM_CAP = 67043328
HID = 5504


def chunks(start, widths):
    out = []
    for w in widths:
        out.append((start, w))
        start += w
    return tuple(out)


AB = chunks(0, (512, 512, 1024, 1024, 1024, 1024, 384))
GG = chunks(0, (512, 1024, 1024, 1024, 1024, 512, 256, 128))
NA, NG = len(AB), len(GG)
NT = 4
TW = 1024 // NT
MW = 512


def aligned(v, m):
    return pl.multiple_of(v, m)


def cols_of(chunk):
    return pl.ds(chunk[0], chunk[1])


def column_tiles(chunk, body, tile=256):
    start, width = chunk
    full = width // tile

    def step(i, carry):
        body(aligned(start + i * tile, 128), tile)
        return carry

    lax.fori_loop(0, full, step, 0)
    if width % tile:
        body(start + full * tile, width % tile)


def dot_nt(a, b):
    return lax.dot_general(a, b, (((1,), (1,)), ((), ())), preferred_element_type=F32)


def dot_nn(a, b):
    return jnp.dot(a, b, preferred_element_type=F32)


class Place:
    def __init__(self):
        self.t = lax.axis_index('tp')
        self.d = lax.axis_index('dp')
        self.cx, self.c = self.d // 2, lax.rem(self.d, 2)
        cx, c = self.cx, self.c
        self.sib = 2 * cx + (1 - c)
        self.opp = 2 * (1 - cx) + c
        self.far = 2 * (1 - cx) + (1 - c)
        self.own_row = aligned(32 * (2 * c + cx), 32)
        self.opp_row = aligned(32 * (2 * c + 1 - cx), 32)
        self.sib_row = aligned(32 * (2 * (1 - c) + cx), 32)
        self.far_row = aligned(32 * (2 * (1 - c) + 1 - cx), 32)
        self.keep = pl.ds(aligned(64 * self.t, 64), 64)
        self.give = pl.ds(aligned(64 * (1 - self.t), 64), 64)

    def rows(self, k):
        if k == 0:
            return self.opp_row, self.own_row, self.far_row, self.sib_row
        return self.own_row, self.opp_row, self.sib_row, self.far_row

    def enter(self):
        barrier = pltpu.get_barrier_semaphore()
        for dt in range(2):
            for dd in range(4):
                if dt or dd:
                    pl.semaphore_signal(barrier, inc=1, device_id_type=MESH, device_id={
                        'tp': lax.rem(self.t + dt, 2), 'dp': lax.rem(self.d + dd, 4)})
        return barrier


class Gather:
    def __init__(self, at, buf, parts, chunk_list, sems):
        self.at, self.buf, self.parts, self.chunks = at, buf, parts, chunk_list
        self.opp_s, self.opp_r, self.sib_s, self.sib_r, self.fwd_s, self.fwd_r = sems

    def copy(self, k, src_row, dst_row, send, recv, to):
        cs = cols_of(self.chunks[k])
        return pltpu.make_async_remote_copy(
            src_ref=self.buf.at[self.parts, pl.ds(src_row, 32), cs],
            dst_ref=self.buf.at[self.parts, pl.ds(dst_row, 32), cs],
            send_sem=send.at[k], recv_sem=recv.at[k], device_id={'dp': to}, device_id_type=MESH)

    def out_opp(self, k, dst=None):
        own = self.at.rows(k)[0]
        return self.copy(k, own, own if dst is None else dst, self.opp_s, self.opp_r, self.at.opp)

    def out_sib(self, k, dst=None):
        own = self.at.rows(k)[0]
        return self.copy(k, own, own if dst is None else dst, self.sib_s, self.sib_r, self.at.sib)

    def out_fwd(self, k, dst=None):
        opp = self.at.rows(k)[1]
        return self.copy(k, opp, opp if dst is None else dst, self.fwd_s, self.fwd_r, self.at.sib)

    def send(self, k):
        self.out_opp(k).start()
        self.out_sib(k).start()

    def forward(self, k):
        self.out_opp(k, self.at.rows(k)[1]).wait_recv()
        self.out_fwd(k).start()

    def arrived(self, k):
        self.out_sib(k, self.at.rows(k)[2]).wait_recv()
        self.out_fwd(k, self.at.rows(k)[3]).wait_recv()

    def drain(self):
        for k in range(len(self.chunks)):
            self.out_opp(k).wait_send()
            self.out_sib(k).wait_send()
            self.out_fwd(k).wait_send()


class RowSum:
    def __init__(self, at, acc, kept, got, ready, landed, sems):
        self.at, self.acc, self.kept, self.got, self.ready, self.landed = at, acc, kept, got, ready, landed
        self.sum_s, self.sum_r, self.row_s, self.row_r = sems
        self.local = at.c == at.t

    def tile(self, n):
        return pl.ds(n * TW, TW)

    def swap(self, n):
        at = self.at
        return pltpu.make_async_remote_copy(
            src_ref=self.acc.at[at.give, self.tile(n)], dst_ref=self.got.at[:, self.tile(n)],
            send_sem=self.sum_s.at[n], recv_sem=self.sum_r.at[n], device_id={'tp': 1 - at.t}, device_id_type=MESH)

    def row_copy(self, n, ox, ot):
        at = self.at
        chip = 1 - at.cx if ox else at.cx
        return pltpu.make_async_remote_copy(
            src_ref=self.ready.at[pl.ds(aligned(32 * chip, 32), 32), self.tile(n)],
            dst_ref=self.landed.at[:, pl.ds(aligned(1024 * at.d + n * TW, 128), TW)],
            send_sem=self.row_s.at[n, 2 * ox + ot], recv_sem=self.row_r.at[n, at.d],
            device_id={'tp': 1 - at.t if ot else at.t, 'dp': 2 * chip + at.t}, device_id_type=MESH)

    def own_copy(self, n):
        at = self.at
        return pltpu.make_async_copy(
            self.ready.at[pl.ds(aligned(32 * at.cx, 32), 32), self.tile(n)],
            self.landed.at[:, pl.ds(aligned(1024 * at.d + n * TW, 128), TW)], self.row_r.at[n, at.d])

    def row_arrive(self, n, s):
        return pltpu.make_async_remote_copy(
            src_ref=self.ready.at[pl.ds(0, 32), self.tile(n)],
            dst_ref=self.landed.at[:, pl.ds(1024 * s + n * TW, TW)],
            send_sem=self.row_s.at[n, 0], recv_sem=self.row_r.at[n, s],
            device_id={'tp': 1 - self.at.t}, device_id_type=MESH)

    def finish(self, n):
        at, ns = self.at, self.tile(n)
        self.swap(n).wait_recv()
        total = self.acc[at.keep, ns] + self.got[:, ns]
        self.ready[:, ns] = (self.kept[at.keep, ns].astype(F32) + total).astype(BF16)
        for ox, ot in ((1, 1), (0, 1)):
            self.row_copy(n, ox, ot).start()

        @pl.when(jnp.logical_not(self.local))
        def _():
            self.row_copy(n, 0, 0).start()

        @pl.when(self.local)
        def _():
            self.own_copy(n).start()

    def collect(self):
        for n in range(NT):
            for s in range(4):
                @pl.when(jnp.logical_not(jnp.logical_and(self.local, self.at.d == s)))
                def _():
                    self.row_arrive(n, s).wait_recv()

            @pl.when(self.local)
            def _():
                self.own_copy(n).wait()

    def drain(self):
        for n in range(NT):
            self.swap(n).wait_send()
            for ox, ot in ((1, 1), (1, 0), (0, 1)):
                self.row_copy(n, ox, ot).wait_send()

        @pl.when(jnp.logical_not(self.local))
        def _():
            for n in range(NT):
                self.row_copy(n, 0, 0).wait_send()


def gate_grads(act, slot, own, cs, a, b, g):
    s = jax.nn.sigmoid(a)
    act[slot, own, cs] = (g * b * s * (1.0 + a * (1.0 - s))).astype(BF16)
    act[slot + 1, own, cs] = (g * (a * s)).astype(BF16)


def front_kernel(x_hbm, dy_hbm, wg_hbm, wu_hbm, wd_hbm,
                 da_out, db_out, act_t_out, cols_t_out, dy_cols_out, y_out, dx_out,
                 x_ref, dy_ref, wg, wu, wd, part, from_sib, from_opp, act, act_t, cols, cols_t, y_acc, dx_acc, y_got, y_ready,
                 in_sem, gu_sem, d_sem, x_send, x_recv, a0_s, a0_r, a1_s, a1_r, a2_s, a2_r, g1_s, g1_r, g2_s, g2_r,
                 h_sems, q_sems, sum_s, sum_r, row_s, row_r, t_sem, q_sem, o_sem, dx_sem):
    at = Place()
    own, opp = pl.ds(at.own_row, 32), pl.ds(at.opp_row, 32)
    sib_half = pl.ds(aligned(64 * (1 - at.c), 64), 64)
    mine, theirs = pl.ds(aligned(32 * at.cx, 32), 32), pl.ds(aligned(32 * (1 - at.cx), 32), 32)

    def gate_up_loads(k):
        cs = cols_of(AB[k])
        return (pltpu.make_async_copy(wg_hbm.at[:, cs], wg.at[:, cs], gu_sem.at[0, k]),
                pltpu.make_async_copy(wu_hbm.at[:, cs], wu.at[:, cs], gu_sem.at[1, k]))

    def down_load(k):
        cs = cols_of(GG[k])
        return pltpu.make_async_copy(wd_hbm.at[cs, :], wd.at[cs, :], d_sem.at[k])

    barrier = at.enter()
    token_loads = (pltpu.make_async_copy(x_hbm, x_ref, in_sem.at[0]),
                   pltpu.make_async_copy(dy_hbm, dy_ref, in_sem.at[1]))
    for load in token_loads:
        load.start()
    for k in range(2):
        for load in gate_up_loads(k):
            load.start()
    pl.semaphore_wait(barrier, 7)

    peers = (at.sib, at.opp, at.far)
    tokens = (x_ref, dy_ref)

    def token_copy(i, q, row):
        return pltpu.make_async_remote_copy(
            src_ref=tokens[i].at[:, pl.ds(aligned(1024 * peers[q], 128), 1024)],
            dst_ref=cols.at[i, pl.ds(row, 32), :],
            send_sem=x_send.at[i, q], recv_sem=x_recv.at[i, q],
            device_id={'dp': peers[q]}, device_id_type=MESH)

    for i in range(2):
        token_loads[i].wait()
        for q in (2, 1, 0):
            token_copy(i, q, at.own_row).start()
    for k in range(2, NA):
        for load in gate_up_loads(k):
            load.start()
    for k in range(NG):
        down_load(k).start()
    for i in range(2):
        cols[i, own, :] = tokens[i][:, pl.ds(aligned(1024 * at.d, 128), 1024)]

    def token_wait(i, which=(0, 1, 2)):
        for q in which:
            token_copy(i, q, (at.sib_row, at.opp_row, at.far_row)[q]).wait_recv()

    def core_copy(parts, chunk, k, send, recv):
        cs = cols_of(chunk)
        return pltpu.make_async_remote_copy(
            src_ref=part.at[parts, sib_half, cs], dst_ref=from_sib.at[parts, :, cs],
            send_sem=send.at[k], recv_sem=recv.at[k], device_id={'dp': at.sib}, device_id_type=MESH)

    def chip_copy(parts, chunk, k, send, recv):
        cs = cols_of(chunk)
        return pltpu.make_async_remote_copy(
            src_ref=part.at[parts, pl.ds(at.rows(k)[1], 32), cs], dst_ref=from_opp.at[parts, :, cs],
            send_sem=send.at[k], recv_sem=recv.at[k], device_id={'dp': at.opp}, device_id_type=MESH)

    ab, gg = pl.ds(0, 2), pl.ds(2, 1)

    def a1(k):
        return core_copy(ab, AB[k], k, a1_s, a1_r)

    def a2(k):
        return chip_copy(ab, AB[k], k, a2_s, a2_r)

    def g1(k):
        return core_copy(gg, GG[k], k, g1_s, g1_r)

    def g2(k):
        return chip_copy(gg, GG[k], k, g2_s, g2_r)

    def first_core_copy(which):
        cs = cols_of(AB[0])
        return pltpu.make_async_remote_copy(
            src_ref=part.at[ab, pl.ds((at.sib_row, at.far_row)[which], 32), cs],
            dst_ref=from_sib.at[ab, (mine, theirs)[which], cs],
            send_sem=a0_s.at[which], recv_sem=a0_r.at[which], device_id={'dp': at.sib}, device_id_type=MESH)

    def first_partials(which):
        upper, lower = [pl.ds(row, 32) for row in ((at.own_row, at.sib_row), (at.opp_row, at.far_row))[which]]
        cs = cols_of(AB[0])
        rows = jnp.concatenate([cols[0, upper, :], cols[0, lower, :]], axis=0)
        for i, w in enumerate((wg, wu)):
            out = dot_nn(rows, w[:, cs])
            part[i, upper, cs] = out[:32]
            part[i, lower, cs] = out[32:]
        first_core_copy(which).start()

    def first_chunk():
        for load in gate_up_loads(0):
            load.wait()
        token_wait(0, (0,))
        first_partials(0)
        first_core_copy(0).wait_recv()
        cs = cols_of(AB[0])
        for i in range(2):
            part[i, own, cs] += from_sib[i, mine, cs]
        a2(0).start()
        token_wait(0, (1, 2))
        first_partials(1)

    def ab_partials(k):
        for load in gate_up_loads(k):
            load.wait()

        def body(col, width):
            cs = pl.ds(col, width)
            part[0, :, cs] = dot_nn(cols[0], wg[:, cs])
            part[1, :, cs] = dot_nn(cols[0], wu[:, cs])

        column_tiles(AB[k], body, 512)
        a1(k).start()

    def ab_sum(k):
        a1(k).wait_recv()

        def add(col, width):
            cs = pl.ds(col, width)
            for i in range(2):
                part[i, opp, cs] += from_sib[i, theirs, cs]

        column_tiles(AB[k], add)
        a2(k).start()

    def g_partials(k):
        down_load(k).wait()
        if k == 0:
            token_wait(1)

        def body(col, width):
            cs = pl.ds(col, width)
            part[2, :, cs] = dot_nt(cols[1], wd[cs, :])

        column_tiles(GG[k], body, 512)
        g1(k).start()

    def g_sum(k):
        g1(k).wait_recv()

        def add(col, width):
            cs = pl.ds(col, width)
            part[2, opp, cs] += from_sib[2, theirs, cs]
            part[2, own, cs] += from_sib[2, mine, cs]

        column_tiles(GG[k], add)

    hg = Gather(at, act, pl.ds(0, 1), AB, [h_sems.at[i] for i in range(6)])
    qg = Gather(at, act, pl.ds(1, 2), GG, [q_sems.at[i] for i in range(6)])

    def hidden(k):
        if k == 0:
            first_core_copy(1).wait_recv()
        a2(k).wait_recv()
        here = pl.ds(at.rows(k)[0], 32)
        core = theirs if k == 0 else mine

        def body(col, width):
            cs = pl.ds(col, width)
            a, b = [part[i, here, cs] + from_sib[i, core, cs] + from_opp[i, :, cs] for i in range(2)]
            part[0, here, cs] = a
            part[1, here, cs] = b
            act[0, here, cs] = (a * jax.nn.sigmoid(a) * b).astype(BF16)

        column_tiles(AB[k], body)
        hg.send(k)

    def act_t_store(k):
        cs = cols_of(AB[k])
        return pltpu.make_async_copy(act_t.at[cs, :], act_t_out.at[cs, :], t_sem.at[k])

    ysum = RowSum(at, y_acc, cols.at[0], y_got, y_ready, y_out, (sum_s, sum_r, row_s, row_r))

    def outputs(k):
        hg.arrived(k)
        cs = cols_of(AB[k])

        def flip(col, width):
            ts = pl.ds(col, width)
            act_t[ts, :] = act[0, :, ts].T

        column_tiles(AB[k], flip)
        act_t_store(k).start()

        def tile(ns):
            y = dot_nn(act[0, :, cs], wd[cs, ns])
            y_acc[:, ns] = y if k == 0 else y_acc[:, ns] + y

        if k < NA - 1:
            @pl.loop(0, 1024 // MW)
            def _(n):
                tile(pl.ds(aligned(n * MW, 128), MW))
        else:
            for n in range(NT):
                tile(pl.ds(n * TW, TW))
                ysum.swap(n).start()

    def hidden_grads(k):
        g2(k).wait_recv()
        here = pl.ds(at.rows(k)[0], 32)

        def body(col, width):
            cs = pl.ds(col, width)
            gate_grads(act, 1, here, cs, part[0, here, cs], part[1, here, cs], part[2, here, cs] + from_opp[2, :, cs])

        column_tiles(GG[k], body)
        qg.send(k)

    def act_stores(k):
        cs = cols_of(GG[k])
        return (pltpu.make_async_copy(act.at[1, :, cs], da_out.at[:, cs], q_sem.at[0, k]),
                pltpu.make_async_copy(act.at[2, :, cs], db_out.at[:, cs], q_sem.at[1, k]))

    def dx_part(k, n):
        cs, ns = cols_of(GG[k]), pl.ds(n * MW, MW)
        if n == 0:
            qg.arrived(k)
            for store in act_stores(k):
                store.start()
        dx = dot_nt(act[1, :, cs], wg[ns, cs]) + dot_nt(act[2, :, cs], wu[ns, cs])
        dx_acc[:, ns] = dx if k == 0 else dx_acc[:, ns] + dx

    def dx_stores(n):
        ns = pl.ds(n * MW, MW)
        for dt in range(2):
            for dd in range(4):
                row = 32 * (2 * (dd % 2) + dd // 2)
                yield pltpu.make_async_copy(dx_acc.at[pl.ds(row, 32), ns], dx_out.at[4 * dt + dd, :, ns],
                                            dx_sem.at[n, 4 * dt + dd])

    stores = [
        pltpu.make_async_copy(cols.at[1], dy_cols_out, o_sem.at[0]),
        pltpu.make_async_copy(cols_t, cols_t_out, o_sem.at[1]),
    ]

    first_chunk()
    for k in range(1, NA):
        ab_partials(k)
        if k >= 2:
            ab_sum(k - 1)
    ab_sum(NA - 1)
    for k in range(NG):
        g_partials(k)
        if k >= 1:
            g_sum(k - 1)
    g_sum(NG - 1)
    stores[0].start()
    for n in range(4):
        cols_t[n * 256:(n + 1) * 256, :] = cols[0, :, n * 256:(n + 1) * 256].T
    stores[1].start()
    for k in range(NA):
        hidden(k)
    for k in range(NG):
        g2(k).start()
    for k in range(NA):
        hg.forward(k)
        if k >= 1:
            outputs(k - 1)
    outputs(NA - 1)
    for k in range(NG):
        hidden_grads(k)
    for n in range(NT):
        ysum.finish(n)
    for n in range(NT):
        ysum.row_copy(n, 1, 0).start()
    for step in ('f0', 'f1', 'd0', 'D0', 'f2', 'd1', 'D1', 'd2', 'f3', 'D2', 'f4', 'd3', 'f5', 'D3', 'f6', 'f7',
                 'd4', 'D4', 'd5', 'D5', 'd6', 'D6', 'd7'):
        k = int(step[1])
        if step[0] == 'f':
            qg.forward(k)
        else:
            dx_part(k, 0 if step[0] == 'd' else 1)
    for n in range(2):
        if n:
            dx_part(NG - 1, n)
        for store in dx_stores(n):
            store.start()
    ysum.collect()
    for i in range(2):
        for q in range(3):
            token_copy(i, q, at.own_row).wait_send()
    for k in range(NA):
        if k == 0:
            first_core_copy(0).wait_send()
            first_core_copy(1).wait_send()
        else:
            a1(k).wait_send()
        a2(k).wait_send()
        act_t_store(k).wait()
    for k in range(NG):
        g1(k).wait_send()
        g2(k).wait_send()
        for store in act_stores(k):
            store.wait()
    hg.drain()
    qg.drain()
    ysum.drain()
    for store in stores:
        store.wait()
    for n in range(2):
        for store in dx_stores(n):
            store.wait()


DMA = pltpu.SemaphoreType.DMA
ANY = pl.BlockSpec(memory_space=pl.ANY)
VMEM = pl.BlockSpec(memory_space=pltpu.VMEM)
HBM = pl.BlockSpec(memory_space=pltpu.HBM)


def shape(dims, dtype):
    return jax.ShapeDtypeStruct(dims, dtype)


def front(x_rows, dy_rows, gate, up, down):
    return pl.pallas_call(
        front_kernel,
        name='front',
        out_shape=(shape((128, HID), BF16), shape((128, HID), BF16), shape((HID, 128), BF16), shape((1024, 128), BF16),
                   shape((128, 1024), BF16), shape((32, 4096), BF16), shape((8, 32, 1024), F32)),
        in_specs=[ANY] * 5,
        out_specs=(ANY,) * 7,
        scratch_shapes=[
            pltpu.VMEM((32, 4096), BF16), pltpu.VMEM((32, 4096), BF16),
            pltpu.VMEM((1024, HID), BF16), pltpu.VMEM((1024, HID), BF16), pltpu.VMEM((HID, 1024), BF16),
            pltpu.VMEM((3, 128, HID), F32), pltpu.VMEM((3, 64, HID), F32), pltpu.VMEM((3, 32, HID), F32),
            pltpu.VMEM((3, 128, HID), BF16), pltpu.VMEM((HID, 128), BF16), pltpu.VMEM((2, 128, 1024), BF16),
            pltpu.VMEM((1024, 128), BF16), pltpu.VMEM((128, 1024), F32), pltpu.VMEM((128, 1024), F32),
            pltpu.VMEM((64, 1024), F32), pltpu.VMEM((64, 1024), BF16),
            DMA((2,)), DMA((2, NA)), DMA((NG,)), DMA((2, 3)), DMA((2, 3)),
            DMA((2,)), DMA((2,)), DMA((NA,)), DMA((NA,)), DMA((NA,)), DMA((NA,)),
            DMA((NG,)), DMA((NG,)), DMA((NG,)), DMA((NG,)),
            DMA((6, NA)), DMA((6, NG)), DMA((NT,)), DMA((NT,)), DMA((NT, 4)), DMA((NT, 4)),
            DMA((NA,)), DMA((2, NG)), DMA((2,)), DMA((2, 8)),
        ],
        compiler_params=pltpu.CompilerParams(collective_id=0, has_side_effects=True, vmem_limit_bytes=VMEM_CAP),
        cost_estimate=pl.CostEstimate(flops=9 * 10**9, bytes_accessed=4 * 10**7, transcendentals=0),
    )(x_rows, dy_rows, gate, up, down)


TILE = 512
SLOTS = 6
MIB = 1 << 20


def stream_tiles(compute, store, width, rest=None):
    full, last = width // TILE, width % TILE
    compute(0, 0, TILE)
    store(0, 0, TILE).start()
    if rest is not None:
        rest()

    def step(i, carry):
        slot = lax.rem(i, SLOTS)

        @pl.when(i >= SLOTS)
        def _():
            store(i - SLOTS, slot, TILE).wait()

        compute(i, slot, TILE)
        store(i, slot, TILE).start()
        return carry

    lax.fori_loop(1, full, step, 0)
    total = full
    if last:
        if full >= SLOTS:
            store(full - SLOTS, full % SLOTS, TILE).wait()
        compute(full, full % SLOTS, last)
        store(full, full % SLOTS, last).start()
        total += 1

    def drain():
        for i in range(max(0, total - SLOTS), total):
            store(i, i % SLOTS, TILE if i < full else last).wait()

    return drain


def column_job(left, right, ring, out, sem):
    def compute(i, slot, width):
        cs = pl.ds(aligned(i * TILE, 128), width)
        ring[slot, :, pl.ds(0, width)] = dot_nn(left[...], right[:, cs])

    def store(i, slot, width):
        return pltpu.make_async_copy(ring.at[slot, :, pl.ds(0, width)],
                                     out.at[:, pl.ds(aligned(i * TILE, 128), width)], sem.at[slot])

    return compute, store


def row_job(left, right, ring, out, sem):
    def compute(i, slot, width):
        ring[slot, pl.ds(0, width), :] = dot_nn(left[pl.ds(aligned(i * TILE, 128), width), :], right[...])

    def store(i, slot, width):
        return pltpu.make_async_copy(ring.at[slot, pl.ds(0, width), :],
                                     out.at[pl.ds(aligned(i * TILE, 128), width), :], sem.at[slot])

    return compute, store


def grads_first_kernel(act_t_hbm, dy_cols_hbm, cols_t_hbm, da_hbm, down_out, gate_out,
                       act_t, dy_cols, cols_t, da, ring_d, ring_c, in_sem, sem_d, sem_c):
    head, tail = pl.ds(0, TILE), pl.ds(TILE, HID - TILE)
    pairs = ((dy_cols_hbm, dy_cols), (act_t_hbm.at[head, :], act_t.at[head, :]),
             (act_t_hbm.at[tail, :], act_t.at[tail, :]), (cols_t_hbm, cols_t), (da_hbm, da))
    loads = [pltpu.make_async_copy(src, dst, in_sem.at[n]) for n, (src, dst) in enumerate(pairs)]
    for load in loads:
        load.start()

    def rest():
        for load in loads[2:]:
            load.wait()

    loads[0].wait()
    loads[1].wait()
    drain_d = stream_tiles(*row_job(act_t, dy_cols, ring_d, down_out, sem_d), HID, rest)
    drain_c = stream_tiles(*column_job(cols_t, da, ring_c, gate_out, sem_c), HID)
    drain_d()
    drain_c()


def grads_first(act_t, dy_cols, cols_t, da):
    return pl.pallas_call(
        grads_first_kernel,
        name='grads_first',
        out_shape=(shape((HID, 1024), F32), shape((1024, HID), F32)),
        in_specs=[HBM] * 4,
        out_specs=(ANY,) * 2,
        scratch_shapes=[pltpu.VMEM((HID, 128), BF16), pltpu.VMEM((128, 1024), BF16), pltpu.VMEM((1024, 128), BF16),
                        pltpu.VMEM((128, HID), BF16),
                        pltpu.VMEM((SLOTS, TILE, 1024), F32), pltpu.VMEM((SLOTS, 1024, TILE), F32),
                        DMA((5,)), DMA((SLOTS,)), DMA((SLOTS,))],
        compiler_params=pltpu.CompilerParams(vmem_limit_bytes=60 * MIB),
        cost_estimate=pl.CostEstimate(flops=2 * 10**10, bytes_accessed=5 * 10**7, transcendentals=0),
    )(act_t, dy_cols, cols_t, da)


def grads_last_kernel(cols_t, db, y_rows, dy_rows, got, up_out, y_out, dx_out, dx_rows, ring, sem, row_sem):
    drain = stream_tiles(*column_job(cols_t, db, ring, up_out, sem), HID)
    copies = (pltpu.make_async_copy(y_rows, y_out, row_sem.at[0]), pltpu.make_async_copy(dx_rows, dx_out, row_sem.at[1]))
    copies[0].start()
    for d in range(4):
        cs = pl.ds(1024 * d, 1024)
        dx_rows[:, cs] = (dy_rows[:, cs].astype(F32) + (got[d] + got[4 + d])).astype(BF16)
    copies[1].start()
    drain()
    for copy in copies:
        copy.wait()


def grads_last(cols_t, db, y, dy, got):
    return pl.pallas_call(
        grads_last_kernel,
        name='grads_last',
        out_shape=(shape((1024, HID), F32), shape((32, 4096), BF16), shape((32, 4096), BF16)),
        in_specs=[VMEM] * 5,
        out_specs=(ANY,) * 3,
        scratch_shapes=[pltpu.VMEM((32, 4096), BF16), pltpu.VMEM((SLOTS, 1024, TILE), F32),
                        DMA((SLOTS,)), DMA((2,))],
        compiler_params=pltpu.CompilerParams(vmem_limit_bytes=20 * MIB),
        cost_estimate=pl.CostEstimate(flops=10**10, bytes_accessed=3 * 10**7, transcendentals=0),
    )(cols_t, db, y, dy, got)


def solution(mesh):
    def device_pass(x_rows, gate_blk, up_blk, down_blk, dy_rows):
        da, db, act_t, cols_t, dy_cols, y_part, dx_part = front(x_rows, dy_rows, gate_blk, up_blk, down_blk)
        got = lax.all_to_all(dx_part, ('tp', 'dp'), 0, 0, tiled=True)
        dw_down, dw_gate = grads_first(act_t, dy_cols, cols_t, da)
        dw_up, y_rows, dx_rows = grads_last(cols_t, db, y_part, dy_rows, got)
        return y_rows, dx_rows, dw_gate, dw_up, dw_down

    row_spec = P('dp', None)
    weight_spec = P('dp', 'tp')
    down_spec = P('tp', 'dp')
    return jax.shard_map(device_pass, mesh=mesh,
                         in_specs=(row_spec, weight_spec, weight_spec, down_spec, row_spec),
                         out_specs=(row_spec, row_spec, weight_spec, weight_spec, down_spec),
                         check_vma=False)
```

```python
import jax
import jax.numpy as jnp
from jax import lax
from jax.experimental import pallas as pl
from jax.experimental.pallas import tpu as pltpu
from jax.sharding import PartitionSpec as P

MESH = pl.DeviceIdType.MESH
F32, BF16 = jnp.float32, jnp.bfloat16
VMEM_CAP = 67043328
HID = 5504


def chunks(start, widths):
    out = []
    for w in widths:
        out.append((start, w))
        start += w
    return tuple(out)


AB = chunks(0, (512, 512, 1024, 1024, 1024, 1024, 384))
GG = chunks(0, (512, 1024, 1024, 1024, 768, 640, 384, 128))
NA, NG = len(AB), len(GG)
NT = 4
TW = 1024 // NT
MW = 512


def aligned(v, m):
    return pl.multiple_of(v, m)


def cols_of(chunk):
    return pl.ds(chunk[0], chunk[1])


def column_tiles(chunk, body, tile=256):
    start, width = chunk
    full = width // tile

    def step(i, carry):
        body(aligned(start + i * tile, 128), tile)
        return carry

    lax.fori_loop(0, full, step, 0)
    if width % tile:
        body(start + full * tile, width % tile)


def dot_nt(a, b):
    return lax.dot_general(a, b, (((1,), (1,)), ((), ())), preferred_element_type=F32)


def dot_nn(a, b):
    return jnp.dot(a, b, preferred_element_type=F32)


class Place:
    def __init__(self):
        self.t = lax.axis_index('tp')
        self.d = lax.axis_index('dp')
        self.cx, self.c = self.d // 2, lax.rem(self.d, 2)
        cx, c = self.cx, self.c
        self.sib = 2 * cx + (1 - c)
        self.opp = 2 * (1 - cx) + c
        self.far = 2 * (1 - cx) + (1 - c)
        self.own_row = aligned(32 * (2 * c + cx), 32)
        self.opp_row = aligned(32 * (2 * c + 1 - cx), 32)
        self.sib_row = aligned(32 * (2 * (1 - c) + cx), 32)
        self.far_row = aligned(32 * (2 * (1 - c) + 1 - cx), 32)
        self.keep = pl.ds(aligned(64 * self.t, 64), 64)
        self.give = pl.ds(aligned(64 * (1 - self.t), 64), 64)

    def rows(self, k):
        if k == 0:
            return self.opp_row, self.own_row, self.far_row, self.sib_row
        return self.own_row, self.opp_row, self.sib_row, self.far_row

    def enter(self):
        barrier = pltpu.get_barrier_semaphore()
        for dt in range(2):
            for dd in range(4):
                if dt or dd:
                    pl.semaphore_signal(barrier, inc=1, device_id_type=MESH, device_id={
                        'tp': lax.rem(self.t + dt, 2), 'dp': lax.rem(self.d + dd, 4)})
        return barrier


class Gather:
    def __init__(self, at, buf, parts, chunk_list, sems):
        self.at, self.buf, self.parts, self.chunks = at, buf, parts, chunk_list
        self.opp_s, self.opp_r, self.sib_s, self.sib_r, self.fwd_s, self.fwd_r = sems

    def copy(self, k, src_row, dst_row, send, recv, to):
        cs = cols_of(self.chunks[k])
        return pltpu.make_async_remote_copy(
            src_ref=self.buf.at[self.parts, pl.ds(src_row, 32), cs],
            dst_ref=self.buf.at[self.parts, pl.ds(dst_row, 32), cs],
            send_sem=send.at[k], recv_sem=recv.at[k], device_id={'dp': to}, device_id_type=MESH)

    def out_opp(self, k, dst=None):
        own = self.at.rows(k)[0]
        return self.copy(k, own, own if dst is None else dst, self.opp_s, self.opp_r, self.at.opp)

    def out_sib(self, k, dst=None):
        own = self.at.rows(k)[0]
        return self.copy(k, own, own if dst is None else dst, self.sib_s, self.sib_r, self.at.sib)

    def out_fwd(self, k, dst=None):
        opp = self.at.rows(k)[1]
        return self.copy(k, opp, opp if dst is None else dst, self.fwd_s, self.fwd_r, self.at.sib)

    def send(self, k):
        self.out_opp(k).start()
        self.out_sib(k).start()

    def forward(self, k):
        self.out_opp(k, self.at.rows(k)[1]).wait_recv()
        self.out_fwd(k).start()

    def arrived(self, k):
        self.out_sib(k, self.at.rows(k)[2]).wait_recv()
        self.out_fwd(k, self.at.rows(k)[3]).wait_recv()

    def drain(self):
        for k in range(len(self.chunks)):
            self.out_opp(k).wait_send()
            self.out_sib(k).wait_send()
            self.out_fwd(k).wait_send()


class RowSum:
    def __init__(self, at, acc, kept, got, ready, landed, sems):
        self.at, self.acc, self.kept, self.got, self.ready, self.landed = at, acc, kept, got, ready, landed
        self.sum_s, self.sum_r, self.row_s, self.row_r = sems
        self.local = at.c == at.t

    def tile(self, n):
        return pl.ds(n * TW, TW)

    def swap(self, n):
        at = self.at
        return pltpu.make_async_remote_copy(
            src_ref=self.acc.at[at.give, self.tile(n)], dst_ref=self.got.at[:, self.tile(n)],
            send_sem=self.sum_s.at[n], recv_sem=self.sum_r.at[n], device_id={'tp': 1 - at.t}, device_id_type=MESH)

    def row_copy(self, n, ox, ot):
        at = self.at
        chip = 1 - at.cx if ox else at.cx
        return pltpu.make_async_remote_copy(
            src_ref=self.ready.at[pl.ds(aligned(32 * chip, 32), 32), self.tile(n)],
            dst_ref=self.landed.at[:, pl.ds(aligned(1024 * at.d + n * TW, 128), TW)],
            send_sem=self.row_s.at[n, 2 * ox + ot], recv_sem=self.row_r.at[n, at.d],
            device_id={'tp': 1 - at.t if ot else at.t, 'dp': 2 * chip + at.t}, device_id_type=MESH)

    def own_copy(self, n):
        at = self.at
        return pltpu.make_async_copy(
            self.ready.at[pl.ds(aligned(32 * at.cx, 32), 32), self.tile(n)],
            self.landed.at[:, pl.ds(aligned(1024 * at.d + n * TW, 128), TW)], self.row_r.at[n, at.d])

    def row_arrive(self, n, s):
        return pltpu.make_async_remote_copy(
            src_ref=self.ready.at[pl.ds(0, 32), self.tile(n)],
            dst_ref=self.landed.at[:, pl.ds(1024 * s + n * TW, TW)],
            send_sem=self.row_s.at[n, 0], recv_sem=self.row_r.at[n, s],
            device_id={'tp': 1 - self.at.t}, device_id_type=MESH)

    def finish(self, n):
        at, ns = self.at, self.tile(n)
        self.swap(n).wait_recv()
        total = self.acc[at.keep, ns] + self.got[:, ns]
        self.ready[:, ns] = (self.kept[at.keep, ns].astype(F32) + total).astype(BF16)
        for ox, ot in ((1, 1), (0, 1)):
            self.row_copy(n, ox, ot).start()

        @pl.when(jnp.logical_not(self.local))
        def _():
            self.row_copy(n, 0, 0).start()

        @pl.when(self.local)
        def _():
            self.own_copy(n).start()

    def collect(self):
        for n in range(NT):
            for s in range(4):
                @pl.when(jnp.logical_not(jnp.logical_and(self.local, self.at.d == s)))
                def _():
                    self.row_arrive(n, s).wait_recv()

            @pl.when(self.local)
            def _():
                self.own_copy(n).wait()

    def drain(self):
        for n in range(NT):
            self.swap(n).wait_send()
            for ox, ot in ((1, 1), (1, 0), (0, 1)):
                self.row_copy(n, ox, ot).wait_send()

        @pl.when(jnp.logical_not(self.local))
        def _():
            for n in range(NT):
                self.row_copy(n, 0, 0).wait_send()


def gate_grads(act, slot, own, cs, a, b, g):
    s = jax.nn.sigmoid(a)
    act[slot, own, cs] = (g * b * s * (1.0 + a * (1.0 - s))).astype(BF16)
    act[slot + 1, own, cs] = (g * (a * s)).astype(BF16)


def front_kernel(x_hbm, dy_hbm, wg_hbm, wu_hbm, wd_hbm,
                 da_out, db_out, act_t_out, cols_t_out, dy_cols_out, y_out, dx_out,
                 x_ref, dy_ref, wg, wu, wd, part, from_sib, from_opp, act, act_t, cols, cols_t, y_acc, dx_acc, y_got, y_ready,
                 in_sem, gu_sem, d_sem, x_send, x_recv, a0_s, a0_r, a1_s, a1_r, a2_s, a2_r, g1_s, g1_r, g2_s, g2_r,
                 h_sems, q_sems, sum_s, sum_r, row_s, row_r, t_sem, q_sem, o_sem, dx_sem):
    at = Place()
    own, opp = pl.ds(at.own_row, 32), pl.ds(at.opp_row, 32)
    sib_half = pl.ds(aligned(64 * (1 - at.c), 64), 64)
    mine, theirs = pl.ds(aligned(32 * at.cx, 32), 32), pl.ds(aligned(32 * (1 - at.cx), 32), 32)

    def gate_up_loads(k):
        cs = cols_of(AB[k])
        return (pltpu.make_async_copy(wg_hbm.at[:, cs], wg.at[:, cs], gu_sem.at[0, k]),
                pltpu.make_async_copy(wu_hbm.at[:, cs], wu.at[:, cs], gu_sem.at[1, k]))

    def down_load(k):
        cs = cols_of(GG[k])
        return pltpu.make_async_copy(wd_hbm.at[cs, :], wd.at[cs, :], d_sem.at[k])

    barrier = at.enter()
    token_loads = (pltpu.make_async_copy(x_hbm, x_ref, in_sem.at[0]),
                   pltpu.make_async_copy(dy_hbm, dy_ref, in_sem.at[1]))
    for load in token_loads:
        load.start()
    for k in range(2):
        for load in gate_up_loads(k):
            load.start()
    pl.semaphore_wait(barrier, 7)

    peers = (at.sib, at.opp, at.far)
    tokens = (x_ref, dy_ref)

    def token_copy(i, q, row):
        return pltpu.make_async_remote_copy(
            src_ref=tokens[i].at[:, pl.ds(aligned(1024 * peers[q], 128), 1024)],
            dst_ref=cols.at[i, pl.ds(row, 32), :],
            send_sem=x_send.at[i, q], recv_sem=x_recv.at[i, q],
            device_id={'dp': peers[q]}, device_id_type=MESH)

    for i in range(2):
        token_loads[i].wait()
        for q in (2, 1, 0):
            token_copy(i, q, at.own_row).start()
    for k in range(2, NA):
        for load in gate_up_loads(k):
            load.start()
    for k in range(NG):
        down_load(k).start()
    for i in range(2):
        cols[i, own, :] = tokens[i][:, pl.ds(aligned(1024 * at.d, 128), 1024)]

    def token_wait(i, which=(0, 1, 2)):
        for q in which:
            token_copy(i, q, (at.sib_row, at.opp_row, at.far_row)[q]).wait_recv()

    def core_copy(parts, chunk, k, send, recv):
        cs = cols_of(chunk)
        return pltpu.make_async_remote_copy(
            src_ref=part.at[parts, sib_half, cs], dst_ref=from_sib.at[parts, :, cs],
            send_sem=send.at[k], recv_sem=recv.at[k], device_id={'dp': at.sib}, device_id_type=MESH)

    def chip_copy(parts, chunk, k, send, recv):
        cs = cols_of(chunk)
        return pltpu.make_async_remote_copy(
            src_ref=part.at[parts, pl.ds(at.rows(k)[1], 32), cs], dst_ref=from_opp.at[parts, :, cs],
            send_sem=send.at[k], recv_sem=recv.at[k], device_id={'dp': at.opp}, device_id_type=MESH)

    ab, gg = pl.ds(0, 2), pl.ds(2, 1)

    def a1(k):
        return core_copy(ab, AB[k], k, a1_s, a1_r)

    def a2(k):
        return chip_copy(ab, AB[k], k, a2_s, a2_r)

    def g1(k):
        return core_copy(gg, GG[k], k, g1_s, g1_r)

    def g2(k):
        return chip_copy(gg, GG[k], k, g2_s, g2_r)

    def first_core_copy(which):
        cs = cols_of(AB[0])
        return pltpu.make_async_remote_copy(
            src_ref=part.at[ab, pl.ds((at.sib_row, at.far_row)[which], 32), cs],
            dst_ref=from_sib.at[ab, (mine, theirs)[which], cs],
            send_sem=a0_s.at[which], recv_sem=a0_r.at[which], device_id={'dp': at.sib}, device_id_type=MESH)

    def first_partials(which):
        upper, lower = [pl.ds(row, 32) for row in ((at.own_row, at.sib_row), (at.opp_row, at.far_row))[which]]
        cs = cols_of(AB[0])
        rows = jnp.concatenate([cols[0, upper, :], cols[0, lower, :]], axis=0)
        for i, w in enumerate((wg, wu)):
            out = dot_nn(rows, w[:, cs])
            part[i, upper, cs] = out[:32]
            part[i, lower, cs] = out[32:]
        first_core_copy(which).start()

    def first_chunk():
        for load in gate_up_loads(0):
            load.wait()
        token_wait(0, (0,))
        first_partials(0)
        first_core_copy(0).wait_recv()
        cs = cols_of(AB[0])
        for i in range(2):
            part[i, own, cs] += from_sib[i, mine, cs]
        a2(0).start()
        token_wait(0, (1, 2))
        first_partials(1)

    def ab_partials(k):
        for load in gate_up_loads(k):
            load.wait()

        def body(col, width):
            cs = pl.ds(col, width)
            part[0, :, cs] = dot_nn(cols[0], wg[:, cs])
            part[1, :, cs] = dot_nn(cols[0], wu[:, cs])

        column_tiles(AB[k], body, 512)
        a1(k).start()

    def ab_sum(k):
        a1(k).wait_recv()

        def add(col, width):
            cs = pl.ds(col, width)
            for i in range(2):
                part[i, opp, cs] += from_sib[i, theirs, cs]

        column_tiles(AB[k], add)
        a2(k).start()

    def g_partials(k):
        down_load(k).wait()
        if k == 0:
            token_wait(1)

        def body(col, width):
            cs = pl.ds(col, width)
            part[2, :, cs] = dot_nt(cols[1], wd[cs, :])

        column_tiles(GG[k], body, 512)
        g1(k).start()

    def g_sum(k):
        g1(k).wait_recv()

        def add(col, width):
            cs = pl.ds(col, width)
            part[2, opp, cs] += from_sib[2, theirs, cs]
            part[2, own, cs] += from_sib[2, mine, cs]

        column_tiles(GG[k], add)

    hg = Gather(at, act, pl.ds(0, 1), AB, [h_sems.at[i] for i in range(6)])
    qg = Gather(at, act, pl.ds(1, 2), GG, [q_sems.at[i] for i in range(6)])

    def hidden(k):
        if k == 0:
            first_core_copy(1).wait_recv()
        a2(k).wait_recv()
        here = pl.ds(at.rows(k)[0], 32)
        core = theirs if k == 0 else mine

        def body(col, width):
            cs = pl.ds(col, width)
            a, b = [part[i, here, cs] + from_sib[i, core, cs] + from_opp[i, :, cs] for i in range(2)]
            part[0, here, cs] = a
            part[1, here, cs] = b
            act[0, here, cs] = (a * jax.nn.sigmoid(a) * b).astype(BF16)

        column_tiles(AB[k], body)
        hg.send(k)

    def act_t_store(k):
        cs = cols_of(AB[k])
        return pltpu.make_async_copy(act_t.at[cs, :], act_t_out.at[cs, :], t_sem.at[k])

    ysum = RowSum(at, y_acc, cols.at[0], y_got, y_ready, y_out, (sum_s, sum_r, row_s, row_r))

    def outputs(k):
        hg.arrived(k)
        cs = cols_of(AB[k])

        def flip(col, width):
            ts = pl.ds(col, width)
            act_t[ts, :] = act[0, :, ts].T

        column_tiles(AB[k], flip)
        act_t_store(k).start()

        def tile(ns):
            y = dot_nn(act[0, :, cs], wd[cs, ns])
            y_acc[:, ns] = y if k == 0 else y_acc[:, ns] + y

        if k < NA - 1:
            @pl.loop(0, 1024 // MW)
            def _(n):
                tile(pl.ds(aligned(n * MW, 128), MW))
        else:
            for n in range(NT):
                tile(pl.ds(n * TW, TW))
                ysum.swap(n).start()

    def hidden_grads(k):
        g2(k).wait_recv()
        here = pl.ds(at.rows(k)[0], 32)

        def body(col, width):
            cs = pl.ds(col, width)
            gate_grads(act, 1, here, cs, part[0, here, cs], part[1, here, cs], part[2, here, cs] + from_opp[2, :, cs])

        column_tiles(GG[k], body)
        qg.send(k)

    def act_stores(k):
        cs = cols_of(GG[k])
        return (pltpu.make_async_copy(act.at[1, :, cs], da_out.at[:, cs], q_sem.at[0, k]),
                pltpu.make_async_copy(act.at[2, :, cs], db_out.at[:, cs], q_sem.at[1, k]))

    def dx_part(k, n):
        cs, ns = cols_of(GG[k]), pl.ds(n * MW, MW)
        if n == 0:
            qg.arrived(k)
            for store in act_stores(k):
                store.start()
        dx = dot_nt(act[1, :, cs], wg[ns, cs]) + dot_nt(act[2, :, cs], wu[ns, cs])
        dx_acc[:, ns] = dx if k == 0 else dx_acc[:, ns] + dx

    def dx_stores(n):
        ns = pl.ds(n * MW, MW)
        for dt in range(2):
            for dd in range(4):
                row = 32 * (2 * (dd % 2) + dd // 2)
                yield pltpu.make_async_copy(dx_acc.at[pl.ds(row, 32), ns], dx_out.at[4 * dt + dd, :, ns],
                                            dx_sem.at[n, 4 * dt + dd])

    stores = [
        pltpu.make_async_copy(cols.at[1], dy_cols_out, o_sem.at[0]),
        pltpu.make_async_copy(cols_t, cols_t_out, o_sem.at[1]),
    ]

    first_chunk()
    for k in range(1, NA):
        ab_partials(k)
        if k >= 2:
            ab_sum(k - 1)
    ab_sum(NA - 1)
    for k in range(NG):
        g_partials(k)
        if k >= 1:
            g_sum(k - 1)
    g_sum(NG - 1)
    stores[0].start()
    for n in range(4):
        cols_t[n * 256:(n + 1) * 256, :] = cols[0, :, n * 256:(n + 1) * 256].T
    stores[1].start()
    for k in range(NA):
        hidden(k)
    for k in range(NG):
        g2(k).start()
    for k in range(NA):
        hg.forward(k)
        if k >= 1:
            outputs(k - 1)
    outputs(NA - 1)
    for k in range(NG):
        hidden_grads(k)
    for n in range(NT):
        ysum.finish(n)
    for n in range(NT):
        ysum.row_copy(n, 1, 0).start()
    for step in ('f0', 'f1', 'd0', 'D0', 'f2', 'd1', 'D1', 'f3', 'd2', 'D2', 'f4', 'd3', 'D3', 'f5', 'd4', 'f6', 'D4',
                 'f7', 'd5', 'D5', 'd6', 'D6', 'd7'):
        k = int(step[1])
        if step[0] == 'f':
            qg.forward(k)
        else:
            dx_part(k, 0 if step[0] == 'd' else 1)
    for n in range(2):
        if n:
            dx_part(NG - 1, n)
        for store in dx_stores(n):
            store.start()
    ysum.collect()
    for i in range(2):
        for q in range(3):
            token_copy(i, q, at.own_row).wait_send()
    for k in range(NA):
        if k == 0:
            first_core_copy(0).wait_send()
            first_core_copy(1).wait_send()
        else:
            a1(k).wait_send()
        a2(k).wait_send()
        act_t_store(k).wait()
    for k in range(NG):
        g1(k).wait_send()
        g2(k).wait_send()
        for store in act_stores(k):
            store.wait()
    hg.drain()
    qg.drain()
    ysum.drain()
    for store in stores:
        store.wait()
    for n in range(2):
        for store in dx_stores(n):
            store.wait()


DMA = pltpu.SemaphoreType.DMA
ANY = pl.BlockSpec(memory_space=pl.ANY)
VMEM = pl.BlockSpec(memory_space=pltpu.VMEM)
HBM = pl.BlockSpec(memory_space=pltpu.HBM)


def shape(dims, dtype):
    return jax.ShapeDtypeStruct(dims, dtype)


def front(x_rows, dy_rows, gate, up, down):
    return pl.pallas_call(
        front_kernel,
        name='front',
        out_shape=(shape((128, HID), BF16), shape((128, HID), BF16), shape((HID, 128), BF16), shape((1024, 128), BF16),
                   shape((128, 1024), BF16), shape((32, 4096), BF16), shape((8, 32, 1024), F32)),
        in_specs=[ANY] * 5,
        out_specs=(ANY,) * 7,
        scratch_shapes=[
            pltpu.VMEM((32, 4096), BF16), pltpu.VMEM((32, 4096), BF16),
            pltpu.VMEM((1024, HID), BF16), pltpu.VMEM((1024, HID), BF16), pltpu.VMEM((HID, 1024), BF16),
            pltpu.VMEM((3, 128, HID), F32), pltpu.VMEM((3, 64, HID), F32), pltpu.VMEM((3, 32, HID), F32),
            pltpu.VMEM((3, 128, HID), BF16), pltpu.VMEM((HID, 128), BF16), pltpu.VMEM((2, 128, 1024), BF16),
            pltpu.VMEM((1024, 128), BF16), pltpu.VMEM((128, 1024), F32), pltpu.VMEM((128, 1024), F32),
            pltpu.VMEM((64, 1024), F32), pltpu.VMEM((64, 1024), BF16),
            DMA((2,)), DMA((2, NA)), DMA((NG,)), DMA((2, 3)), DMA((2, 3)),
            DMA((2,)), DMA((2,)), DMA((NA,)), DMA((NA,)), DMA((NA,)), DMA((NA,)),
            DMA((NG,)), DMA((NG,)), DMA((NG,)), DMA((NG,)),
            DMA((6, NA)), DMA((6, NG)), DMA((NT,)), DMA((NT,)), DMA((NT, 4)), DMA((NT, 4)),
            DMA((NA,)), DMA((2, NG)), DMA((2,)), DMA((2, 8)),
        ],
        compiler_params=pltpu.CompilerParams(collective_id=0, has_side_effects=True, vmem_limit_bytes=VMEM_CAP),
        cost_estimate=pl.CostEstimate(flops=9 * 10**9, bytes_accessed=4 * 10**7, transcendentals=0),
    )(x_rows, dy_rows, gate, up, down)


TILE = 512
SLOTS = 6
MIB = 1 << 20


def stream_tiles(compute, store, width, rest=None):
    full, last = width // TILE, width % TILE
    compute(0, 0, TILE)
    store(0, 0, TILE).start()
    if rest is not None:
        rest()

    def step(i, carry):
        slot = lax.rem(i, SLOTS)

        @pl.when(i >= SLOTS)
        def _():
            store(i - SLOTS, slot, TILE).wait()

        compute(i, slot, TILE)
        store(i, slot, TILE).start()
        return carry

    lax.fori_loop(1, full, step, 0)
    total = full
    if last:
        if full >= SLOTS:
            store(full - SLOTS, full % SLOTS, TILE).wait()
        compute(full, full % SLOTS, last)
        store(full, full % SLOTS, last).start()
        total += 1

    def drain():
        for i in range(max(0, total - SLOTS), total):
            store(i, i % SLOTS, TILE if i < full else last).wait()

    return drain


def column_job(left, right, ring, out, sem):
    def compute(i, slot, width):
        cs = pl.ds(aligned(i * TILE, 128), width)
        ring[slot, :, pl.ds(0, width)] = dot_nn(left[...], right[:, cs])

    def store(i, slot, width):
        return pltpu.make_async_copy(ring.at[slot, :, pl.ds(0, width)],
                                     out.at[:, pl.ds(aligned(i * TILE, 128), width)], sem.at[slot])

    return compute, store


def row_job(left, right, ring, out, sem):
    def compute(i, slot, width):
        ring[slot, pl.ds(0, width), :] = dot_nn(left[pl.ds(aligned(i * TILE, 128), width), :], right[...])

    def store(i, slot, width):
        return pltpu.make_async_copy(ring.at[slot, pl.ds(0, width), :],
                                     out.at[pl.ds(aligned(i * TILE, 128), width), :], sem.at[slot])

    return compute, store


def grads_first_kernel(act_t_hbm, dy_cols_hbm, cols_t_hbm, da_hbm, down_out, gate_out,
                       act_t, dy_cols, cols_t, da, ring_d, ring_c, in_sem, sem_d, sem_c):
    head, tail = pl.ds(0, TILE), pl.ds(TILE, HID - TILE)
    pairs = ((dy_cols_hbm, dy_cols), (act_t_hbm.at[head, :], act_t.at[head, :]),
             (act_t_hbm.at[tail, :], act_t.at[tail, :]), (cols_t_hbm, cols_t), (da_hbm, da))
    loads = [pltpu.make_async_copy(src, dst, in_sem.at[n]) for n, (src, dst) in enumerate(pairs)]
    for load in loads:
        load.start()

    def rest():
        for load in loads[2:]:
            load.wait()

    loads[0].wait()
    loads[1].wait()
    drain_d = stream_tiles(*row_job(act_t, dy_cols, ring_d, down_out, sem_d), HID, rest)
    drain_c = stream_tiles(*column_job(cols_t, da, ring_c, gate_out, sem_c), HID)
    drain_d()
    drain_c()


def grads_first(act_t, dy_cols, cols_t, da):
    return pl.pallas_call(
        grads_first_kernel,
        name='grads_first',
        out_shape=(shape((HID, 1024), F32), shape((1024, HID), F32)),
        in_specs=[HBM] * 4,
        out_specs=(ANY,) * 2,
        scratch_shapes=[pltpu.VMEM((HID, 128), BF16), pltpu.VMEM((128, 1024), BF16), pltpu.VMEM((1024, 128), BF16),
                        pltpu.VMEM((128, HID), BF16),
                        pltpu.VMEM((SLOTS, TILE, 1024), F32), pltpu.VMEM((SLOTS, 1024, TILE), F32),
                        DMA((5,)), DMA((SLOTS,)), DMA((SLOTS,))],
        compiler_params=pltpu.CompilerParams(vmem_limit_bytes=60 * MIB),
        cost_estimate=pl.CostEstimate(flops=2 * 10**10, bytes_accessed=5 * 10**7, transcendentals=0),
    )(act_t, dy_cols, cols_t, da)


def grads_last_kernel(cols_t, db, y_rows, dy_rows, got, up_out, y_out, dx_out, dx_rows, ring, sem, row_sem):
    drain = stream_tiles(*column_job(cols_t, db, ring, up_out, sem), HID)
    copies = (pltpu.make_async_copy(y_rows, y_out, row_sem.at[0]), pltpu.make_async_copy(dx_rows, dx_out, row_sem.at[1]))
    copies[0].start()
    for d in range(4):
        cs = pl.ds(1024 * d, 1024)
        dx_rows[:, cs] = (dy_rows[:, cs].astype(F32) + (got[d] + got[4 + d])).astype(BF16)
    copies[1].start()
    drain()
    for copy in copies:
        copy.wait()


def grads_last(cols_t, db, y, dy, got):
    return pl.pallas_call(
        grads_last_kernel,
        name='grads_last',
        out_shape=(shape((1024, HID), F32), shape((32, 4096), BF16), shape((32, 4096), BF16)),
        in_specs=[VMEM] * 5,
        out_specs=(ANY,) * 3,
        scratch_shapes=[pltpu.VMEM((32, 4096), BF16), pltpu.VMEM((SLOTS, 1024, TILE), F32),
                        DMA((SLOTS,)), DMA((2,))],
        compiler_params=pltpu.CompilerParams(vmem_limit_bytes=20 * MIB),
        cost_estimate=pl.CostEstimate(flops=10**10, bytes_accessed=3 * 10**7, transcendentals=0),
    )(cols_t, db, y, dy, got)


def solution(mesh):
    def device_pass(x_rows, gate_blk, up_blk, down_blk, dy_rows):
        da, db, act_t, cols_t, dy_cols, y_part, dx_part = front(x_rows, dy_rows, gate_blk, up_blk, down_blk)
        got = lax.all_to_all(dx_part, ('tp', 'dp'), 0, 0, tiled=True)
        dw_down, dw_gate = grads_first(act_t, dy_cols, cols_t, da)
        dw_up, y_rows, dx_rows = grads_last(cols_t, db, y_part, dy_rows, got)
        return y_rows, dx_rows, dw_gate, dw_up, dw_down

    row_spec = P('dp', None)
    weight_spec = P('dp', 'tp')
    down_spec = P('tp', 'dp')
    return jax.shard_map(device_pass, mesh=mesh,
                         in_specs=(row_spec, weight_spec, weight_spec, down_spec, row_spec),
                         out_specs=(row_spec, row_spec, weight_spec, weight_spec, down_spec),
                         check_vma=False)
```

```python
import jax
import jax.numpy as jnp
from jax import lax
from jax.experimental import pallas as pl
from jax.experimental.pallas import tpu as pltpu
from jax.sharding import PartitionSpec as P

MESH = pl.DeviceIdType.MESH
F32, BF16 = jnp.float32, jnp.bfloat16
VMEM_CAP = 67043328
HID = 5504


def chunks(start, widths):
    out = []
    for w in widths:
        out.append((start, w))
        start += w
    return tuple(out)


AB = chunks(0, (512, 512, 1024, 1024, 1024, 1024, 384))
GG = chunks(0, (512, 1024, 1024, 1024, 768, 640, 384, 128))
NA, NG = len(AB), len(GG)
NT = 4
TW = 1024 // NT
MW = 512


def aligned(v, m):
    return pl.multiple_of(v, m)


def cols_of(chunk):
    return pl.ds(chunk[0], chunk[1])


def column_tiles(chunk, body, tile=256):
    start, width = chunk
    full = width // tile

    def step(i, carry):
        body(aligned(start + i * tile, 128), tile)
        return carry

    lax.fori_loop(0, full, step, 0)
    if width % tile:
        body(start + full * tile, width % tile)


def dot_nt(a, b):
    return lax.dot_general(a, b, (((1,), (1,)), ((), ())), preferred_element_type=F32)


def dot_nn(a, b):
    return jnp.dot(a, b, preferred_element_type=F32)


class Place:
    def __init__(self):
        self.t = lax.axis_index('tp')
        self.d = lax.axis_index('dp')
        self.cx, self.c = self.d // 2, lax.rem(self.d, 2)
        cx, c = self.cx, self.c
        self.sib = 2 * cx + (1 - c)
        self.opp = 2 * (1 - cx) + c
        self.far = 2 * (1 - cx) + (1 - c)
        self.own_row = aligned(32 * (2 * c + cx), 32)
        self.opp_row = aligned(32 * (2 * c + 1 - cx), 32)
        self.sib_row = aligned(32 * (2 * (1 - c) + cx), 32)
        self.far_row = aligned(32 * (2 * (1 - c) + 1 - cx), 32)
        self.keep = pl.ds(aligned(64 * self.t, 64), 64)
        self.give = pl.ds(aligned(64 * (1 - self.t), 64), 64)

    def rows(self, k):
        if k == 0:
            return self.opp_row, self.own_row, self.far_row, self.sib_row
        return self.own_row, self.opp_row, self.sib_row, self.far_row

    def enter(self):
        barrier = pltpu.get_barrier_semaphore()
        for dt in range(2):
            for dd in range(4):
                if dt or dd:
                    pl.semaphore_signal(barrier, inc=1, device_id_type=MESH, device_id={
                        'tp': lax.rem(self.t + dt, 2), 'dp': lax.rem(self.d + dd, 4)})
        return barrier


class Gather:
    def __init__(self, at, buf, parts, chunk_list, sems):
        self.at, self.buf, self.parts, self.chunks = at, buf, parts, chunk_list
        self.opp_s, self.opp_r, self.sib_s, self.sib_r, self.fwd_s, self.fwd_r = sems

    def copy(self, k, src_row, dst_row, send, recv, to):
        cs = cols_of(self.chunks[k])
        return pltpu.make_async_remote_copy(
            src_ref=self.buf.at[self.parts, pl.ds(src_row, 32), cs],
            dst_ref=self.buf.at[self.parts, pl.ds(dst_row, 32), cs],
            send_sem=send.at[k], recv_sem=recv.at[k], device_id={'dp': to}, device_id_type=MESH)

    def out_opp(self, k, dst=None):
        own = self.at.rows(k)[0]
        return self.copy(k, own, own if dst is None else dst, self.opp_s, self.opp_r, self.at.opp)

    def out_sib(self, k, dst=None):
        own = self.at.rows(k)[0]
        return self.copy(k, own, own if dst is None else dst, self.sib_s, self.sib_r, self.at.sib)

    def out_fwd(self, k, dst=None):
        opp = self.at.rows(k)[1]
        return self.copy(k, opp, opp if dst is None else dst, self.fwd_s, self.fwd_r, self.at.sib)

    def send(self, k):
        self.out_opp(k).start()
        self.out_sib(k).start()

    def forward(self, k):
        self.out_opp(k, self.at.rows(k)[1]).wait_recv()
        self.out_fwd(k).start()

    def arrived(self, k):
        self.out_sib(k, self.at.rows(k)[2]).wait_recv()
        self.out_fwd(k, self.at.rows(k)[3]).wait_recv()

    def drain(self):
        for k in range(len(self.chunks)):
            self.out_opp(k).wait_send()
            self.out_sib(k).wait_send()
            self.out_fwd(k).wait_send()


class RowSum:
    def __init__(self, at, acc, kept, got, ready, landed, sems):
        self.at, self.acc, self.kept, self.got, self.ready, self.landed = at, acc, kept, got, ready, landed
        self.sum_s, self.sum_r, self.row_s, self.row_r = sems
        self.local = at.c == at.t

    def tile(self, n):
        return pl.ds(n * TW, TW)

    def swap(self, n):
        at = self.at
        return pltpu.make_async_remote_copy(
            src_ref=self.acc.at[at.give, self.tile(n)], dst_ref=self.got.at[:, self.tile(n)],
            send_sem=self.sum_s.at[n], recv_sem=self.sum_r.at[n], device_id={'tp': 1 - at.t}, device_id_type=MESH)

    def row_copy(self, n, ox, ot):
        at = self.at
        chip = 1 - at.cx if ox else at.cx
        return pltpu.make_async_remote_copy(
            src_ref=self.ready.at[pl.ds(aligned(32 * chip, 32), 32), self.tile(n)],
            dst_ref=self.landed.at[:, pl.ds(aligned(1024 * at.d + n * TW, 128), TW)],
            send_sem=self.row_s.at[n, 2 * ox + ot], recv_sem=self.row_r.at[n, at.d],
            device_id={'tp': 1 - at.t if ot else at.t, 'dp': 2 * chip + at.t}, device_id_type=MESH)

    def own_copy(self, n):
        at = self.at
        return pltpu.make_async_copy(
            self.ready.at[pl.ds(aligned(32 * at.cx, 32), 32), self.tile(n)],
            self.landed.at[:, pl.ds(aligned(1024 * at.d + n * TW, 128), TW)], self.row_r.at[n, at.d])

    def row_arrive(self, n, s):
        return pltpu.make_async_remote_copy(
            src_ref=self.ready.at[pl.ds(0, 32), self.tile(n)],
            dst_ref=self.landed.at[:, pl.ds(1024 * s + n * TW, TW)],
            send_sem=self.row_s.at[n, 0], recv_sem=self.row_r.at[n, s],
            device_id={'tp': 1 - self.at.t}, device_id_type=MESH)

    def finish(self, n):
        at, ns = self.at, self.tile(n)
        self.swap(n).wait_recv()
        total = self.acc[at.keep, ns] + self.got[:, ns]
        self.ready[:, ns] = (self.kept[at.keep, ns].astype(F32) + total).astype(BF16)
        for ox, ot in ((1, 1), (0, 1)):
            self.row_copy(n, ox, ot).start()

        @pl.when(jnp.logical_not(self.local))
        def _():
            self.row_copy(n, 0, 0).start()

        @pl.when(self.local)
        def _():
            self.own_copy(n).start()

    def collect(self):
        for n in range(NT):
            for s in range(4):
                @pl.when(jnp.logical_not(jnp.logical_and(self.local, self.at.d == s)))
                def _():
                    self.row_arrive(n, s).wait_recv()

            @pl.when(self.local)
            def _():
                self.own_copy(n).wait()

    def drain(self):
        for n in range(NT):
            self.swap(n).wait_send()
            for ox, ot in ((1, 1), (1, 0), (0, 1)):
                self.row_copy(n, ox, ot).wait_send()

        @pl.when(jnp.logical_not(self.local))
        def _():
            for n in range(NT):
                self.row_copy(n, 0, 0).wait_send()


def gate_grads(act, slot, own, cs, a, b, g):
    s = jax.nn.sigmoid(a)
    act[slot, own, cs] = (g * b * s * (1.0 + a * (1.0 - s))).astype(BF16)
    act[slot + 1, own, cs] = (g * (a * s)).astype(BF16)


def front_kernel(x_hbm, dy_hbm, wg_hbm, wu_hbm, wd_hbm,
                 da_out, db_out, act_t_out, cols_t_out, dy_cols_out, y_out, dx_out,
                 x_ref, dy_ref, wg, wu, wd, part, from_sib, from_opp, act, act_t, cols, cols_t, y_acc, dx_acc, y_got, y_ready,
                 in_sem, gu_sem, d_sem, x_send, x_recv, a0_s, a0_r, a1_s, a1_r, a2_s, a2_r, g1_s, g1_r, g2_s, g2_r,
                 h_sems, q_sems, sum_s, sum_r, row_s, row_r, t_sem, q_sem, o_sem, dx_sem):
    at = Place()
    own, opp = pl.ds(at.own_row, 32), pl.ds(at.opp_row, 32)
    sib_half = pl.ds(aligned(64 * (1 - at.c), 64), 64)
    mine, theirs = pl.ds(aligned(32 * at.cx, 32), 32), pl.ds(aligned(32 * (1 - at.cx), 32), 32)

    def gate_up_loads(k):
        cs = cols_of(AB[k])
        return (pltpu.make_async_copy(wg_hbm.at[:, cs], wg.at[:, cs], gu_sem.at[0, k]),
                pltpu.make_async_copy(wu_hbm.at[:, cs], wu.at[:, cs], gu_sem.at[1, k]))

    def down_load(k):
        cs = cols_of(GG[k])
        return pltpu.make_async_copy(wd_hbm.at[cs, :], wd.at[cs, :], d_sem.at[k])

    barrier = at.enter()
    token_loads = (pltpu.make_async_copy(x_hbm, x_ref, in_sem.at[0]),
                   pltpu.make_async_copy(dy_hbm, dy_ref, in_sem.at[1]))
    for load in token_loads:
        load.start()
    for k in range(2):
        for load in gate_up_loads(k):
            load.start()
    pl.semaphore_wait(barrier, 7)

    peers = (at.sib, at.opp, at.far)
    tokens = (x_ref, dy_ref)

    def token_copy(i, q, row):
        return pltpu.make_async_remote_copy(
            src_ref=tokens[i].at[:, pl.ds(aligned(1024 * peers[q], 128), 1024)],
            dst_ref=cols.at[i, pl.ds(row, 32), :],
            send_sem=x_send.at[i, q], recv_sem=x_recv.at[i, q],
            device_id={'dp': peers[q]}, device_id_type=MESH)

    for i in range(2):
        token_loads[i].wait()
        for q in (2, 1, 0):
            token_copy(i, q, at.own_row).start()
    for k in range(2, NA):
        for load in gate_up_loads(k):
            load.start()
    for k in range(NG):
        down_load(k).start()
    for i in range(2):
        cols[i, own, :] = tokens[i][:, pl.ds(aligned(1024 * at.d, 128), 1024)]

    def token_wait(i, which=(0, 1, 2)):
        for q in which:
            token_copy(i, q, (at.sib_row, at.opp_row, at.far_row)[q]).wait_recv()

    def core_copy(parts, chunk, k, send, recv):
        cs = cols_of(chunk)
        return pltpu.make_async_remote_copy(
            src_ref=part.at[parts, sib_half, cs], dst_ref=from_sib.at[parts, :, cs],
            send_sem=send.at[k], recv_sem=recv.at[k], device_id={'dp': at.sib}, device_id_type=MESH)

    def chip_copy(parts, chunk, k, send, recv):
        cs = cols_of(chunk)
        return pltpu.make_async_remote_copy(
            src_ref=part.at[parts, pl.ds(at.rows(k)[1], 32), cs], dst_ref=from_opp.at[parts, :, cs],
            send_sem=send.at[k], recv_sem=recv.at[k], device_id={'dp': at.opp}, device_id_type=MESH)

    ab, gg = pl.ds(0, 2), pl.ds(2, 1)

    def a1(k):
        return core_copy(ab, AB[k], k, a1_s, a1_r)

    def a2(k):
        return chip_copy(ab, AB[k], k, a2_s, a2_r)

    def g1(k):
        return core_copy(gg, GG[k], k, g1_s, g1_r)

    def g2(k):
        return chip_copy(gg, GG[k], k, g2_s, g2_r)

    def first_core_copy(which):
        cs = cols_of(AB[0])
        return pltpu.make_async_remote_copy(
            src_ref=part.at[ab, pl.ds((at.sib_row, at.far_row)[which], 32), cs],
            dst_ref=from_sib.at[ab, (mine, theirs)[which], cs],
            send_sem=a0_s.at[which], recv_sem=a0_r.at[which], device_id={'dp': at.sib}, device_id_type=MESH)

    def first_partials(which):
        upper, lower = [pl.ds(row, 32) for row in ((at.own_row, at.sib_row), (at.opp_row, at.far_row))[which]]
        cs = cols_of(AB[0])
        rows = jnp.concatenate([cols[0, upper, :], cols[0, lower, :]], axis=0)
        for i, w in enumerate((wg, wu)):
            out = dot_nn(rows, w[:, cs])
            part[i, upper, cs] = out[:32]
            part[i, lower, cs] = out[32:]
        first_core_copy(which).start()

    def first_chunk():
        for load in gate_up_loads(0):
            load.wait()
        token_wait(0, (0,))
        first_partials(0)
        first_core_copy(0).wait_recv()
        cs = cols_of(AB[0])
        for i in range(2):
            part[i, own, cs] += from_sib[i, mine, cs]
        a2(0).start()
        token_wait(0, (1, 2))
        first_partials(1)

    def ab_partials(k):
        for load in gate_up_loads(k):
            load.wait()

        def body(col, width):
            cs = pl.ds(col, width)
            part[0, :, cs] = dot_nn(cols[0], wg[:, cs])
            part[1, :, cs] = dot_nn(cols[0], wu[:, cs])

        column_tiles(AB[k], body, 512)
        a1(k).start()

    def ab_sum(k):
        a1(k).wait_recv()

        def add(col, width):
            cs = pl.ds(col, width)
            for i in range(2):
                part[i, opp, cs] += from_sib[i, theirs, cs]

        column_tiles(AB[k], add)
        a2(k).start()

    def g_partials(k):
        down_load(k).wait()
        if k == 0:
            token_wait(1)

        def body(col, width):
            cs = pl.ds(col, width)
            part[2, :, cs] = dot_nt(cols[1], wd[cs, :])

        column_tiles(GG[k], body, 512)
        g1(k).start()

    def g_sum(k):
        g1(k).wait_recv()

        def add(col, width):
            cs = pl.ds(col, width)
            part[2, opp, cs] += from_sib[2, theirs, cs]
            part[2, own, cs] += from_sib[2, mine, cs]

        column_tiles(GG[k], add)

    hg = Gather(at, act, pl.ds(0, 1), AB, [h_sems.at[i] for i in range(6)])
    qg = Gather(at, act, pl.ds(1, 2), GG, [q_sems.at[i] for i in range(6)])

    def hidden(k):
        if k == 0:
            first_core_copy(1).wait_recv()
        a2(k).wait_recv()
        here = pl.ds(at.rows(k)[0], 32)
        core = theirs if k == 0 else mine

        def body(col, width):
            cs = pl.ds(col, width)
            a, b = [part[i, here, cs] + from_sib[i, core, cs] + from_opp[i, :, cs] for i in range(2)]
            part[0, here, cs] = a
            part[1, here, cs] = b
            act[0, here, cs] = (a * jax.nn.sigmoid(a) * b).astype(BF16)

        column_tiles(AB[k], body)
        hg.send(k)

    def act_t_store(k):
        cs = cols_of(AB[k])
        return pltpu.make_async_copy(act_t.at[cs, :], act_t_out.at[cs, :], t_sem.at[k])

    ysum = RowSum(at, y_acc, cols.at[0], y_got, y_ready, y_out, (sum_s, sum_r, row_s, row_r))

    def outputs(k):
        hg.arrived(k)
        cs = cols_of(AB[k])

        def flip(col, width):
            ts = pl.ds(col, width)
            act_t[ts, :] = act[0, :, ts].T

        column_tiles(AB[k], flip)
        act_t_store(k).start()

        def tile(ns):
            y = dot_nn(act[0, :, cs], wd[cs, ns])
            y_acc[:, ns] = y if k == 0 else y_acc[:, ns] + y

        if k < NA - 1:
            @pl.loop(0, 1024 // MW)
            def _(n):
                tile(pl.ds(aligned(n * MW, 128), MW))
        else:
            for n in range(NT):
                tile(pl.ds(n * TW, TW))
                ysum.swap(n).start()

    def hidden_grads(k):
        g2(k).wait_recv()
        here = pl.ds(at.rows(k)[0], 32)

        def body(col, width):
            cs = pl.ds(col, width)
            gate_grads(act, 1, here, cs, part[0, here, cs], part[1, here, cs], part[2, here, cs] + from_opp[2, :, cs])

        column_tiles(GG[k], body)
        qg.send(k)

    def act_stores(k):
        cs = cols_of(GG[k])
        return (pltpu.make_async_copy(act.at[1, :, cs], da_out.at[:, cs], q_sem.at[0, k]),
                pltpu.make_async_copy(act.at[2, :, cs], db_out.at[:, cs], q_sem.at[1, k]))

    def dx_part(k, n):
        cs, ns = cols_of(GG[k]), pl.ds(n * MW, MW)
        if n == 0:
            qg.arrived(k)
            for store in act_stores(k):
                store.start()
        dx = dot_nt(act[1, :, cs], wg[ns, cs]) + dot_nt(act[2, :, cs], wu[ns, cs])
        dx_acc[:, ns] = dx if k == 0 else dx_acc[:, ns] + dx

    def dx_stores(n):
        ns = pl.ds(n * MW, MW)
        for dt in range(2):
            for dd in range(4):
                row = 32 * (2 * (dd % 2) + dd // 2)
                yield pltpu.make_async_copy(dx_acc.at[pl.ds(row, 32), ns], dx_out.at[4 * dt + dd, :, ns],
                                            dx_sem.at[n, 4 * dt + dd])

    stores = [
        pltpu.make_async_copy(cols.at[1], dy_cols_out, o_sem.at[0]),
        pltpu.make_async_copy(cols_t, cols_t_out, o_sem.at[1]),
    ]

    first_chunk()
    for k in range(1, NA):
        ab_partials(k)
        if k >= 2:
            ab_sum(k - 1)
    ab_sum(NA - 1)
    for k in range(NG):
        g_partials(k)
        if k >= 1:
            g_sum(k - 1)
    g_sum(NG - 1)
    stores[0].start()
    for n in range(4):
        cols_t[n * 256:(n + 1) * 256, :] = cols[0, :, n * 256:(n + 1) * 256].T
    stores[1].start()
    for k in range(NA):
        hidden(k)
    for k in range(NG):
        g2(k).start()
    for k in range(NA):
        hg.forward(k)
        if k >= 1:
            outputs(k - 1)
    outputs(NA - 1)
    for k in range(NG):
        hidden_grads(k)
    for n in range(NT):
        ysum.finish(n)
    for n in range(NT):
        ysum.row_copy(n, 1, 0).start()
    for step in ('f0', 'f1', 'd0', 'D0', 'f2', 'd1', 'D1', 'f3', 'd2', 'D2', 'f4', 'd3', 'D3', 'f5', 'd4', 'f6', 'D4',
                 'f7', 'd5', 'D5', 'd6', 'D6', 'd7'):
        k = int(step[1])
        if step[0] == 'f':
            qg.forward(k)
        else:
            dx_part(k, 0 if step[0] == 'd' else 1)
    for n in range(2):
        if n:
            dx_part(NG - 1, n)
        for store in dx_stores(n):
            store.start()
    ysum.collect()
    for i in range(2):
        for q in range(3):
            token_copy(i, q, at.own_row).wait_send()
    for k in range(NA):
        if k == 0:
            first_core_copy(0).wait_send()
            first_core_copy(1).wait_send()
        else:
            a1(k).wait_send()
        a2(k).wait_send()
        act_t_store(k).wait()
    for k in range(NG):
        g1(k).wait_send()
        g2(k).wait_send()
        for store in act_stores(k):
            store.wait()
    hg.drain()
    qg.drain()
    ysum.drain()
    for store in stores:
        store.wait()
    for n in range(2):
        for store in dx_stores(n):
            store.wait()


DMA = pltpu.SemaphoreType.DMA
ANY = pl.BlockSpec(memory_space=pl.ANY)
VMEM = pl.BlockSpec(memory_space=pltpu.VMEM)
HBM = pl.BlockSpec(memory_space=pltpu.HBM)


def shape(dims, dtype):
    return jax.ShapeDtypeStruct(dims, dtype)


def front(x_rows, dy_rows, gate, up, down):
    return pl.pallas_call(
        front_kernel,
        name='front',
        out_shape=(shape((128, HID), BF16), shape((128, HID), BF16), shape((HID, 128), BF16), shape((1024, 128), BF16),
                   shape((128, 1024), BF16), shape((32, 4096), BF16), shape((8, 32, 1024), F32)),
        in_specs=[ANY] * 5,
        out_specs=(ANY,) * 7,
        scratch_shapes=[
            pltpu.VMEM((32, 4096), BF16), pltpu.VMEM((32, 4096), BF16),
            pltpu.VMEM((1024, HID), BF16), pltpu.VMEM((1024, HID), BF16), pltpu.VMEM((HID, 1024), BF16),
            pltpu.VMEM((3, 128, HID), F32), pltpu.VMEM((3, 64, HID), F32), pltpu.VMEM((3, 32, HID), F32),
            pltpu.VMEM((3, 128, HID), BF16), pltpu.VMEM((HID, 128), BF16), pltpu.VMEM((2, 128, 1024), BF16),
            pltpu.VMEM((1024, 128), BF16), pltpu.VMEM((128, 1024), F32), pltpu.VMEM((128, 1024), F32),
            pltpu.VMEM((64, 1024), F32), pltpu.VMEM((64, 1024), BF16),
            DMA((2,)), DMA((2, NA)), DMA((NG,)), DMA((2, 3)), DMA((2, 3)),
            DMA((2,)), DMA((2,)), DMA((NA,)), DMA((NA,)), DMA((NA,)), DMA((NA,)),
            DMA((NG,)), DMA((NG,)), DMA((NG,)), DMA((NG,)),
            DMA((6, NA)), DMA((6, NG)), DMA((NT,)), DMA((NT,)), DMA((NT, 4)), DMA((NT, 4)),
            DMA((NA,)), DMA((2, NG)), DMA((2,)), DMA((2, 8)),
        ],
        compiler_params=pltpu.CompilerParams(collective_id=0, has_side_effects=True, vmem_limit_bytes=VMEM_CAP),
        cost_estimate=pl.CostEstimate(flops=9 * 10**9, bytes_accessed=4 * 10**7, transcendentals=0),
    )(x_rows, dy_rows, gate, up, down)


TILE = 512
SLOTS = 6
MIB = 1 << 20


def stream_tiles(compute, store, width, rest=None):
    full, last = width // TILE, width % TILE
    for off in range(0, TILE, 128):
        compute(0, 0, 128, off)
        store(0, 0, 128, off).start()
    if rest is not None:
        rest()

    def step(i, carry):
        slot = lax.rem(i, SLOTS)

        @pl.when(i >= SLOTS)
        def _():
            store(i - SLOTS, slot, TILE).wait()

        compute(i, slot, TILE)
        store(i, slot, TILE).start()
        return carry

    lax.fori_loop(1, full, step, 0)
    total = full
    if last:
        if full >= SLOTS:
            store(full - SLOTS, full % SLOTS, TILE).wait()
        compute(full, full % SLOTS, last)
        store(full, full % SLOTS, last).start()
        total += 1

    def drain():
        for i in range(max(0, total - SLOTS), total):
            store(i, i % SLOTS, TILE if i < full else last).wait()

    return drain


def column_job(left, right, ring, out, sem):
    def compute(i, slot, width, off=0):
        cs = pl.ds(aligned(i * TILE + off, 128), width)
        ring[slot, :, pl.ds(off, width)] = dot_nn(left[...], right[:, cs])

    def store(i, slot, width, off=0):
        return pltpu.make_async_copy(ring.at[slot, :, pl.ds(off, width)],
                                     out.at[:, pl.ds(aligned(i * TILE + off, 128), width)], sem.at[slot])

    return compute, store


def row_job(left, right, ring, out, sem):
    def compute(i, slot, width, off=0):
        ring[slot, pl.ds(off, width), :] = dot_nn(left[pl.ds(aligned(i * TILE + off, 128), width), :], right[...])

    def store(i, slot, width, off=0):
        return pltpu.make_async_copy(ring.at[slot, pl.ds(off, width), :],
                                     out.at[pl.ds(aligned(i * TILE + off, 128), width), :], sem.at[slot])

    return compute, store


def grads_first_kernel(act_t_hbm, dy_cols_hbm, cols_t_hbm, da_hbm, down_out, gate_out,
                       act_t, dy_cols, cols_t, da, ring_d, ring_c, in_sem, sem_d, sem_c):
    head, tail = pl.ds(0, TILE), pl.ds(TILE, HID - TILE)
    pairs = ((dy_cols_hbm, dy_cols), (act_t_hbm.at[head, :], act_t.at[head, :]),
             (act_t_hbm.at[tail, :], act_t.at[tail, :]), (cols_t_hbm, cols_t), (da_hbm, da))
    loads = [pltpu.make_async_copy(src, dst, in_sem.at[n]) for n, (src, dst) in enumerate(pairs)]
    for load in loads:
        load.start()

    def rest():
        for load in loads[2:]:
            load.wait()

    loads[0].wait()
    loads[1].wait()
    drain_d = stream_tiles(*row_job(act_t, dy_cols, ring_d, down_out, sem_d), HID, rest)
    drain_c = stream_tiles(*column_job(cols_t, da, ring_c, gate_out, sem_c), HID)
    drain_d()
    drain_c()


def grads_first(act_t, dy_cols, cols_t, da):
    return pl.pallas_call(
        grads_first_kernel,
        name='grads_first',
        out_shape=(shape((HID, 1024), F32), shape((1024, HID), F32)),
        in_specs=[HBM] * 4,
        out_specs=(ANY,) * 2,
        scratch_shapes=[pltpu.VMEM((HID, 128), BF16), pltpu.VMEM((128, 1024), BF16), pltpu.VMEM((1024, 128), BF16),
                        pltpu.VMEM((128, HID), BF16),
                        pltpu.VMEM((SLOTS, TILE, 1024), F32), pltpu.VMEM((SLOTS, 1024, TILE), F32),
                        DMA((5,)), DMA((SLOTS,)), DMA((SLOTS,))],
        compiler_params=pltpu.CompilerParams(vmem_limit_bytes=60 * MIB),
        cost_estimate=pl.CostEstimate(flops=2 * 10**10, bytes_accessed=5 * 10**7, transcendentals=0),
    )(act_t, dy_cols, cols_t, da)


def grads_last_kernel(cols_t, db, y_rows, dy_rows, got, up_out, y_out, dx_out, dx_rows, ring, sem, row_sem):
    drain = stream_tiles(*column_job(cols_t, db, ring, up_out, sem), HID)
    copies = (pltpu.make_async_copy(y_rows, y_out, row_sem.at[0]), pltpu.make_async_copy(dx_rows, dx_out, row_sem.at[1]))
    copies[0].start()
    for d in range(4):
        cs = pl.ds(1024 * d, 1024)
        dx_rows[:, cs] = (dy_rows[:, cs].astype(F32) + (got[d] + got[4 + d])).astype(BF16)
    copies[1].start()
    drain()
    for copy in copies:
        copy.wait()


def grads_last(cols_t, db, y, dy, got):
    return pl.pallas_call(
        grads_last_kernel,
        name='grads_last',
        out_shape=(shape((1024, HID), F32), shape((32, 4096), BF16), shape((32, 4096), BF16)),
        in_specs=[VMEM] * 5,
        out_specs=(ANY,) * 3,
        scratch_shapes=[pltpu.VMEM((32, 4096), BF16), pltpu.VMEM((SLOTS, 1024, TILE), F32),
                        DMA((SLOTS,)), DMA((2,))],
        compiler_params=pltpu.CompilerParams(vmem_limit_bytes=20 * MIB),
        cost_estimate=pl.CostEstimate(flops=10**10, bytes_accessed=3 * 10**7, transcendentals=0),
    )(cols_t, db, y, dy, got)


def solution(mesh):
    def device_pass(x_rows, gate_blk, up_blk, down_blk, dy_rows):
        da, db, act_t, cols_t, dy_cols, y_part, dx_part = front(x_rows, dy_rows, gate_blk, up_blk, down_blk)
        got = lax.all_to_all(dx_part, ('tp', 'dp'), 0, 0, tiled=True)
        dw_down, dw_gate = grads_first(act_t, dy_cols, cols_t, da)
        dw_up, y_rows, dx_rows = grads_last(cols_t, db, y_part, dy_rows, got)
        return y_rows, dx_rows, dw_gate, dw_up, dw_down

    row_spec = P('dp', None)
    weight_spec = P('dp', 'tp')
    down_spec = P('tp', 'dp')
    return jax.shard_map(device_pass, mesh=mesh,
                         in_specs=(row_spec, weight_spec, weight_spec, down_spec, row_spec),
                         out_specs=(row_spec, row_spec, weight_spec, weight_spec, down_spec),
                         check_vma=False)
```
